256 devices in a mesh: ep: 16 (over z, core), fsdp: 4 (over x), tp: 4 (over y).
Axes of the slice: x: 4, y: 4, z: 8, core: 2. Of those that a mesh axis runs over, the one named last changes fastest.
Arguments:
- out_grad: bfloat16 [8192, 4096], P(('ep', 'fsdp')), may hold values from -1.5 to 1.5
- routes: int32 [8192, 2], P(('ep', 'fsdp')), may hold values from 0 to 15, all different within a row; in each aligned block of 128 rows (0 to 127, 128 to 255, ...) at most 32 rows name the same one
- chosen_logits: float32 [8192, 2], P(('ep', 'fsdp')), may hold values from -4 to 4
- routed_inputs: bfloat16 [16, 16, 4, 32, 4096], P('ep', None, 'fsdp'), may hold values from -6 to 6
- w_gate: bfloat16 [16, 4096, 1024], P('ep', 'fsdp', 'tp'), may hold values from -0.09375 to 0.09375
- w_up: bfloat16 [16, 4096, 1024], P('ep', 'fsdp', 'tp'), may hold values from -0.09375 to 0.09375
- w_down: bfloat16 [16, 1024, 4096], P('ep', 'tp', 'fsdp'), may hold values from -0.1875 to 0.1875
Outputs:
- input_grad: bfloat16 [8192, 4096], P(('ep', 'fsdp'))
- logit_grad: float32 [8192, 2], P(('ep', 'fsdp'))
- grad_gate: float32 [16, 4096, 1024], P('ep', 'fsdp', 'tp')
- grad_up: float32 [16, 4096, 1024], P('ep', 'fsdp', 'tp')
- grad_down: float32 [16, 1024, 4096], P('ep', 'tp', 'fsdp')
The draws below stay inside these ranges and needn't reach their ends.
Inputs may be any that keep to these rules, and one draw needn't show every extreme that they name: Each row of routes names 2 different experts. In each token group of 128 consecutive rows no expert is named by more than 32 rows, a bound that some block reaches.
All inputs are finite; a program needn't handle non-finite values.
Results may differ from the reference program's by a relative error of at most 0.015.
Values may be sent and summed in bfloat16 or wider, within the bound.
No kernel may reach another device: no remote copies, remote signals or barrier semaphores. Data moves between devices by JAX's collectives and lax.ppermute only.
A program may use at most 128 MiB of HBM per device.

```python
import math
import jax
import jax.numpy as jnp
import numpy as np
from jax import lax

D = 4096
TOP = 2
FF = 1024
TOK_DEV = 128
EXPERTS = 16
SOURCES = 16
GROUPS = 4
CAPACITY = 32
TOKENS = 8192


def steps_of(key, extent, shards, least, top_value):
    factor_of = 1.0
    for axis_at, parts in shards:
        draws = jax.random.uniform(jax.random.fold_in(jax.random.fold_in(key, 6), axis_at), (parts,), jnp.float32, least / len(shards), top_value / len(shards))
        factor_of = factor_of * jnp.repeat(jnp.exp(draws), extent[axis_at] // parts).reshape((-1,) + (1,) * (len(extent) - 1 - axis_at))
    return factor_of


def shared_out(key, own, number, rows, amount, top, reach, skew):
    order = jax.random.permutation(key, amount)
    crowded, common = shares(amount, rows * top, reach, skew, True), shares(amount, rows * top, reach, skew, False)
    places = jnp.arange(amount)

    def named(sizes, rotation):
        used = int((sizes > 0).sum())
        fixed = max(1, used // 4)
        moved = fixed + (places - fixed + rotation * (used - fixed)) % max(1, amount - fixed)
        return jnp.zeros((amount,), jnp.int32).at[order[jnp.where(places < fixed, places, moved)]].set(jnp.asarray(sizes, jnp.int32))

    sizes = jnp.where(number % 4 == 0, named(crowded, number // 4), named(common, number - number // 4 - 1))
    mixed = jax.random.permutation(jax.random.fold_in(own, 3), amount)
    donor, receiver = mixed[0:amount // 2 * 2:2], mixed[1:amount // 2 * 2:2]
    room = jnp.minimum(sizes[donor] - 1, reach - sizes[receiver]) // 2
    room = jnp.where((donor == order[0]) | (receiver == order[0]) | (sizes[receiver] == 0), 0, jnp.maximum(room, 0))
    moved = jax.random.randint(jax.random.fold_in(own, 4), (amount // 2,), 0, 1 << 20) % (room + 1)
    sizes = sizes.at[donor].add(-moved).at[receiver].add(moved)
    labels = jnp.searchsorted(jnp.cumsum(sizes), jnp.arange(rows * top), side="right").astype(jnp.int32)
    grid = labels.reshape(top, rows).T
    grid = grid[jax.random.permutation(jax.random.fold_in(own, 1), rows)]
    rotation = jax.random.randint(jax.random.fold_in(own, 2), (rows, 1), 0, top)
    return jnp.take_along_axis(grid, (jnp.arange(top)[None, :] + rotation) % top, axis=1)


def shares(count, total, bound, slope, full):
    loads = [(1 << 20) // math.isqrt(standing ** slope) + 1 for standing in range(1, count + 1)]
    largest = bound if full else min(bound, max(-(-total // count), total * loads[0] // sum(loads)))
    least = 1 if total - largest >= count - 1 else 0
    holding, spare = [largest] + [least] * (count - 1), total - largest - least * (count - 1)
    while spare > 0:
        candidates = [i for i in range(1, count) if holding[i] < largest] or [i for i in range(1, count) if holding[i] < bound]
        mass, remaining = sum([loads[i] for i in candidates]), spare
        for i in candidates:
            more = min(bound - holding[i], max(1, remaining * loads[i] // mass), spare)
            holding[i] = holding[i] + more
            spare = spare - more
    return np.array(holding)


def scatter_about(own_key, dims, spread, reach, cuts=(), kind=jnp.bfloat16):
    drawn = jax.random.normal(own_key, dims, jnp.float32) * spread
    if len(cuts) > 0:
        drawn = steps_of(own_key, dims, cuts, -0.22, 0.18) * drawn
    return jnp.clip(drawn, min=-reach, max=reach).astype(kind)


def setup_inputs(seed: int = 0) -> dict:
    arg_keys = jax.random.split(jax.random.key(seed), 8)
    out_grad = scatter_about(arg_keys[0], (TOKENS, D), 0.25, 1.5, ((0, 64),))
    routes_keys = jax.random.split(jax.random.fold_in(arg_keys[1], 1), TOKENS // TOK_DEV)
    routes_turns = jax.random.permutation(jax.random.fold_in(arg_keys[1], 3), TOKENS // TOK_DEV)
    routes = jax.vmap(lambda own, number: shared_out(jax.random.fold_in(arg_keys[1], 2), own, number, TOK_DEV, EXPERTS, TOP, CAPACITY, 1))(routes_keys, routes_turns).reshape((TOKENS, TOP))
    chosen_logits = scatter_about(arg_keys[2], (TOKENS, TOP), 1.0, 4.0, ((0, 64),), jnp.float32)
    routed_inputs = scatter_about(arg_keys[3], (EXPERTS, SOURCES, GROUPS, CAPACITY, D), 1.0, 6.0, ((0, 16), (2, 4)))
    w_gate = scatter_about(arg_keys[4], (EXPERTS, D, FF), D ** -0.5, 0.09375, ((0, 16), (1, 4), (2, 4)))
    w_up = scatter_about(arg_keys[5], (EXPERTS, D, FF), D ** -0.5, 0.09375, ((0, 16), (1, 4), (2, 4)))
    w_down = scatter_about(arg_keys[6], (EXPERTS, FF, D), FF ** -0.5, 0.1875, ((0, 16), (1, 4), (2, 4)))
    return dict(out_grad=out_grad, routes=routes, chosen_logits=chosen_logits, routed_inputs=routed_inputs, w_gate=w_gate, w_up=w_up, w_down=w_down)


def group_slots(routes):
    flat_routes = routes.reshape(-1, TOK_DEV * TOP)
    onehot = (flat_routes[:, :, None] == jnp.arange(EXPERTS, dtype=jnp.int32)[None, None, :]).astype(jnp.int32)
    earlier = (jnp.cumsum(onehot, axis=1) - onehot).astype(jnp.int32)
    position = jnp.sum(earlier * onehot, axis=2).astype(jnp.int32)
    return (flat_routes * CAPACITY + position).astype(jnp.int32)


def take_rows(row_values, row_index):
    return jnp.take(row_values, row_index, axis=0)


def expert_pass(operands):
    inputs, scaled, gate_weight, up_weight, down_weight = operands
    gate_act = jnp.dot(inputs, gate_weight, preferred_element_type=jnp.float32)
    up_act = jnp.dot(inputs, up_weight, preferred_element_type=jnp.float32)
    sigmoid_gate = jax.nn.sigmoid(gate_act)
    silu_gate = gate_act * sigmoid_gate
    hidden = (silu_gate * up_act).astype(jnp.bfloat16)
    hidden_grad = jnp.dot(scaled, down_weight.T, preferred_element_type=jnp.float32)
    products = jnp.sum(hidden_grad * hidden.astype(jnp.float32), axis=1).astype(jnp.bfloat16)
    up_grad = (hidden_grad * silu_gate).astype(jnp.bfloat16)
    gate_grad = (hidden_grad * up_act * sigmoid_gate * (1.0 + gate_act * (1.0 - sigmoid_gate))).astype(jnp.bfloat16)
    grad_gate = jnp.dot(inputs.T, gate_grad, preferred_element_type=jnp.float32)
    grad_up = jnp.dot(inputs.T, up_grad, preferred_element_type=jnp.float32)
    grad_down = jnp.dot(hidden.T, scaled, preferred_element_type=jnp.float32)
    slot_grad = jnp.dot(gate_grad, gate_weight.T, preferred_element_type=jnp.float32)
    slot_grad = (slot_grad + jnp.dot(up_grad, up_weight.T, preferred_element_type=jnp.float32)).astype(jnp.bfloat16)
    return grad_gate, grad_up, grad_down, slot_grad, products


def reference(out_grad, routes, chosen_logits, routed_inputs, w_gate, w_up, w_down):
    groups = TOKENS // TOK_DEV
    pair_count = TOK_DEV * TOP
    gate_probs = jax.nn.softmax(chosen_logits, axis=-1)
    slot_index = group_slots(routes)
    weighted = (gate_probs[:, :, None] * out_grad.astype(jnp.float32)[:, None, :]).astype(jnp.bfloat16)
    weighted = weighted.reshape(groups, pair_count, D)
    weighted = jnp.concatenate([weighted, jnp.zeros((groups, 1, D), jnp.bfloat16)], axis=1)
    source = jnp.full((groups, EXPERTS * CAPACITY), pair_count, jnp.int32)
    group_rows = jnp.arange(groups, dtype=jnp.int32)[:, None]
    pair_ids = jnp.broadcast_to(jnp.arange(pair_count, dtype=jnp.int32)[None, :], (groups, pair_count))
    source = source.at[group_rows, slot_index].set(pair_ids)
    scaled = jax.vmap(take_rows)(weighted, source)
    scaled = scaled.reshape(groups, EXPERTS, CAPACITY, D).transpose(1, 0, 2, 3).reshape(EXPERTS, groups * CAPACITY, D)
    inputs = routed_inputs.reshape(EXPERTS, groups * CAPACITY, D)
    grad_gate, grad_up, grad_down, slot_grad, products = lax.map(expert_pass, (inputs, scaled, w_gate, w_up, w_down))
    slot_grad = slot_grad.reshape(EXPERTS, groups, CAPACITY, D).transpose(1, 0, 2, 3).reshape(groups, EXPERTS * CAPACITY, D)
    picked = jax.vmap(take_rows)(slot_grad, slot_index).astype(jnp.float32)
    input_grad = jnp.sum(picked.reshape(TOKENS, TOP, D), axis=1).astype(jnp.bfloat16)
    products = products.reshape(EXPERTS, groups, CAPACITY).transpose(1, 0, 2).reshape(groups, EXPERTS * CAPACITY)
    chosen = jnp.take_along_axis(products, slot_index, axis=1).astype(jnp.float32).reshape(TOKENS, TOP)
    logit_grad = chosen - gate_probs * jnp.sum(chosen, axis=1, keepdims=True)
    return (input_grad, logit_grad, grad_gate, grad_up, grad_down)
```

```python
import jax
import jax.numpy as jnp
from jax import lax
from jax.sharding import PartitionSpec as P

CHUNKS = 2
LANES = 128


def shift(x, axis, step):
    n = lax.axis_size(axis)
    return lax.ppermute(x, axis, [(i, (i + step) % n) for i in range(n)])


def ring_gather(block, axis):
    half = block.shape[0] // 2
    prev = shift(block, axis, 1)
    following = shift(block, axis, -1)
    far_top = shift(prev[:half], axis, 1)
    far_bottom = shift(following[half:], axis, -1)
    return block, following, (far_top, far_bottom), prev


def ring_reduce(own, following, far, prev, axis):
    half = following.shape[0] // 2
    down = jnp.bfloat16
    top = shift(far[0].astype(down), axis, 1).astype(jnp.float32)
    bottom = shift(far[1].astype(down), axis, -1).astype(jnp.float32)
    following = jnp.concatenate([following[:half] + top, following[half:]]).astype(down)
    prev = jnp.concatenate([prev[:half], prev[half:] + bottom]).astype(down)
    from_prev = shift(following, axis, 1).astype(jnp.float32)
    from_next = shift(prev, axis, -1).astype(jnp.float32)
    return own + from_prev + from_next


def dot(left, right, left_dim, right_dim):
    return lax.dot_general(
        left, right, (((left_dim,), (right_dim,)), ((), ())), preferred_element_type=jnp.float32
    )


def slots_of(routes, experts, capacity):
    tokens = routes.shape[0]
    part = capacity // CHUNKS
    hot = (routes[:, :, None] == jnp.arange(experts, dtype=jnp.int32)).astype(jnp.bfloat16)
    before = jnp.arange(tokens)[:, None] > jnp.arange(tokens)[None, :]
    earlier = dot(before.astype(jnp.bfloat16), hot[:, 0] + hot[:, 1], 1, 0)
    place = jnp.sum(earlier[:, None, :] * hot.astype(jnp.float32), axis=2).astype(jnp.int32)
    return (place // part) * (experts * part) + routes * part + place % part


def split_float(x):
    high = x.astype(jnp.bfloat16)
    low = (x - high.astype(jnp.float32)).astype(jnp.bfloat16)
    return high, low


def on_device(out_grad, routes, chosen_logits, routed_inputs, w_gate, w_up, w_down):
    experts = lax.axis_size("ep")
    ring = lax.axis_size("fsdp")
    f, t = lax.axis_index("fsdp"), lax.axis_index("tp")
    tokens, model_width = out_grad.shape
    capacity = routed_inputs.shape[3]
    part = capacity // CHUNKS
    rows = experts * part
    slots = experts * capacity
    narrow = model_width // ring
    width = w_gate.shape[2]

    gate_up = ring_gather(jnp.concatenate([w_gate[0], w_up[0]], axis=1), "fsdp")
    down = ring_gather(w_down[0], "fsdp")

    gate_probs = jax.nn.softmax(chosen_logits, axis=-1)
    slot_index = slots_of(routes, experts, capacity)
    picks = (slot_index[:, :, None] == jnp.arange(slots, dtype=jnp.int32)).astype(jnp.bfloat16)
    mine = (f + t) % ring
    piece = lax.dynamic_slice_in_dim(out_grad, mine * narrow, narrow, 1).astype(jnp.float32)
    weighted = (gate_probs[:, :, None] * piece[:, None, :]).astype(jnp.bfloat16)
    outgoing = lax.dot_general(
        picks, weighted, (((0, 1), (0, 1)), ((), ())), preferred_element_type=jnp.float32
    ).astype(jnp.bfloat16)
    outgoing = outgoing.reshape(CHUNKS, experts, part, narrow)
    scaled = []
    for h in range(CHUNKS):
        arrived = lax.all_to_all(outgoing[h], "ep", split_axis=0, concat_axis=0, tiled=True)
        own, following, far, prev = ring_gather(arrived.reshape(rows, narrow), "tp")
        by_distance = jnp.concatenate([own, following, far[0], far[1], prev])
        by_distance = by_distance.reshape(ring, rows, narrow)
        scaled.append(
            [
                lax.dynamic_index_in_dim(by_distance, (r - t) % ring, 0, keepdims=False)
                for r in range(ring)
            ]
        )

    inputs = routed_inputs[0, :, 0].reshape(experts, CHUNKS, part, model_width)
    inputs = inputs.transpose(1, 0, 2, 3).reshape(slots, model_width)
    inputs = [
        lax.dynamic_slice_in_dim(inputs, ((f + r) % ring) * narrow, narrow, 1) for r in range(ring)
    ]

    half = narrow // 2
    act = dot(inputs[0], gate_up[0], 1, 0)
    act += dot(inputs[1], gate_up[1], 1, 0) + dot(inputs[3], gate_up[3], 1, 0)
    act += dot(inputs[2][:, :half], gate_up[2][0], 1, 0)
    act += dot(inputs[2][:, half:], gate_up[2][1], 1, 0)
    gate_act, up_act = act[:, :width], act[:, width:]
    sigmoid_gate = jax.nn.sigmoid(gate_act)
    silu_gate = gate_act * sigmoid_gate
    hidden = (silu_gate * up_act).astype(jnp.bfloat16)
    gate_slope = up_act * sigmoid_gate * (1.0 + gate_act * (1.0 - sigmoid_gate))

    gate_up_stack = jnp.concatenate(
        [gate_up[0], gate_up[1], gate_up[2][0], gate_up[2][1], gate_up[3]]
    ).reshape(ring, narrow, 2 * width)
    down_far = jnp.concatenate(down[2])
    downs = [down[0], down[1], down_far, down[3]]

    pair_grads, back = [], []
    for h in range(CHUNKS):
        own = slice(h * rows, (h + 1) * rows)
        hidden_grad = sum(dot(scaled[h][r], downs[r], 1, 1) for r in range(ring))
        products = jnp.sum(hidden_grad * hidden[own].astype(jnp.float32), axis=1)
        pair = jnp.concatenate(
            [
                (hidden_grad * gate_slope[own]).astype(jnp.bfloat16),
                (hidden_grad * silu_gate[own]).astype(jnp.bfloat16),
            ],
            axis=1,
        )
        pair_grads.append(pair)
        slot_parts = [
            dot(
                pair,
                lax.dynamic_index_in_dim(gate_up_stack, (t + q) % ring, 0, keepdims=False),
                1,
                1,
            )
            for q in range(ring)
        ]
        far = slot_parts[2]
        slot_grad = ring_reduce(
            slot_parts[0], slot_parts[1], (far[: rows // 2], far[rows // 2 :]), slot_parts[3], "tp"
        ).astype(jnp.bfloat16)
        high, low = split_float(products)
        lane = jnp.arange(LANES)[None, :]
        extra = jnp.where(lane == 0, high[:, None], jnp.where(lane == 1, low[:, None], 0))
        leaving = jnp.concatenate([slot_grad, extra.astype(jnp.bfloat16)], axis=1)
        back.append(
            lax.all_to_all(
                leaving.reshape(experts, part, narrow + LANES),
                "ep",
                split_axis=0,
                concat_axis=0,
                tiled=True,
            ).reshape(rows, narrow + LANES)
        )

    pairs = jnp.concatenate(pair_grads)

    def down_chunk(r, first=0, count=width):
        return sum(
            dot(
                hidden[h * rows : (h + 1) * rows, first : first + count], scaled[h][r], 0, 0
            )
            for h in range(CHUNKS)
        )

    grad_down = ring_reduce(
        down_chunk(0),
        down_chunk(1),
        (down_chunk(2, 0, width // 2), down_chunk(2, width // 2, width // 2)),
        down_chunk(3),
        "fsdp",
    )
    grad_gate_up = ring_reduce(
        dot(inputs[0], pairs, 0, 0),
        dot(inputs[1], pairs, 0, 0),
        (dot(inputs[2][:, :half], pairs, 0, 0), dot(inputs[2][:, half:], pairs, 0, 0)),
        dot(inputs[3], pairs, 0, 0),
        "fsdp",
    )

    back = jnp.concatenate(back)
    combined = dot(picks[:, 0] + picks[:, 1], back[:, :narrow], 1, 0).astype(jnp.bfloat16)
    chosen = lax.dot_general(
        picks, back[:, narrow:], (((2,), (0,)), ((), ())), preferred_element_type=jnp.float32
    )
    chosen = chosen[:, :, 0] + chosen[:, :, 1]
    high, low = split_float(chosen)
    tail = jnp.pad(jnp.concatenate([high, low], axis=1), ((0, 0), (0, LANES - 4)))
    token_rows = jnp.concatenate([combined, tail], axis=1)
    gathered = [token_rows] + [shift(token_rows, "tp", -q) for q in range(1, ring)]
    input_grad = jnp.zeros((tokens, model_width), jnp.bfloat16)
    total = jnp.zeros((tokens, 2), jnp.float32)
    for q in range(ring):
        input_grad = lax.dynamic_update_slice_in_dim(
            input_grad, gathered[q][:, :narrow], ((mine + q) % ring) * narrow, 1
        )
        tail = gathered[q][:, narrow : narrow + 4].astype(jnp.float32)
        total += tail[:, :2] + tail[:, 2:]
    total = total.astype(jnp.bfloat16).astype(jnp.float32)
    logit_grad = total - gate_probs * jnp.sum(total, axis=1, keepdims=True)
    return (
        input_grad,
        logit_grad,
        grad_gate_up[:, :width][None],
        grad_gate_up[:, width:][None],
        grad_down[None],
    )


def solution(mesh):
    return jax.shard_map(
        on_device,
        mesh=mesh,
        in_specs=(
            P(("ep", "fsdp"), None),
            P(("ep", "fsdp"), None),
            P(("ep", "fsdp"), None),
            P("ep", None, "fsdp", None, None),
            P("ep", "fsdp", "tp"),
            P("ep", "fsdp", "tp"),
            P("ep", "tp", "fsdp"),
        ),
        out_specs=(
            P(("ep", "fsdp"), None),
            P(("ep", "fsdp"), None),
            P("ep", "fsdp", "tp"),
            P("ep", "fsdp", "tp"),
            P("ep", "tp", "fsdp"),
        ),
        check_vma=False,
    )
```

```python
import functools

import jax
import jax.numpy as jnp
from jax import lax
from jax.experimental import pallas as pl
from jax.experimental.pallas import tpu as pltpu
from jax.sharding import PartitionSpec as P


CHUNKS = 2
RING = 4
LANES = 128
VMEM_LIMIT = 48 << 20


def shift(x, axis, step):
    n = lax.axis_size(axis)
    return lax.ppermute(x, axis, [(i, (i + step) % n) for i in range(n)])


def exchange(x):
    return lax.all_to_all(x, "ep", split_axis=0, concat_axis=0, tiled=True)


def ring_gather(block, axis):
    half = block.shape[0] // 2
    prev = shift(block, axis, 1)
    following = shift(block, axis, -1)
    far_top = shift(prev[:half], axis, 1)
    far_bottom = shift(following[half:], axis, -1)
    return block, following, far_top, far_bottom, prev


def ring_reduce(following, far_top, far_bottom, prev, axis):
    top = shift(far_top, axis, 1)
    bottom = shift(far_bottom, axis, -1)
    following = add_half(following, top, 0)
    prev = add_half(prev, bottom, 1)
    from_prev = shift(following, axis, 1)
    from_next = shift(prev, axis, -1)
    return from_prev, from_next


def call(kernel, out_shape, **options):
    return pl.pallas_call(
        kernel,
        out_shape=out_shape,
        compiler_params=pltpu.CompilerParams(vmem_limit_bytes=VMEM_LIMIT),
        **options,
    )


def bf16(*shape):
    return jax.ShapeDtypeStruct(shape, jnp.bfloat16)


def f32(*shape):
    return jax.ShapeDtypeStruct(shape, jnp.float32)


def dot(left, right, left_dim=1, right_dim=0):
    return lax.dot_general(
        left, right, (((left_dim,), (right_dim,)), ((), ())), preferred_element_type=jnp.float32
    )


def add_half(whole, half, index):
    def kernel(whole_ref, half_ref, out_ref):
        total = whole_ref[...].astype(jnp.float32) + half_ref[...].astype(jnp.float32)
        out_ref[...] = total.astype(jnp.bfloat16)

    spec = pl.BlockSpec(half.shape, lambda i: (index, 0))
    return call(
        kernel,
        bf16(*whole.shape),
        grid=(1,),
        in_specs=[spec, pl.BlockSpec(half.shape, lambda i: (0, 0))],
        out_specs=spec,
        input_output_aliases={0: 0},
    )(whole, half)


def pack(w_gate, w_up, w_down):
    depth, width = w_gate.shape

    def kernel(gate_ref, up_ref, down_ref, out_ref):
        out_ref[:depth] = gate_ref[...]
        out_ref[depth : 2 * depth] = up_ref[...]
        for c in range(depth // width):
            out_ref[pl.ds(2 * depth + c * width, width)] = down_ref[:, c * width : (c + 1) * width]

    return call(kernel, bf16(3 * depth, width))(w_gate, w_up, w_down)


def weight_parts(refs, r, depth):
    half = depth // 2
    if r == 2:
        places = [(refs[2], i * half) for i in range(3)] + [(refs[3], i * half) for i in range(3)]
    else:
        ref = refs[(0, 1, None, 4)[r]]
        places = [(ref, i * half) for i in range(6)]
    return places[0:2], places[2:4], places[4:6]


def activations(here, routed_inputs, weights, width):
    _, sources, _, capacity, model_width = routed_inputs.shape
    depth = model_width // RING
    part = capacity // CHUNKS
    rows = sources * part
    half = depth // 2

    def kernel(here_ref, x_ref, w0, w1, w2, w3, w4, hidden_ref, silu_ref, slope_ref, gate, up):
        refs = (w0, w1, w2, w3, w4)
        step = pl.program_id(0)
        for r in range(RING):

            @pl.when(step == r)
            def _():
                gates, ups, _ = weight_parts(refs, r, depth)
                for h in range(CHUNKS):
                    x = x_ref[0, :, 0, h * part : (h + 1) * part, :].reshape(rows, depth)
                    own = slice(h * rows, (h + 1) * rows)
                    for pieces, total in ((gates, gate), (ups, up)):
                        value = sum(
                            dot(x[:, i * half : (i + 1) * half], ref[pl.ds(first, half)])
                            for i, (ref, first) in enumerate(pieces)
                        )
                        total[own] = value if r == 0 else total[own] + value

        @pl.when(step == RING - 1)
        def _():
            gate_act, up_act = gate[...], up[...]
            sigmoid_gate = jax.nn.sigmoid(gate_act)
            silu_gate = gate_act * sigmoid_gate
            hidden_ref[...] = (silu_gate * up_act).astype(jnp.bfloat16)
            silu_ref[...] = silu_gate
            slope_ref[...] = up_act * sigmoid_gate * (1.0 + gate_act * (1.0 - sigmoid_gate))

    slots = sources * capacity
    whole = pl.BlockSpec(memory_space=pltpu.VMEM)
    return call(
        kernel,
        (bf16(slots, width), f32(slots, width), f32(slots, width)),
        grid_spec=pltpu.PrefetchScalarGridSpec(
            num_scalar_prefetch=1,
            grid=(RING,),
            in_specs=[
                pl.BlockSpec(
                    (1, sources, 1, capacity, depth),
                    lambda i, here: (0, 0, 0, 0, (here[0] + i) % RING),
                )
            ]
            + [whole] * 5,
            out_specs=(pl.BlockSpec((slots, width), lambda i, here: (0, 0)),) * 3,
            scratch_shapes=[pltpu.VMEM((slots, width), jnp.float32)] * 2,
        ),
    )(here, routed_inputs, *weights)


def gradients(here, h, scaled, weights, hidden, silu, slope):
    rows, depth = scaled[0].shape
    width = hidden.shape[1]
    half = depth // 2
    blocks = depth // width

    def kernel(here_ref, *refs):
        scaled_refs, weight_refs, refs = refs[:5], refs[5:10], refs[10:]
        hidden_ref, silu_ref, slope_ref, refs = *refs[:3], refs[3:]
        pair_ref, extra_ref, own_ref, next_ref, top_ref, bottom_ref, prev_ref, by_r, refs = (
            *refs[:8],
            refs[8:],
        )
        parts, sems = refs
        t = here_ref[1]
        copies = []
        for i, (q, first, count) in enumerate(
            (
                (0, 0, rows),
                (1, 0, rows),
                (2, 0, rows // 2),
                (2, rows // 2, rows // 2),
                (3, 0, rows),
            )
        ):
            copies.append(
                pltpu.make_async_copy(
                    scaled_refs[i],
                    by_r.at[(t + q) % RING, pl.ds(first, count)],
                    sems.at[i],
                )
            )
        for copy in copies:
            copy.start()
        for copy in copies:
            copy.wait()
        hidden_grad = jnp.zeros((rows, width), jnp.float32)
        for r in range(RING):
            _, _, downs = weight_parts(weight_refs, r, depth)
            for c in range(blocks):
                ref, first = downs[c * 2 // blocks]
                first += (c % (blocks // 2)) * width
                hidden_grad += dot(
                    by_r[r, :, c * width : (c + 1) * width], ref[pl.ds(first, width)], 1, 1
                )
        products = jnp.sum(
            hidden_grad * hidden_ref[...].astype(jnp.float32), axis=1, keepdims=True
        )
        high = products.astype(jnp.bfloat16).astype(jnp.float32)
        lane = lax.broadcasted_iota(jnp.int32, (rows, LANES), 1)
        extra = jnp.where(lane == 0, high, jnp.where(lane == 1, products - high, 0.0))
        extra_ref[...] = extra.astype(jnp.bfloat16)
        gate_grad = (hidden_grad * slope_ref[...]).astype(jnp.bfloat16)
        up_grad = (hidden_grad * silu_ref[...]).astype(jnp.bfloat16)
        pair_ref[:, :width] = gate_grad
        pair_ref[:, width:] = up_grad
        for r in range(RING):
            gates, ups, _ = weight_parts(weight_refs, r, depth)
            q = (r - t + RING) % RING
            for i in range(2):
                gate_ref, gate_first = gates[i]
                up_ref, up_first = ups[i]
                value = dot(gate_grad, gate_ref[pl.ds(gate_first, half)], 1, 1)
                value += dot(up_grad, up_ref[pl.ds(up_first, half)], 1, 1)
                parts[q, :, i * half : (i + 1) * half] = value.astype(jnp.bfloat16)
        own_ref[...] = parts[0]
        next_ref[...] = parts[1]
        top_ref[...] = parts[2, : rows // 2]
        bottom_ref[...] = parts[2, rows // 2 :]
        prev_ref[...] = parts[3]

    anywhere = pl.BlockSpec(memory_space=pl.ANY)
    whole = pl.BlockSpec(memory_space=pltpu.VMEM)
    mine = pl.BlockSpec((rows, width), lambda i, here: (h, 0))
    return call(
        kernel,
        (
            bf16(rows, 2 * width),
            bf16(rows, LANES),
            bf16(rows, depth),
            bf16(rows, depth),
            bf16(rows // 2, depth),
            bf16(rows // 2, depth),
            bf16(rows, depth),
            bf16(RING, rows, depth),
        ),
        grid_spec=pltpu.PrefetchScalarGridSpec(
            num_scalar_prefetch=1,
            grid=(1,),
            in_specs=[anywhere] * 5 + [whole] * 5 + [mine] * 3,
            out_specs=(whole,) * 8,
            scratch_shapes=[
                pltpu.VMEM((RING, rows, depth), jnp.bfloat16),
                pltpu.SemaphoreType.DMA((5,)),
            ],
        ),
    )(here, *scaled, *weights, hidden, silu, slope)


def weight_chunk(here, r, routed_inputs, hidden, pairs, scaled, received=None):
    _, sources, _, capacity, model_width = routed_inputs.shape
    depth = model_width // RING
    part = capacity // CHUNKS
    rows = sources * part
    width = hidden.shape[1]
    half = depth // 2

    def kernel(here_ref, x_ref, hidden_ref, *refs):
        pair_refs, scaled_refs, refs = refs[:CHUNKS], refs[CHUNKS : 2 * CHUNKS], refs[2 * CHUNKS :]

        def inputs(h, i):
            x = x_ref[0, :, 0, h * part : (h + 1) * part, i * half : (i + 1) * half]
            return x.reshape(rows, half)

        for i in range(6):
            if i < 4:
                lanes = slice((i // 2) * width, (i // 2 + 1) * width)
                value = sum(
                    dot(inputs(h, i % 2), pair_refs[h][:, lanes], 0, 0) for h in range(CHUNKS)
                )
                values = [(value, slice(0, half))]
            else:
                values = []
                for c in range(half // width):
                    first = (i - 4) * half + c * width
                    value = sum(
                        dot(
                            hidden_ref[h * rows : (h + 1) * rows],
                            scaled_refs[h][0, :, first : first + width],
                            0,
                            0,
                        )
                        for h in range(CHUNKS)
                    )
                    values.append((value, slice(c * width, (c + 1) * width)))
            for value, place in values:
                source = pl.ds(i * half + place.start, place.stop - place.start)
                if r:
                    out_ref = refs[i // 3] if r == 2 else refs[0]
                    at = (i % 3 if r == 2 else i) * half + place.start
                    out_ref[pl.ds(at, place.stop - place.start)] = value.astype(jnp.bfloat16)
                    continue
                value += refs[0][source].astype(jnp.float32) + refs[1][source].astype(jnp.float32)
                if i < 4:
                    refs[2 + i // 2][pl.ds((i % 2) * half, half)] = value
                else:
                    first = (i - 4) * half + place.start
                    refs[4][:, first : first + width] = value

    whole = pl.BlockSpec(memory_space=pltpu.VMEM)
    chunk = pl.BlockSpec((1, rows, depth), lambda i, here: (r, 0, 0))
    if r == 0:
        outs = (f32(depth, width), f32(depth, width), f32(width, depth))
    elif r == 2:
        outs = (bf16(3 * half, width), bf16(3 * half, width))
    else:
        outs = (bf16(6 * half, width),)
    received = received or ()
    return call(
        kernel,
        outs,
        grid_spec=pltpu.PrefetchScalarGridSpec(
            num_scalar_prefetch=1,
            grid=(1,),
            in_specs=[
                pl.BlockSpec(
                    (1, sources, 1, capacity, depth),
                    lambda i, here: (0, 0, 0, 0, (here[0] + r) % RING),
                ),
                whole,
            ]
            + [whole] * CHUNKS
            + [chunk] * CHUNKS
            + [whole] * len(received),
            out_specs=(whole,) * len(outs),
        ),
    )(here, routed_inputs, hidden, *pairs, *scaled, *received)


def leaving_rows(own, from_prev, from_next, extra):
    rows, narrow = own.shape

    def kernel(own_ref, prev_ref, next_ref, extra_ref, out_ref):
        total = own_ref[...].astype(jnp.float32) + prev_ref[...].astype(jnp.float32)
        total += next_ref[...].astype(jnp.float32)
        out_ref[:, :narrow] = total.astype(jnp.bfloat16)
        out_ref[:, narrow:] = extra_ref[...]

    return call(kernel, bf16(rows, narrow + LANES))(own, from_prev, from_next, extra)


def token_rows(slot_index, back):
    tokens = slot_index.shape[0]
    rows, wide = back[0].shape
    narrow = wide - LANES

    def kernel(slot_ref, *refs):
        back_refs, out_ref = refs[:CHUNKS], refs[CHUNKS]
        total = jnp.zeros((tokens, narrow), jnp.float32)
        chosen = [jnp.zeros((tokens, LANES), jnp.float32)] * 2
        for h in range(CHUNKS):
            slot = lax.broadcasted_iota(jnp.int32, (tokens, rows), 1) + h * rows
            picks = [
                jnp.where(slot_ref[:, k : k + 1] == slot, 1.0, 0.0).astype(jnp.bfloat16)
                for k in range(2)
            ]
            total += dot(picks[0] + picks[1], back_refs[h][:, :narrow])
            chosen = [c + dot(p, back_refs[h][:, narrow:]) for c, p in zip(chosen, picks)]
        out_ref[:, :narrow] = total.astype(jnp.bfloat16)
        lane = lax.broadcasted_iota(jnp.int32, (tokens, LANES), 1)
        tail = jnp.zeros((tokens, LANES), jnp.float32)
        for k in range(2):
            value = chosen[k][:, 0:1] + chosen[k][:, 1:2]
            high = value.astype(jnp.bfloat16).astype(jnp.float32)
            tail = jnp.where(lane == 2 * k, high, jnp.where(lane == 2 * k + 1, value - high, tail))
        out_ref[:, narrow:] = tail.astype(jnp.bfloat16)

    return call(kernel, bf16(tokens, wide))(slot_index, *back)


def finish_tokens(here, gate_probs, gathered):
    tokens, wide = gathered[0].shape
    narrow = wide - LANES

    def kernel(here_ref, probs_ref, *refs):
        out_ref, logit_ref = refs[RING:]
        total = jnp.zeros((tokens, LANES), jnp.float32)
        for q in range(RING):
            first = ((here_ref[0] + here_ref[1] + q) % RING) * narrow
            out_ref[:, pl.ds(pl.multiple_of(first, LANES), narrow)] = refs[q][:, :narrow]
            total += refs[q][:, narrow:].astype(jnp.float32)
        chosen = [
            (total[:, 2 * k : 2 * k + 1] + total[:, 2 * k + 1 : 2 * k + 2])
            .astype(jnp.bfloat16)
            .astype(jnp.float32)
            for k in range(2)
        ]
        both = chosen[0] + chosen[1]
        for k in range(2):
            logit_ref[:, k : k + 1] = chosen[k] - probs_ref[:, k : k + 1] * both

    whole = pl.BlockSpec(memory_space=pltpu.VMEM)
    return call(
        kernel,
        (bf16(tokens, RING * narrow), f32(tokens, 2)),
        grid_spec=pltpu.PrefetchScalarGridSpec(
            num_scalar_prefetch=1,
            grid=(1,),
            in_specs=[whole] * (RING + 1),
            out_specs=(whole,) * 2,
        ),
    )(here, gate_probs, *gathered)


def slots_of(routes, experts, capacity):
    tokens = routes.shape[0]
    part = capacity // CHUNKS
    hot = (routes[:, :, None] == jnp.arange(experts, dtype=jnp.int32)).astype(jnp.bfloat16)
    before = jnp.arange(tokens)[:, None] > jnp.arange(tokens)[None, :]
    earlier = dot(before.astype(jnp.bfloat16), hot[:, 0] + hot[:, 1])
    place = jnp.sum(earlier[:, None, :] * hot.astype(jnp.float32), axis=2).astype(jnp.int32)
    return (place // part) * (experts * part) + routes * part + place % part


def layer(out_grad, routes, chosen_logits, routed_inputs, w_gate, w_up, w_down):
    experts = lax.axis_size("ep")
    f, t = lax.axis_index("fsdp"), lax.axis_index("tp")
    here = jnp.stack([f, t]).astype(jnp.int32)
    model_width = out_grad.shape[1]
    capacity = routed_inputs.shape[3]
    part = capacity // CHUNKS
    rows = experts * part
    slots = experts * capacity
    narrow = model_width // RING
    width = w_gate.shape[2]

    weights = ring_gather(pack(w_gate[0], w_up[0], w_down[0]), "fsdp")

    gate_probs = jax.nn.softmax(chosen_logits, axis=-1)
    slot_index = slots_of(routes, experts, capacity)
    picks = (slot_index[:, :, None] == jnp.arange(slots, dtype=jnp.int32)).astype(jnp.bfloat16)
    mine = (f + t) % RING
    piece = lax.dynamic_slice_in_dim(out_grad, mine * narrow, narrow, 1).astype(jnp.float32)
    weighted = (gate_probs[:, :, None] * piece[:, None, :]).astype(jnp.bfloat16)
    outgoing = lax.dot_general(
        picks, weighted, (((0, 1), (0, 1)), ((), ())), preferred_element_type=jnp.float32
    ).astype(jnp.bfloat16)
    outgoing = outgoing.reshape(CHUNKS, experts, part, narrow)
    arrived = [
        ring_gather(exchange(outgoing[h]).reshape(rows, narrow), "tp")
        for h in range(CHUNKS)
    ]

    hidden, silu, slope = activations(here, routed_inputs, weights, width)
    pairs, scaled, back = [], [], []
    for h in range(CHUNKS):
        pair, extra, own, following, top, bottom, prev, by_r = gradients(
            here, h, arrived[h], weights, hidden, silu, slope
        )
        pairs.append(pair)
        scaled.append(by_r)
        received = ring_reduce(following, top, bottom, prev, "tp")
        leaving = leaving_rows(own, *received, extra)
        leaving = leaving.reshape(experts, part, narrow + LANES)
        back.append(exchange(leaving).reshape(rows, narrow + LANES))

    chunk = functools.partial(
        weight_chunk, here, routed_inputs=routed_inputs, hidden=hidden, pairs=pairs, scaled=scaled
    )
    received = ring_reduce(*chunk(1), *chunk(2), *chunk(3), "fsdp")
    grad_gate, grad_up, grad_down = chunk(0, received=received)

    mine_rows = token_rows(slot_index, back)
    gathered = [mine_rows] + [shift(mine_rows, "tp", -q) for q in range(1, RING)]
    input_grad, logit_grad = finish_tokens(here, gate_probs, gathered)
    return input_grad, logit_grad, grad_gate[None], grad_up[None], grad_down[None]


def solution(mesh):
    return jax.shard_map(
        layer,
        mesh=mesh,
        in_specs=(
            P(("ep", "fsdp"), None),
            P(("ep", "fsdp"), None),
            P(("ep", "fsdp"), None),
            P("ep", None, "fsdp", None, None),
            P("ep", "fsdp", "tp"),
            P("ep", "fsdp", "tp"),
            P("ep", "tp", "fsdp"),
        ),
        out_specs=(
            P(("ep", "fsdp"), None),
            P(("ep", "fsdp"), None),
            P("ep", "fsdp", "tp"),
            P("ep", "fsdp", "tp"),
            P("ep", "tp", "fsdp"),
        ),
        check_vma=False,
    )
```

```python
import functools

import jax
import jax.numpy as jnp
from jax import lax
from jax.experimental import pallas as pl
from jax.experimental.pallas import tpu as pltpu
from jax.sharding import PartitionSpec as P


CHUNKS = 1
RING = 4
LANES = 128
MIB = 1 << 20


def shift(x, axis, step):
    n = lax.axis_size(axis)
    return lax.ppermute(x, axis, [(i, (i + step) % n) for i in range(n)])


def exchange(x):
    return lax.all_to_all(x, "ep", split_axis=0, concat_axis=0, tiled=True)


def ring_gather(block, axis):
    half = block.shape[0] // 2
    prev = shift(block, axis, 1)
    following = shift(block, axis, -1)
    far_top = shift(prev[:half], axis, 1)
    far_bottom = shift(following[half:], axis, -1)
    return block, following, far_top, far_bottom, prev


def ring_reduce(following, far_top, far_bottom, prev, axis):
    top = shift(far_top, axis, 1)
    bottom = shift(far_bottom, axis, -1)
    following = add_half(following, top, 0)
    prev = add_half(prev, bottom, 1)
    from_prev = shift(following, axis, 1)
    from_next = shift(prev, axis, -1)
    return from_prev, from_next


def call(kernel, out_shape, mib=8, **options):
    return pl.pallas_call(
        kernel,
        out_shape=out_shape,
        compiler_params=pltpu.CompilerParams(vmem_limit_bytes=mib * MIB),
        **options,
    )


def bf16(*shape):
    return jax.ShapeDtypeStruct(shape, jnp.bfloat16)


def f32(*shape):
    return jax.ShapeDtypeStruct(shape, jnp.float32)


def dot(left, right, left_dim=1, right_dim=0):
    return lax.dot_general(
        left, right, (((left_dim,), (right_dim,)), ((), ())), preferred_element_type=jnp.float32
    )


def add_half(whole, half, index):
    def kernel(whole_ref, half_ref, out_ref):
        total = whole_ref[...].astype(jnp.float32) + half_ref[...].astype(jnp.float32)
        out_ref[...] = total.astype(jnp.bfloat16)

    spec = pl.BlockSpec(half.shape, lambda i: (index, 0))
    return call(
        kernel,
        bf16(*whole.shape),
        grid=(1,),
        in_specs=[spec, pl.BlockSpec(half.shape, lambda i: (0, 0))],
        out_specs=spec,
        input_output_aliases={0: 0},
    )(whole, half)


def pack(w_gate, w_up, w_down):
    depth, width = w_gate.shape

    blocks = depth // width

    def kernel(gate_ref, up_ref, down_ref, out_ref, sems):
        pairs = [(gate_ref, 0, depth), (up_ref, depth, depth)]
        for c in range(blocks):
            lanes = down_ref.at[:, pl.ds(c * width, width)]
            pairs.append((lanes, 2 * depth + c * width, width))
        copies = [
            pltpu.make_async_copy(source, out_ref.at[pl.ds(first, count)], sems.at[i])
            for i, (source, first, count) in enumerate(pairs)
        ]
        for copy in copies:
            copy.start()
        for copy in copies:
            copy.wait()

    return call(
        kernel,
        bf16(3 * depth, width),
        in_specs=[pl.BlockSpec(memory_space=pltpu.HBM)] * 3,
        out_specs=pl.BlockSpec(memory_space=pltpu.VMEM),
        scratch_shapes=[pltpu.SemaphoreType.DMA((2 + blocks,))],
    )(w_gate, w_up, w_down)


def weight_parts(refs, r, depth):
    half = depth // 2
    if r == 2:
        places = [(refs[2], i * half) for i in range(3)] + [(refs[3], i * half) for i in range(3)]
    else:
        ref = refs[(0, 1, None, 4)[r]]
        places = [(ref, i * half) for i in range(6)]
    return places[0:2], places[2:4], places[4:6]


def activations(here, routed_inputs, weights, width):
    _, sources, _, capacity, model_width = routed_inputs.shape
    depth = model_width // RING
    part = capacity // CHUNKS
    rows = sources * part
    half = depth // 2

    def kernel(here_ref, x_ref, w0, w1, w2, w3, w4, hidden_ref, silu_ref, slope_ref, gate, up):
        refs = (w0, w1, w2, w3, w4)
        step = pl.program_id(0)
        for r in range(RING):

            @pl.when(step == r)
            def _():
                gates, ups, _ = weight_parts(refs, r, depth)
                for h in range(CHUNKS):
                    x = x_ref[0, :, 0, h * part : (h + 1) * part, :].reshape(rows, depth)
                    own = slice(h * rows, (h + 1) * rows)
                    for pieces, total in ((gates, gate), (ups, up)):
                        value = sum(
                            dot(x[:, i * half : (i + 1) * half], ref[pl.ds(first, half)])
                            for i, (ref, first) in enumerate(pieces)
                        )
                        total[own] = value if r == 0 else total[own] + value

        @pl.when(step == RING - 1)
        def _():
            gate_act, up_act = gate[...], up[...]
            sigmoid_gate = jax.nn.sigmoid(gate_act)
            silu_gate = gate_act * sigmoid_gate
            hidden_ref[...] = (silu_gate * up_act).astype(jnp.bfloat16)
            silu_ref[...] = silu_gate
            slope_ref[...] = up_act * sigmoid_gate * (1.0 + gate_act * (1.0 - sigmoid_gate))

    slots = sources * capacity
    whole = pl.BlockSpec(memory_space=pltpu.VMEM)
    return call(
        kernel,
        (bf16(slots, width), f32(slots, width), f32(slots, width)),
        mib=14,
        grid_spec=pltpu.PrefetchScalarGridSpec(
            num_scalar_prefetch=1,
            grid=(RING,),
            in_specs=[
                pl.BlockSpec(
                    (1, sources, 1, capacity, depth),
                    lambda i, here: (0, 0, 0, 0, (here[0] + i) % RING),
                )
            ]
            + [whole] * 5,
            out_specs=(pl.BlockSpec((slots, width), lambda i, here: (0, 0)),) * 3,
            scratch_shapes=[pltpu.VMEM((slots, width), jnp.float32)] * 2,
        ),
    )(here, routed_inputs, *weights)


def pair_gradients(here, h, scaled, weights, hidden, silu, slope):
    rows, depth = scaled[0].shape
    width = hidden.shape[1]
    half = depth // 2
    blocks = depth // width
    places = ((0, 0, rows), (1, 0, rows), (2, 0, rows // 2), (2, rows // 2, rows // 2), (3, 0, rows))

    def kernel(here_ref, *refs):
        scaled_refs, weight_refs, refs = refs[:5], refs[5:10], refs[10:]
        hidden_ref, silu_ref, slope_ref = refs[:3]
        pair_ref, extra_ref, top_ref, bottom_ref, by_r, sems = refs[3:]
        t = here_ref[1]
        copies = [
            pltpu.make_async_copy(
                scaled_refs[i], by_r.at[(t + q) % RING, pl.ds(first, count)], sems.at[i]
            )
            for i, (q, first, count) in enumerate(places)
        ]
        for copy in copies:
            copy.start()
        for copy in copies:
            copy.wait()
        hidden_grad = jnp.zeros((rows, width), jnp.float32)
        for r in range(RING):
            _, _, downs = weight_parts(weight_refs, r, depth)
            for c in range(blocks):
                ref, first = downs[c * 2 // blocks]
                first += (c % (blocks // 2)) * width
                hidden_grad += dot(
                    by_r[r, :, c * width : (c + 1) * width], ref[pl.ds(first, width)], 1, 1
                )
        products = jnp.sum(
            hidden_grad * hidden_ref[...].astype(jnp.float32), axis=1, keepdims=True
        )
        high = products.astype(jnp.bfloat16).astype(jnp.float32)
        lane = lax.broadcasted_iota(jnp.int32, (rows, LANES), 1)
        extra = jnp.where(lane == 0, high, jnp.where(lane == 1, products - high, 0.0))
        extra_ref[...] = extra.astype(jnp.bfloat16)
        pair_ref[:, :width] = (hidden_grad * slope_ref[...]).astype(jnp.bfloat16)
        pair_ref[:, width:] = (hidden_grad * silu_ref[...]).astype(jnp.bfloat16)
        for r in range(RING):

            @pl.when((t + 2) % RING == r)
            def _():
                for i, value in enumerate(slot_part(pair_ref, weight_refs, r, depth)):
                    top_ref[:, i * half : (i + 1) * half] = value[: rows // 2]
                    bottom_ref[:, i * half : (i + 1) * half] = value[rows // 2 :]

    anywhere = pl.BlockSpec(memory_space=pl.ANY)
    whole = pl.BlockSpec(memory_space=pltpu.VMEM)
    mine = pl.BlockSpec((rows, width), lambda i, here: (h, 0))
    return call(
        kernel,
        (
            bf16(rows, 2 * width),
            bf16(rows, LANES),
            bf16(rows // 2, depth),
            bf16(rows // 2, depth),
            bf16(RING, rows, depth),
        ),
        mib=20,
        grid_spec=pltpu.PrefetchScalarGridSpec(
            num_scalar_prefetch=1,
            grid=(1,),
            in_specs=[anywhere] * 5 + [whole] * 5 + [mine] * 3,
            out_specs=(whole,) * 5,
            scratch_shapes=[pltpu.SemaphoreType.DMA((5,))],
        ),
    )(here, *scaled, *weights, hidden, silu, slope)


def slot_part(pair_ref, weight_refs, r, depth):
    half = depth // 2
    width = pair_ref.shape[1] // 2
    gates, ups, _ = weight_parts(weight_refs, r, depth)
    values = []
    for i in range(2):
        gate_ref, gate_first = gates[i]
        up_ref, up_first = ups[i]
        value = dot(pair_ref[:, :width], gate_ref[pl.ds(gate_first, half)], 1, 1)
        value += dot(pair_ref[:, width:], up_ref[pl.ds(up_first, half)], 1, 1)
        values.append(value.astype(jnp.bfloat16))
    return values


def slot_gradients(here, pair, weights):
    rows = pair.shape[0]
    depth = weights[0].shape[0] // 3
    half = depth // 2

    def kernel(here_ref, pair_ref, *refs):
        weight_refs, (own_ref, next_ref, prev_ref, parts) = refs[:5], refs[5:]
        t = here_ref[1]
        for r in range(RING):
            q = (r - t + RING) % RING

            @pl.when(q != 2)
            def _():
                for i, value in enumerate(slot_part(pair_ref, weight_refs, r, depth)):
                    parts[q, :, i * half : (i + 1) * half] = value

        own_ref[...] = parts[0]
        next_ref[...] = parts[1]
        prev_ref[...] = parts[3]

    whole = pl.BlockSpec(memory_space=pltpu.VMEM)
    return call(
        kernel,
        (bf16(rows, depth),) * 3,
        mib=16,
        grid_spec=pltpu.PrefetchScalarGridSpec(
            num_scalar_prefetch=1,
            grid=(1,),
            in_specs=[whole] * 6,
            out_specs=(whole,) * 3,
            scratch_shapes=[pltpu.VMEM((RING, rows, depth), jnp.bfloat16)],
        ),
    )(here, pair, *weights)


def weight_chunk(here, r, routed_inputs, hidden, pairs, scaled, received=None):
    _, sources, _, capacity, model_width = routed_inputs.shape
    depth = model_width // RING
    part = capacity // CHUNKS
    rows = sources * part
    width = hidden.shape[1]
    half = depth // 2

    def kernel(here_ref, x_ref, hidden_ref, *refs):
        pair_refs, scaled_refs, refs = refs[:CHUNKS], refs[CHUNKS : 2 * CHUNKS], refs[2 * CHUNKS :]

        def inputs(h, i):
            x = x_ref[0, :, 0, h * part : (h + 1) * part, i * half : (i + 1) * half]
            return x.reshape(rows, half)

        for i in range(6):
            if i < 4:
                lanes = slice((i // 2) * width, (i // 2 + 1) * width)
                value = sum(
                    dot(inputs(h, i % 2), pair_refs[h][:, lanes], 0, 0) for h in range(CHUNKS)
                )
                values = [(value, slice(0, half))]
            else:
                values = []
                for c in range(half // width):
                    first = (i - 4) * half + c * width
                    value = sum(
                        dot(
                            hidden_ref[h * rows : (h + 1) * rows],
                            scaled_refs[h][0, :, first : first + width],
                            0,
                            0,
                        )
                        for h in range(CHUNKS)
                    )
                    values.append((value, slice(c * width, (c + 1) * width)))
            for value, place in values:
                source = pl.ds(i * half + place.start, place.stop - place.start)
                if r:
                    out_ref = refs[i // 3] if r == 2 else refs[0]
                    at = (i % 3 if r == 2 else i) * half + place.start
                    out_ref[pl.ds(at, place.stop - place.start)] = value.astype(jnp.bfloat16)
                    continue
                value += refs[0][source].astype(jnp.float32) + refs[1][source].astype(jnp.float32)
                if i < 4:
                    refs[2 + i // 2][pl.ds((i % 2) * half, half)] = value
                else:
                    first = (i - 4) * half + place.start
                    refs[4][:, first : first + width] = value

    whole = pl.BlockSpec(memory_space=pltpu.VMEM)
    chunk = pl.BlockSpec((1, rows, depth), lambda i, here: (r, 0, 0))
    if r == 0:
        outs = (f32(depth, width), f32(depth, width), f32(width, depth))
    elif r == 2:
        outs = (bf16(3 * half, width), bf16(3 * half, width))
    else:
        outs = (bf16(6 * half, width),)
    received = received or ()
    return call(
        kernel,
        outs,
        mib=16 if r == 0 else 10,
        grid_spec=pltpu.PrefetchScalarGridSpec(
            num_scalar_prefetch=1,
            grid=(1,),
            in_specs=[
                pl.BlockSpec(
                    (1, sources, 1, capacity, depth),
                    lambda i, here: (0, 0, 0, 0, (here[0] + r) % RING),
                ),
                whole,
            ]
            + [whole] * CHUNKS
            + [chunk] * CHUNKS
            + [whole] * len(received),
            out_specs=(whole,) * len(outs),
        ),
    )(here, routed_inputs, hidden, *pairs, *scaled, *received)


def leaving_rows(own, from_prev, from_next, extra):
    rows, narrow = own.shape

    def kernel(own_ref, prev_ref, next_ref, extra_ref, out_ref):
        total = own_ref[...].astype(jnp.float32) + prev_ref[...].astype(jnp.float32)
        total += next_ref[...].astype(jnp.float32)
        out_ref[:, :narrow] = total.astype(jnp.bfloat16)
        out_ref[:, narrow:] = extra_ref[...]

    return call(kernel, bf16(rows, narrow + LANES))(own, from_prev, from_next, extra)


def token_rows(slot_index, back):
    tokens = slot_index.shape[0]
    rows, wide = back[0].shape
    narrow = wide - LANES

    def kernel(slot_ref, *refs):
        back_refs, out_ref = refs[:CHUNKS], refs[CHUNKS]
        total = jnp.zeros((tokens, narrow), jnp.float32)
        chosen = [jnp.zeros((tokens, LANES), jnp.float32)] * 2
        for h in range(CHUNKS):
            slot = lax.broadcasted_iota(jnp.int32, (tokens, rows), 1) + h * rows
            picks = [
                jnp.where(slot_ref[:, k : k + 1] == slot, 1.0, 0.0).astype(jnp.bfloat16)
                for k in range(2)
            ]
            total += dot(picks[0] + picks[1], back_refs[h][:, :narrow])
            chosen = [c + dot(p, back_refs[h][:, narrow:]) for c, p in zip(chosen, picks)]
        out_ref[:, :narrow] = total.astype(jnp.bfloat16)
        lane = lax.broadcasted_iota(jnp.int32, (tokens, LANES), 1)
        tail = jnp.zeros((tokens, LANES), jnp.float32)
        for k in range(2):
            value = chosen[k][:, 0:1] + chosen[k][:, 1:2]
            high = value.astype(jnp.bfloat16).astype(jnp.float32)
            tail = jnp.where(lane == 2 * k, high, jnp.where(lane == 2 * k + 1, value - high, tail))
        out_ref[:, narrow:] = tail.astype(jnp.bfloat16)

    return call(kernel, bf16(tokens, wide))(slot_index, *back)


def finish_tokens(here, gate_probs, gathered):
    tokens, wide = gathered[0].shape
    narrow = wide - LANES

    def kernel(here_ref, probs_ref, *refs):
        out_ref, logit_ref = refs[RING:]
        total = jnp.zeros((tokens, LANES), jnp.float32)
        for q in range(RING):
            first = ((here_ref[0] + here_ref[1] + q) % RING) * narrow
            out_ref[:, pl.ds(pl.multiple_of(first, LANES), narrow)] = refs[q][:, :narrow]
            total += refs[q][:, narrow:].astype(jnp.float32)
        chosen = [
            (total[:, 2 * k : 2 * k + 1] + total[:, 2 * k + 1 : 2 * k + 2])
            .astype(jnp.bfloat16)
            .astype(jnp.float32)
            for k in range(2)
        ]
        both = chosen[0] + chosen[1]
        for k in range(2):
            logit_ref[:, k : k + 1] = chosen[k] - probs_ref[:, k : k + 1] * both

    whole = pl.BlockSpec(memory_space=pltpu.VMEM)
    return call(
        kernel,
        (bf16(tokens, RING * narrow), f32(tokens, 2)),
        grid_spec=pltpu.PrefetchScalarGridSpec(
            num_scalar_prefetch=1,
            grid=(1,),
            in_specs=[whole] * (RING + 1),
            out_specs=(whole,) * 2,
        ),
    )(here, gate_probs, *gathered)


def slots_of(routes, experts, capacity):
    tokens = routes.shape[0]
    part = capacity // CHUNKS
    hot = (routes[:, :, None] == jnp.arange(experts, dtype=jnp.int32)).astype(jnp.bfloat16)
    before = jnp.arange(tokens)[:, None] > jnp.arange(tokens)[None, :]
    earlier = dot(before.astype(jnp.bfloat16), hot[:, 0] + hot[:, 1])
    place = jnp.sum(earlier[:, None, :] * hot.astype(jnp.float32), axis=2).astype(jnp.int32)
    return (place // part) * (experts * part) + routes * part + place % part


def layer(out_grad, routes, chosen_logits, routed_inputs, w_gate, w_up, w_down):
    experts = lax.axis_size("ep")
    f, t = lax.axis_index("fsdp"), lax.axis_index("tp")
    here = jnp.stack([f, t]).astype(jnp.int32)
    model_width = out_grad.shape[1]
    capacity = routed_inputs.shape[3]
    part = capacity // CHUNKS
    rows = experts * part
    slots = experts * capacity
    narrow = model_width // RING
    width = w_gate.shape[2]

    weights = ring_gather(pack(w_gate[0], w_up[0], w_down[0]), "fsdp")

    gate_probs = jax.nn.softmax(chosen_logits, axis=-1)
    slot_index = slots_of(routes, experts, capacity)
    picks = (slot_index[:, :, None] == jnp.arange(slots, dtype=jnp.int32)).astype(jnp.bfloat16)
    mine = (f + t) % RING
    piece = lax.dynamic_slice_in_dim(out_grad, mine * narrow, narrow, 1).astype(jnp.float32)
    weighted = (gate_probs[:, :, None] * piece[:, None, :]).astype(jnp.bfloat16)
    outgoing = lax.dot_general(
        picks, weighted, (((0, 1), (0, 1)), ((), ())), preferred_element_type=jnp.float32
    ).astype(jnp.bfloat16)
    outgoing = outgoing.reshape(CHUNKS, experts, part, narrow)
    arrived = [
        ring_gather(exchange(outgoing[h]).reshape(rows, narrow), "tp")
        for h in range(CHUNKS)
    ]

    hidden, silu, slope = activations(here, routed_inputs, weights, width)
    pairs, scaled, back = [], [], []
    for h in range(CHUNKS):
        pair, extra, top, bottom, by_r = pair_gradients(
            here, h, arrived[h], weights, hidden, silu, slope
        )
        own, following, prev = slot_gradients(here, pair, weights)
        pairs.append(pair)
        scaled.append(by_r)
        received = ring_reduce(following, top, bottom, prev, "tp")
        leaving = leaving_rows(own, *received, extra)
        leaving = leaving.reshape(experts, part, narrow + LANES)
        back.append(exchange(leaving).reshape(rows, narrow + LANES))

    chunk = functools.partial(
        weight_chunk, here, routed_inputs=routed_inputs, hidden=hidden, pairs=pairs, scaled=scaled
    )
    received = ring_reduce(*chunk(1), *chunk(2), *chunk(3), "fsdp")
    grad_gate, grad_up, grad_down = chunk(0, received=received)

    mine_rows = token_rows(slot_index, back)
    gathered = [mine_rows] + [shift(mine_rows, "tp", -q) for q in range(1, RING)]
    input_grad, logit_grad = finish_tokens(here, gate_probs, gathered)
    return input_grad, logit_grad, grad_gate[None], grad_up[None], grad_down[None]


def solution(mesh):
    return jax.shard_map(
        layer,
        mesh=mesh,
        in_specs=(
            P(("ep", "fsdp"), None),
            P(("ep", "fsdp"), None),
            P(("ep", "fsdp"), None),
            P("ep", None, "fsdp", None, None),
            P("ep", "fsdp", "tp"),
            P("ep", "fsdp", "tp"),
            P("ep", "tp", "fsdp"),
        ),
        out_specs=(
            P(("ep", "fsdp"), None),
            P(("ep", "fsdp"), None),
            P("ep", "fsdp", "tp"),
            P("ep", "fsdp", "tp"),
            P("ep", "tp", "fsdp"),
        ),
        check_vma=False,
    )
```

```python
import functools

import jax
import jax.numpy as jnp
from jax import lax
from jax.experimental import pallas as pl
from jax.experimental.pallas import tpu as pltpu
from jax.sharding import PartitionSpec as P


RING = 4
LANES = 128
MIB = 1 << 20


SHIFTS = (0, 1, -1, 2, -2, 3, -3, 4)
GROUPS = ((0, 1, 2, 3, 4), (5, 6, 7))


def shift(x, axis, step):
    n = lax.axis_size(axis)
    return lax.ppermute(x, axis, [(i, (i + step) % n) for i in range(n)])


def shift_z(x, step):
    n = lax.axis_size("ep")
    return lax.ppermute(x, "ep", [(i, (i + 2 * step) % n) for i in range(n)])


def swap_cores(x):
    return lax.ppermute(x, "ep", [(i, i ^ 1) for i in range(lax.axis_size("ep"))])


def ring_gather(block, axis):
    half = block.shape[0] // 2
    prev = shift(block, axis, 1)
    following = shift(block, axis, -1)
    far_top = shift(prev[:half], axis, 1)
    far_bottom = shift(following[half:], axis, -1)
    return block, following, far_top, far_bottom, prev


def ring_reduce(following, far_top, far_bottom, prev, axis):
    top = shift(far_top, axis, 1)
    bottom = shift(far_bottom, axis, -1)
    following = add_half(following, top, 0)
    prev = add_half(prev, bottom, 1)
    from_prev = shift(following, axis, 1)
    from_next = shift(prev, axis, -1)
    return from_prev, from_next


def call(kernel, out_shape, mib=8, **options):
    return pl.pallas_call(
        kernel,
        out_shape=out_shape,
        compiler_params=pltpu.CompilerParams(vmem_limit_bytes=mib * MIB),
        **options,
    )


def bf16(*shape):
    return jax.ShapeDtypeStruct(shape, jnp.bfloat16)


def f32(*shape):
    return jax.ShapeDtypeStruct(shape, jnp.float32)


def dot(left, right, left_dim=1, right_dim=0):
    return lax.dot_general(
        left, right, (((left_dim,), (right_dim,)), ((), ())), preferred_element_type=jnp.float32
    )


def add_half(whole, half, index):
    def kernel(whole_ref, half_ref, out_ref):
        total = whole_ref[...].astype(jnp.float32) + half_ref[...].astype(jnp.float32)
        out_ref[...] = total.astype(jnp.bfloat16)

    spec = pl.BlockSpec(half.shape, lambda i: (index, 0))
    return call(
        kernel,
        bf16(*whole.shape),
        grid=(1,),
        in_specs=[spec, pl.BlockSpec(half.shape, lambda i: (0, 0))],
        out_specs=spec,
        input_output_aliases={0: 0},
    )(whole, half)


def pack(w_gate, w_up, w_down):
    depth, width = w_gate.shape

    blocks = depth // width

    def kernel(gate_ref, up_ref, down_ref, out_ref, sems):
        pairs = [(gate_ref, 0, depth), (up_ref, depth, depth)]
        for c in range(blocks):
            lanes = down_ref.at[:, pl.ds(c * width, width)]
            pairs.append((lanes, 2 * depth + c * width, width))
        copies = [
            pltpu.make_async_copy(source, out_ref.at[pl.ds(first, count)], sems.at[i])
            for i, (source, first, count) in enumerate(pairs)
        ]
        for copy in copies:
            copy.start()
        for copy in copies:
            copy.wait()

    return call(
        kernel,
        bf16(3 * depth, width),
        in_specs=[pl.BlockSpec(memory_space=pltpu.HBM)] * 3,
        out_specs=pl.BlockSpec(memory_space=pltpu.VMEM),
        scratch_shapes=[pltpu.SemaphoreType.DMA((2 + blocks,))],
    )(w_gate, w_up, w_down)


def weight_parts(refs, r, depth):
    half = depth // 2
    if r == 2:
        places = [(refs[2], i * half) for i in range(3)] + [(refs[3], i * half) for i in range(3)]
    else:
        ref = refs[(0, 1, None, 4)[r]]
        places = [(ref, i * half) for i in range(6)]
    return places[0:2], places[2:4], places[4:6]


def fill_rows(here_ref, x_ref, rows_ref):
    capacity = x_ref.shape[3]
    z, core = here_ref[2], here_ref[3]
    count = len(SHIFTS)
    for j, step in enumerate(SHIFTS):
        for k in range(2):
            source = ((z - step + count) % count) * 2 + (core if k == 0 else 1 - core)
            rows_ref[pl.ds((2 * j + k) * capacity, capacity)] = x_ref[0, source, 0]


def activations(here, routed_inputs, weights, width):
    _, sources, _, capacity, model_width = routed_inputs.shape
    depth = model_width // RING
    slots = sources * capacity
    half = depth // 2

    def kernel(here_ref, x_ref, w0, w1, w2, w3, w4, hidden_ref, silu_ref, slope_ref, x, gate, up):
        refs = (w0, w1, w2, w3, w4)
        step = pl.program_id(0)
        fill_rows(here_ref, x_ref, x)
        for r in range(RING):

            @pl.when(step == r)
            def _():
                gates, ups, _ = weight_parts(refs, r, depth)
                for pieces, total in ((gates, gate), (ups, up)):
                    value = sum(
                        dot(x[:, i * half : (i + 1) * half], ref[pl.ds(first, half)])
                        for i, (ref, first) in enumerate(pieces)
                    )
                    total[...] = value if r == 0 else total[...] + value

        @pl.when(step == RING - 1)
        def _():
            gate_act, up_act = gate[...], up[...]
            sigmoid_gate = jax.nn.sigmoid(gate_act)
            silu_gate = gate_act * sigmoid_gate
            hidden_ref[...] = (silu_gate * up_act).astype(jnp.bfloat16)
            silu_ref[...] = silu_gate
            slope_ref[...] = up_act * sigmoid_gate * (1.0 + gate_act * (1.0 - sigmoid_gate))

    whole = pl.BlockSpec(memory_space=pltpu.VMEM)
    return call(
        kernel,
        (bf16(slots, width), f32(slots, width), f32(slots, width)),
        mib=16,
        grid_spec=pltpu.PrefetchScalarGridSpec(
            num_scalar_prefetch=1,
            grid=(RING,),
            in_specs=[
                pl.BlockSpec(
                    (1, sources, 1, capacity, depth),
                    lambda i, here: (0, 0, 0, 0, (here[0] + i) % RING),
                )
            ]
            + [whole] * 5,
            out_specs=(pl.BlockSpec((slots, width), lambda i, here: (0, 0)),) * 3,
            scratch_shapes=[pltpu.VMEM((slots, depth), jnp.bfloat16)]
            + [pltpu.VMEM((slots, width), jnp.float32)] * 2,
        ),
    )(here, routed_inputs, *weights)


def pair_gradients(here, start, scaled, weights, hidden, silu, slope):
    rows, depth = scaled[0].shape
    width = hidden.shape[1]
    half = depth // 2
    blocks = depth // width
    places = ((0, 0, rows), (1, 0, rows), (2, 0, rows // 2), (2, rows // 2, rows // 2), (3, 0, rows))

    def kernel(here_ref, *refs):
        scaled_refs, weight_refs, refs = refs[:5], refs[5:10], refs[10:]
        hidden_ref, silu_ref, slope_ref = refs[:3]
        pair_ref, extra_ref, top_ref, bottom_ref, by_r, sems = refs[3:]
        t = here_ref[1]
        copies = [
            pltpu.make_async_copy(
                scaled_refs[i], by_r.at[(t + q) % RING, pl.ds(first, count)], sems.at[i]
            )
            for i, (q, first, count) in enumerate(places)
        ]
        for copy in copies:
            copy.start()
        for copy in copies:
            copy.wait()
        hidden_grad = jnp.zeros((rows, width), jnp.float32)
        for r in range(RING):
            _, _, downs = weight_parts(weight_refs, r, depth)
            for c in range(blocks):
                ref, first = downs[c * 2 // blocks]
                first += (c % (blocks // 2)) * width
                hidden_grad += dot(
                    by_r[r, :, c * width : (c + 1) * width], ref[pl.ds(first, width)], 1, 1
                )
        products = jnp.sum(
            hidden_grad * hidden_ref[start : start + rows].astype(jnp.float32), axis=1, keepdims=True
        )
        high = products.astype(jnp.bfloat16).astype(jnp.float32)
        lane = lax.broadcasted_iota(jnp.int32, (rows, LANES), 1)
        extra = jnp.where(lane == 0, high, jnp.where(lane == 1, products - high, 0.0))
        extra_ref[...] = extra.astype(jnp.bfloat16)
        pair_ref[:, :width] = (hidden_grad * slope_ref[start : start + rows]).astype(jnp.bfloat16)
        pair_ref[:, width:] = (hidden_grad * silu_ref[start : start + rows]).astype(jnp.bfloat16)
        for r in range(RING):

            @pl.when((t + 2) % RING == r)
            def _():
                for i, value in enumerate(slot_part(pair_ref, weight_refs, r, depth)):
                    top_ref[:, i * half : (i + 1) * half] = value[: rows // 2]
                    bottom_ref[:, i * half : (i + 1) * half] = value[rows // 2 :]

    anywhere = pl.BlockSpec(memory_space=pl.ANY)
    whole = pl.BlockSpec(memory_space=pltpu.VMEM)
    return call(
        kernel,
        (
            bf16(rows, 2 * width),
            bf16(rows, LANES),
            bf16(rows // 2, depth),
            bf16(rows // 2, depth),
            bf16(RING, rows, depth),
        ),
        mib=20,
        grid_spec=pltpu.PrefetchScalarGridSpec(
            num_scalar_prefetch=1,
            grid=(1,),
            in_specs=[anywhere] * 5 + [whole] * 8,
            out_specs=(whole,) * 5,
            scratch_shapes=[pltpu.SemaphoreType.DMA((5,))],
        ),
    )(here, *scaled, *weights, hidden, silu, slope)


def slot_part(pair_ref, weight_refs, r, depth):
    half = depth // 2
    width = pair_ref.shape[1] // 2
    gates, ups, _ = weight_parts(weight_refs, r, depth)
    values = []
    for i in range(2):
        gate_ref, gate_first = gates[i]
        up_ref, up_first = ups[i]
        value = dot(pair_ref[:, :width], gate_ref[pl.ds(gate_first, half)], 1, 1)
        value += dot(pair_ref[:, width:], up_ref[pl.ds(up_first, half)], 1, 1)
        values.append(value.astype(jnp.bfloat16))
    return values


def slot_gradients(here, pair, weights):
    rows = pair.shape[0]
    depth = weights[0].shape[0] // 3
    half = depth // 2

    def kernel(here_ref, pair_ref, *refs):
        weight_refs, (own_ref, next_ref, prev_ref, parts) = refs[:5], refs[5:]
        t = here_ref[1]
        for r in range(RING):
            q = (r - t + RING) % RING

            @pl.when(q != 2)
            def _():
                for i, value in enumerate(slot_part(pair_ref, weight_refs, r, depth)):
                    parts[q, :, i * half : (i + 1) * half] = value

        own_ref[...] = parts[0]
        next_ref[...] = parts[1]
        prev_ref[...] = parts[3]

    whole = pl.BlockSpec(memory_space=pltpu.VMEM)
    return call(
        kernel,
        (bf16(rows, depth),) * 3,
        mib=16,
        grid_spec=pltpu.PrefetchScalarGridSpec(
            num_scalar_prefetch=1,
            grid=(1,),
            in_specs=[whole] * 6,
            out_specs=(whole,) * 3,
            scratch_shapes=[pltpu.VMEM((RING, rows, depth), jnp.bfloat16)],
        ),
    )(here, pair, *weights)


def weight_chunk(here, r, routed_inputs, hidden, pairs, scaled, received=None):
    _, sources, _, capacity, model_width = routed_inputs.shape
    depth = model_width // RING
    width = hidden.shape[1]
    half = depth // 2
    groups = len(pairs)
    spans, at = [], 0
    for pair in pairs:
        spans.append(slice(at, at + pair.shape[0]))
        at += pair.shape[0]

    def kernel(here_ref, x_ref, hidden_ref, *refs):
        pair_refs, scaled_refs, refs = refs[:groups], refs[groups : 2 * groups], refs[2 * groups :]
        x, refs = refs[-1], refs[:-1]
        fill_rows(here_ref, x_ref, x)

        for i in range(6):
            if i < 4:
                lanes = slice((i // 2) * width, (i // 2 + 1) * width)
                columns = slice((i % 2) * half, (i % 2 + 1) * half)
                value = sum(
                    dot(x[spans[h], columns], pair_refs[h][:, lanes], 0, 0) for h in range(groups)
                )
                values = [(value, slice(0, half))]
            else:
                values = []
                for c in range(half // width):
                    first = (i - 4) * half + c * width
                    value = sum(
                        dot(
                            hidden_ref[spans[h]],
                            scaled_refs[h][0, :, first : first + width],
                            0,
                            0,
                        )
                        for h in range(groups)
                    )
                    values.append((value, slice(c * width, (c + 1) * width)))
            for value, place in values:
                source = pl.ds(i * half + place.start, place.stop - place.start)
                if r:
                    out_ref = refs[i // 3] if r == 2 else refs[0]
                    at = (i % 3 if r == 2 else i) * half + place.start
                    out_ref[pl.ds(at, place.stop - place.start)] = value.astype(jnp.bfloat16)
                    continue
                value += refs[0][source].astype(jnp.float32) + refs[1][source].astype(jnp.float32)
                if i < 4:
                    refs[2 + i // 2][pl.ds((i % 2) * half, half)] = value
                else:
                    first = (i - 4) * half + place.start
                    refs[4][:, first : first + width] = value

    whole = pl.BlockSpec(memory_space=pltpu.VMEM)
    chunks = [
        pl.BlockSpec((1, pair.shape[0], depth), lambda i, here: (r, 0, 0)) for pair in pairs
    ]
    if r == 0:
        outs = (f32(depth, width), f32(depth, width), f32(width, depth))
    elif r == 2:
        outs = (bf16(3 * half, width), bf16(3 * half, width))
    else:
        outs = (bf16(6 * half, width),)
    received = received or ()
    return call(
        kernel,
        outs,
        mib=18 if r == 0 else 12,
        grid_spec=pltpu.PrefetchScalarGridSpec(
            num_scalar_prefetch=1,
            grid=(1,),
            in_specs=[
                pl.BlockSpec(
                    (1, sources, 1, capacity, depth),
                    lambda i, here: (0, 0, 0, 0, (here[0] + r) % RING),
                ),
                whole,
            ]
            + [whole] * groups
            + chunks
            + [whole] * len(received),
            out_specs=(whole,) * len(outs),
            scratch_shapes=[pltpu.VMEM((sources * capacity, depth), jnp.bfloat16)],
        ),
    )(here, routed_inputs, hidden, *pairs, *scaled, *received)


def join(arrays):
    def kernel(*refs):
        at = 0
        for ref in refs[:-1]:
            refs[-1][pl.ds(at, ref.shape[0])] = ref[...]
            at += ref.shape[0]

    return call(kernel, bf16(sum(a.shape[0] for a in arrays), arrays[0].shape[1]))(*arrays)


def messages(own, other):
    count = len(SHIFTS)
    rows, columns = own.shape
    rows //= count

    def kernel(own_ref, other_ref, *out_refs):
        for j, out_ref in enumerate(out_refs):
            out_ref[:rows] = own_ref[j * rows : (j + 1) * rows]
            out_ref[rows:] = other_ref[j * rows : (j + 1) * rows]

    return call(kernel, (bf16(2 * rows, columns),) * count)(own, other)


def unpack_messages(blocks):
    rows, columns = blocks[0].shape
    rows //= 2

    def kernel(*refs):
        own_ref, other_ref = refs[-2:]
        for j, ref in enumerate(refs[:-2]):
            own_ref[pl.ds(j * rows, rows)] = ref[:rows]
            other_ref[pl.ds(j * rows, rows)] = ref[rows:]

    return call(kernel, (bf16(len(blocks) * rows, columns),) * 2)(*blocks)


def leaving_rows(own, from_prev, from_next, extra, count):
    rows, narrow = own.shape
    rows //= count

    def kernel(own_ref, prev_ref, next_ref, extra_ref, *out_refs):
        for j, out_ref in enumerate(out_refs):
            span = slice(j * rows, (j + 1) * rows)
            total = own_ref[span].astype(jnp.float32) + prev_ref[span].astype(jnp.float32)
            total += next_ref[span].astype(jnp.float32)
            out_ref[:, :narrow] = total.astype(jnp.bfloat16)
            out_ref[:, narrow:] = extra_ref[span]

    outs = (bf16(rows, narrow + LANES),) * count
    return call(kernel, outs)(own, from_prev, from_next, extra)


def token_rows(slot_index, back):
    tokens = slot_index.shape[0]
    rows, wide = back[0].shape
    narrow = wide - LANES

    def kernel(slot_ref, *refs):
        out_ref = refs[-1]
        total = jnp.zeros((tokens, narrow), jnp.float32)
        chosen = [jnp.zeros((tokens, LANES), jnp.float32)] * 2
        for h, back_ref in enumerate(refs[:-1]):
            slot = lax.broadcasted_iota(jnp.int32, (tokens, rows), 1) + h * rows
            picks = [
                jnp.where(slot_ref[:, k : k + 1] == slot, 1.0, 0.0).astype(jnp.bfloat16)
                for k in range(2)
            ]
            total += dot(picks[0] + picks[1], back_ref[:, :narrow])
            chosen = [c + dot(p, back_ref[:, narrow:]) for c, p in zip(chosen, picks)]
        out_ref[:, :narrow] = total.astype(jnp.bfloat16)
        lane = lax.broadcasted_iota(jnp.int32, (tokens, LANES), 1)
        tail = jnp.zeros((tokens, LANES), jnp.float32)
        for k in range(2):
            value = chosen[k][:, 0:1] + chosen[k][:, 1:2]
            high = value.astype(jnp.bfloat16).astype(jnp.float32)
            tail = jnp.where(lane == 2 * k, high, jnp.where(lane == 2 * k + 1, value - high, tail))
        out_ref[:, narrow:] = tail.astype(jnp.bfloat16)

    return call(kernel, bf16(tokens, wide))(slot_index, *back)


def finish_tokens(here, gate_probs, gathered):
    tokens, wide = gathered[0].shape
    narrow = wide - LANES

    def kernel(here_ref, probs_ref, *refs):
        out_ref, logit_ref = refs[RING:]
        total = jnp.zeros((tokens, LANES), jnp.float32)
        for q in range(RING):
            first = ((here_ref[0] + here_ref[1] + q) % RING) * narrow
            out_ref[:, pl.ds(pl.multiple_of(first, LANES), narrow)] = refs[q][:, :narrow]
            total += refs[q][:, narrow:].astype(jnp.float32)
        chosen = [
            (total[:, 2 * k : 2 * k + 1] + total[:, 2 * k + 1 : 2 * k + 2])
            .astype(jnp.bfloat16)
            .astype(jnp.float32)
            for k in range(2)
        ]
        both = chosen[0] + chosen[1]
        for k in range(2):
            logit_ref[:, k : k + 1] = chosen[k] - probs_ref[:, k : k + 1] * both

    whole = pl.BlockSpec(memory_space=pltpu.VMEM)
    return call(
        kernel,
        (bf16(tokens, RING * narrow), f32(tokens, 2)),
        grid_spec=pltpu.PrefetchScalarGridSpec(
            num_scalar_prefetch=1,
            grid=(1,),
            in_specs=[whole] * (RING + 1),
            out_specs=(whole,) * 2,
        ),
    )(here, gate_probs, *gathered)


def slots_of(routes, z, core, capacity, experts):
    tokens = routes.shape[0]
    hot = (routes[:, :, None] == jnp.arange(experts, dtype=jnp.int32)).astype(jnp.bfloat16)
    before = jnp.arange(tokens)[:, None] > jnp.arange(tokens)[None, :]
    earlier = dot(before.astype(jnp.bfloat16), hot[:, 0] + hot[:, 1])
    place = jnp.sum(earlier[:, None, :] * hot.astype(jnp.float32), axis=2).astype(jnp.int32)
    count = len(SHIFTS)
    distance = (routes // 2 - z + count) % count
    index = jnp.where(
        distance <= count // 2, jnp.maximum(2 * distance - 1, 0), 2 * (count - distance)
    )
    other = (routes % 2 != core).astype(jnp.int32)
    return (other * count + index) * capacity + place


def layer(out_grad, routes, chosen_logits, routed_inputs, w_gate, w_up, w_down):
    experts = lax.axis_size("ep")
    f, t = lax.axis_index("fsdp"), lax.axis_index("tp")
    z, core = lax.axis_index("ep") // 2, lax.axis_index("ep") % 2
    here = jnp.stack([f, t, z, core]).astype(jnp.int32)
    model_width = out_grad.shape[1]
    capacity = routed_inputs.shape[3]
    slots = experts * capacity
    narrow = model_width // RING
    width = w_gate.shape[2]
    block = 2 * capacity

    weights = ring_gather(pack(w_gate[0], w_up[0], w_down[0]), "fsdp")

    gate_probs = jax.nn.softmax(chosen_logits, axis=-1)
    slot_index = slots_of(routes, z, core, capacity, experts)
    piece = lax.dynamic_slice_in_dim(out_grad, ((f + t) % RING) * narrow, narrow, 1)
    weighted = gate_probs[:, :, None] * piece.astype(jnp.float32)[:, None, :]
    weighted = weighted.astype(jnp.bfloat16)

    def routed(first):
        slot = first + jnp.arange(slots // 2, dtype=jnp.int32)
        picks = (slot_index[:, :, None] == slot).astype(jnp.bfloat16)
        return lax.dot_general(
            picks, weighted, (((0, 1), (0, 1)), ((), ())), preferred_element_type=jnp.float32
        ).astype(jnp.bfloat16)

    own, other = routed(0), swap_cores(routed(slots // 2))
    sent = messages(own, other)
    arrived = [sent[0]] + [shift_z(sent[j], SHIFTS[j]) for j in range(1, len(SHIFTS))]
    gathered = [ring_gather(join([arrived[j] for j in group]), "tp") for group in GROUPS]

    hidden, silu, slope = activations(here, routed_inputs, weights, width)
    pairs, scaled, leaving = [], [], []
    for g, group in enumerate(GROUPS):
        pair, extra, top, bottom, by_r = pair_gradients(
            here, group[0] * block, gathered[g], weights, hidden, silu, slope
        )
        pairs.append(pair)
        scaled.append(by_r)
        own, following, prev = slot_gradients(here, pair, weights)
        received = ring_reduce(following, top, bottom, prev, "tp")
        leaving += leaving_rows(own, *received, extra, len(group))

    chunk = functools.partial(
        weight_chunk, here, routed_inputs=routed_inputs, hidden=hidden, pairs=pairs, scaled=scaled
    )
    received = ring_reduce(*chunk(1), *chunk(2), *chunk(3), "fsdp")
    grad_gate, grad_up, grad_down = chunk(0, received=received)

    returned = [leaving[0]] + [shift_z(leaving[j], -SHIFTS[j]) for j in range(1, len(SHIFTS))]
    own, other = unpack_messages(returned)
    mine = token_rows(slot_index, [own, swap_cores(other)])
    tokens_by_ring = [mine] + [shift(mine, "tp", -q) for q in range(1, RING)]
    input_grad, logit_grad = finish_tokens(here, gate_probs, tokens_by_ring)
    return input_grad, logit_grad, grad_gate[None], grad_up[None], grad_down[None]


def solution(mesh):
    return jax.shard_map(
        layer,
        mesh=mesh,
        in_specs=(
            P(("ep", "fsdp"), None),
            P(("ep", "fsdp"), None),
            P(("ep", "fsdp"), None),
            P("ep", None, "fsdp", None, None),
            P("ep", "fsdp", "tp"),
            P("ep", "fsdp", "tp"),
            P("ep", "tp", "fsdp"),
        ),
        out_specs=(
            P(("ep", "fsdp"), None),
            P(("ep", "fsdp"), None),
            P("ep", "fsdp", "tp"),
            P("ep", "fsdp", "tp"),
            P("ep", "tp", "fsdp"),
        ),
        check_vma=False,
    )
```

```python
import functools

import jax
import jax.numpy as jnp
from jax import lax
from jax.experimental import pallas as pl
from jax.experimental.pallas import tpu as pltpu
from jax.sharding import PartitionSpec as P


RING = 4
LANES = 128
MIB = 1 << 20


SHIFTS = (0, 1, -1, 2, -2, 3, -3, 4)
GROUPS = ((0, 1, 2, 3, 4), (5, 6, 7))


def shift(x, axis, step):
    n = lax.axis_size(axis)
    return lax.ppermute(x, axis, [(i, (i + step) % n) for i in range(n)])


def shift_z(x, step):
    n = lax.axis_size("ep")
    return lax.ppermute(x, "ep", [(i, (i + 2 * step) % n) for i in range(n)])


def swap_cores(x):
    return lax.ppermute(x, "ep", [(i, i ^ 1) for i in range(lax.axis_size("ep"))])


def ring_gather(block, axis):
    half = block.shape[0] // 2
    prev = shift(block, axis, 1)
    following = shift(block, axis, -1)
    far_top = shift(prev[:half], axis, 1)
    far_bottom = shift(following[half:], axis, -1)
    return block, following, far_top, far_bottom, prev


def ring_reduce(following, far_top, far_bottom, prev, axis):
    top = shift(far_top, axis, 1)
    bottom = shift(far_bottom, axis, -1)
    following = add_half(following, top, 0)
    prev = add_half(prev, bottom, 1)
    from_prev = shift(following, axis, 1)
    from_next = shift(prev, axis, -1)
    return from_prev, from_next


def call(kernel, out_shape, mib=8, **options):
    return pl.pallas_call(
        kernel,
        out_shape=out_shape,
        compiler_params=pltpu.CompilerParams(vmem_limit_bytes=mib * MIB),
        **options,
    )


def bf16(*shape):
    return jax.ShapeDtypeStruct(shape, jnp.bfloat16)


def f32(*shape):
    return jax.ShapeDtypeStruct(shape, jnp.float32)


def dot(left, right, left_dim=1, right_dim=0):
    return lax.dot_general(
        left, right, (((left_dim,), (right_dim,)), ((), ())), preferred_element_type=jnp.float32
    )


def add_half(whole, half, index):
    def kernel(whole_ref, half_ref, out_ref):
        total = whole_ref[...].astype(jnp.float32) + half_ref[...].astype(jnp.float32)
        out_ref[...] = total.astype(jnp.bfloat16)

    spec = pl.BlockSpec(half.shape, lambda i: (index, 0))
    return call(
        kernel,
        bf16(*whole.shape),
        grid=(1,),
        in_specs=[spec, pl.BlockSpec(half.shape, lambda i: (0, 0))],
        out_specs=spec,
        input_output_aliases={0: 0},
    )(whole, half)


def pack(w_gate, w_up, w_down):
    depth, width = w_gate.shape

    blocks = depth // width

    def kernel(gate_ref, up_ref, down_ref, out_ref, sems):
        pairs = [(gate_ref, 0, depth), (up_ref, depth, depth)]
        for c in range(blocks):
            lanes = down_ref.at[:, pl.ds(c * width, width)]
            pairs.append((lanes, 2 * depth + c * width, width))
        copies = [
            pltpu.make_async_copy(source, out_ref.at[pl.ds(first, count)], sems.at[i])
            for i, (source, first, count) in enumerate(pairs)
        ]
        for copy in copies:
            copy.start()
        for copy in copies:
            copy.wait()

    return call(
        kernel,
        bf16(3 * depth, width),
        in_specs=[pl.BlockSpec(memory_space=pltpu.HBM)] * 3,
        out_specs=pl.BlockSpec(memory_space=pltpu.VMEM),
        scratch_shapes=[pltpu.SemaphoreType.DMA((2 + blocks,))],
    )(w_gate, w_up, w_down)


def weight_parts(refs, r, depth):
    half = depth // 2
    if r == 2:
        top, bottom = refs[2], refs[3]
        return [(top, 0, depth)], [(top, depth, half), (bottom, 0, half)], [(bottom, half, depth)]
    ref = refs[(0, 1, None, 4)[r]]
    return tuple([(ref, i * depth, depth)] for i in range(3))


def fill_rows(here_ref, x_ref, rows_ref):
    capacity = x_ref.shape[3]
    z, core = here_ref[2], here_ref[3]
    count = len(SHIFTS)
    for j, step in enumerate(SHIFTS):
        for k in range(2):
            source = ((z - step + count) % count) * 2 + (core if k == 0 else 1 - core)
            rows_ref[pl.ds((2 * j + k) * capacity, capacity)] = x_ref[0, source, 0]


def activations(here, routed_inputs, weights, width):
    _, sources, _, capacity, model_width = routed_inputs.shape
    depth = model_width // RING
    slots = sources * capacity

    def kernel(here_ref, x_ref, w0, w1, w2, w3, w4, hidden_ref, silu_ref, slope_ref, x, gate, up):
        refs = (w0, w1, w2, w3, w4)
        step = pl.program_id(0)
        fill_rows(here_ref, x_ref, x)
        for r in range(RING):

            @pl.when(step == r)
            def _():
                gates, ups, _ = weight_parts(refs, r, depth)
                for pieces, total in ((gates, gate), (ups, up)):
                    at, value = 0, None
                    for ref, first, count in pieces:
                        term = dot(x[:, at : at + count], ref[pl.ds(first, count)])
                        value = term if value is None else value + term
                        at += count
                    total[...] = value if r == 0 else total[...] + value

        @pl.when(step == RING - 1)
        def _():
            gate_act, up_act = gate[...], up[...]
            sigmoid_gate = jax.nn.sigmoid(gate_act)
            silu_gate = gate_act * sigmoid_gate
            hidden_ref[...] = (silu_gate * up_act).astype(jnp.bfloat16)
            silu_ref[...] = silu_gate
            slope_ref[...] = up_act * sigmoid_gate * (1.0 + gate_act * (1.0 - sigmoid_gate))

    whole = pl.BlockSpec(memory_space=pltpu.VMEM)
    return call(
        kernel,
        (bf16(slots, width), f32(slots, width), f32(slots, width)),
        mib=16,
        grid_spec=pltpu.PrefetchScalarGridSpec(
            num_scalar_prefetch=1,
            grid=(RING,),
            in_specs=[
                pl.BlockSpec(
                    (1, sources, 1, capacity, depth),
                    lambda i, here: (0, 0, 0, 0, (here[0] + i) % RING),
                )
            ]
            + [whole] * 5,
            out_specs=(pl.BlockSpec((slots, width), lambda i, here: (0, 0)),) * 3,
            scratch_shapes=[pltpu.VMEM((slots, depth), jnp.bfloat16)]
            + [pltpu.VMEM((slots, width), jnp.float32)] * 2,
        ),
    )(here, routed_inputs, *weights)


def pair_gradients(here, scaled, weights, hidden, silu, slope):
    slots, width = hidden.shape
    depth = scaled[0][0].shape[1]
    blocks = depth // width
    spans, places, at = [], [], 0
    for group in scaled:
        rows = group[0].shape[0]
        spans.append((at, rows))
        for q, first, count in (
            (0, 0, rows),
            (1, 0, rows),
            (2, 0, rows // 2),
            (2, rows // 2, rows // 2),
            (3, 0, rows),
        ):
            places.append((q, at + first, count))
        at += rows

    def kernel(here_ref, *refs):
        scaled_refs, refs = refs[: len(places)], refs[len(places) :]
        weight_refs, (hidden_ref, silu_ref, slope_ref) = refs[:5], refs[5:8]
        pair_ref, extra_ref, by_r = refs[8:11]
        far_refs, sems = refs[11:-1], refs[-1]
        t = here_ref[1]
        copies = [
            pltpu.make_async_copy(
                scaled_refs[i], by_r.at[(t + q) % RING, pl.ds(first, count)], sems.at[i]
            )
            for i, (q, first, count) in enumerate(places)
        ]
        for copy in copies:
            copy.start()
        for copy in copies:
            copy.wait()
        hidden_grad = jnp.zeros((slots, width), jnp.float32)
        for r in range(RING):
            ((ref, first, _),) = weight_parts(weight_refs, r, depth)[2]
            for c in range(blocks):
                hidden_grad += dot(
                    by_r[r, :, c * width : (c + 1) * width],
                    ref[pl.ds(first + c * width, width)],
                    1,
                    1,
                )
        products = jnp.sum(
            hidden_grad * hidden_ref[...].astype(jnp.float32), axis=1, keepdims=True
        )
        high = products.astype(jnp.bfloat16).astype(jnp.float32)
        lane = lax.broadcasted_iota(jnp.int32, (slots, LANES), 1)
        extra = jnp.where(lane == 0, high, jnp.where(lane == 1, products - high, 0.0))
        extra_ref[...] = extra.astype(jnp.bfloat16)
        pair_ref[:, :width] = (hidden_grad * slope_ref[...]).astype(jnp.bfloat16)
        pair_ref[:, width:] = (hidden_grad * silu_ref[...]).astype(jnp.bfloat16)
        for r in range(RING):

            @pl.when((t + 2) % RING == r)
            def _():
                for columns, value in slot_part(pair_ref, weight_refs, r, depth):
                    for i, (start, rows) in enumerate(spans):
                        middle = start + rows // 2
                        far_refs[2 * i][:, columns] = value[start:middle]
                        far_refs[2 * i + 1][:, columns] = value[middle : start + rows]

    anywhere = pl.BlockSpec(memory_space=pl.ANY)
    whole = pl.BlockSpec(memory_space=pltpu.VMEM)
    outs = [bf16(slots, 2 * width), bf16(slots, LANES), bf16(RING, slots, depth)]
    outs += [bf16(rows // 2, depth) for _, rows in spans for _ in range(2)]
    pair, extra, by_r, *far = call(
        kernel,
        tuple(outs),
        mib=20,
        grid_spec=pltpu.PrefetchScalarGridSpec(
            num_scalar_prefetch=1,
            grid=(1,),
            in_specs=[anywhere] * len(places) + [whole] * 8,
            out_specs=(whole,) * len(outs),
            scratch_shapes=[pltpu.SemaphoreType.DMA((len(places),))],
        ),
    )(here, *[part for group in scaled for part in group], *weights, hidden, silu, slope)
    return pair, extra, by_r, [far[2 * i : 2 * i + 2] for i in range(len(spans))]


def slot_part(pair_ref, weight_refs, r, depth):
    half = depth // 2
    width = pair_ref.shape[1] // 2
    gates, ups, _ = weight_parts(weight_refs, r, depth)
    if len(ups) == 1:
        ups = [(ups[0][0], ups[0][1] + i * half, half) for i in range(2)]
    for i, (up_ref, up_first, _) in enumerate(ups):
        gate_ref, gate_first, _ = gates[0]
        value = dot(pair_ref[:, :width], gate_ref[pl.ds(gate_first + i * half, half)], 1, 1)
        value += dot(pair_ref[:, width:], up_ref[pl.ds(up_first, half)], 1, 1)
        yield slice(i * half, (i + 1) * half), value.astype(jnp.bfloat16)


def slot_gradients(here, pair, weights, groups):
    slots = pair.shape[0]
    depth = weights[0].shape[0] // 3
    spans, at = [], 0
    for rows in groups:
        spans.append(slice(at, at + rows))
        at += rows

    def kernel(here_ref, pair_ref, *refs):
        weight_refs, out_refs, parts = refs[:5], refs[5:-1], refs[-1]
        t = here_ref[1]
        for r in range(RING):
            q = (r - t + RING) % RING

            @pl.when(q != 2)
            def _():
                for columns, value in slot_part(pair_ref, weight_refs, r, depth):
                    parts[q, :, columns] = value

        for i, span in enumerate(spans):
            for j, q in enumerate((0, 1, 3)):
                out_refs[3 * i + j][...] = parts[q, span]

    whole = pl.BlockSpec(memory_space=pltpu.VMEM)
    outs = tuple(bf16(rows, depth) for rows in groups for _ in range(3))
    parts = call(
        kernel,
        outs,
        mib=16,
        grid_spec=pltpu.PrefetchScalarGridSpec(
            num_scalar_prefetch=1,
            grid=(1,),
            in_specs=[whole] * 6,
            out_specs=(whole,) * len(outs),
            scratch_shapes=[pltpu.VMEM((RING, slots, depth), jnp.bfloat16)],
        ),
    )(here, pair, *weights)
    return [parts[3 * i : 3 * i + 3] for i in range(len(groups))]


def weight_chunk(here, r, routed_inputs, hidden, pairs, scaled, received=None):
    _, sources, _, capacity, model_width = routed_inputs.shape
    depth = model_width // RING
    width = hidden.shape[1]
    half = depth // 2
    groups = len(pairs)
    spans, at = [], 0
    for pair in pairs:
        spans.append(slice(at, at + pair.shape[0]))
        at += pair.shape[0]

    def kernel(here_ref, x_ref, hidden_ref, *refs):
        pair_refs, scaled_refs, refs = refs[:groups], refs[groups : 2 * groups], refs[2 * groups :]
        x, refs = refs[-1], refs[:-1]
        fill_rows(here_ref, x_ref, x)

        for i in range(6):
            if i < 4:
                lanes = slice((i // 2) * width, (i // 2 + 1) * width)
                columns = slice((i % 2) * half, (i % 2 + 1) * half)
                value = sum(
                    dot(x[spans[h], columns], pair_refs[h][:, lanes], 0, 0) for h in range(groups)
                )
                values = [(value, slice(0, half))]
            else:
                values = []
                for c in range(half // width):
                    first = (i - 4) * half + c * width
                    value = sum(
                        dot(
                            hidden_ref[spans[h]],
                            scaled_refs[h][0, :, first : first + width],
                            0,
                            0,
                        )
                        for h in range(groups)
                    )
                    values.append((value, slice(c * width, (c + 1) * width)))
            for value, place in values:
                source = pl.ds(i * half + place.start, place.stop - place.start)
                if r:
                    out_ref = refs[i // 3] if r == 2 else refs[0]
                    at = (i % 3 if r == 2 else i) * half + place.start
                    out_ref[pl.ds(at, place.stop - place.start)] = value.astype(jnp.bfloat16)
                    continue
                value += refs[0][source].astype(jnp.float32) + refs[1][source].astype(jnp.float32)
                if i < 4:
                    refs[2 + i // 2][pl.ds((i % 2) * half, half)] = value
                else:
                    first = (i - 4) * half + place.start
                    refs[4][:, first : first + width] = value

    whole = pl.BlockSpec(memory_space=pltpu.VMEM)
    chunks = [
        pl.BlockSpec((1, pair.shape[0], depth), lambda i, here: (r, 0, 0)) for pair in pairs
    ]
    if r == 0:
        outs = (f32(depth, width), f32(depth, width), f32(width, depth))
    elif r == 2:
        outs = (bf16(3 * half, width), bf16(3 * half, width))
    else:
        outs = (bf16(6 * half, width),)
    received = received or ()
    return call(
        kernel,
        outs,
        mib=18 if r == 0 else 12,
        grid_spec=pltpu.PrefetchScalarGridSpec(
            num_scalar_prefetch=1,
            grid=(1,),
            in_specs=[
                pl.BlockSpec(
                    (1, sources, 1, capacity, depth),
                    lambda i, here: (0, 0, 0, 0, (here[0] + r) % RING),
                ),
                whole,
            ]
            + [whole] * groups
            + chunks
            + [whole] * len(received),
            out_specs=(whole,) * len(outs),
            scratch_shapes=[pltpu.VMEM((sources * capacity, depth), jnp.bfloat16)],
        ),
    )(here, routed_inputs, hidden, *pairs, *scaled, *received)


def join(arrays):
    def kernel(*refs):
        at = 0
        for ref in refs[:-1]:
            refs[-1][pl.ds(at, ref.shape[0])] = ref[...]
            at += ref.shape[0]

    return call(kernel, bf16(sum(a.shape[0] for a in arrays), arrays[0].shape[1]))(*arrays)


def messages(own, other):
    count = len(SHIFTS)
    rows, columns = own.shape
    rows //= count

    def kernel(own_ref, other_ref, *out_refs):
        for j, out_ref in enumerate(out_refs):
            out_ref[:rows] = own_ref[j * rows : (j + 1) * rows]
            out_ref[rows:] = other_ref[j * rows : (j + 1) * rows]

    return call(kernel, (bf16(2 * rows, columns),) * count)(own, other)


def unpack_messages(blocks):
    rows, columns = blocks[0].shape
    rows //= 2

    def kernel(*refs):
        own_ref, other_ref = refs[-2:]
        for j, ref in enumerate(refs[:-2]):
            own_ref[pl.ds(j * rows, rows)] = ref[:rows]
            other_ref[pl.ds(j * rows, rows)] = ref[rows:]

    return call(kernel, (bf16(len(blocks) * rows, columns),) * 2)(*blocks)


def leaving_rows(own, from_prev, from_next, extra, start, count):
    rows, narrow = own.shape
    rows //= count

    def kernel(own_ref, prev_ref, next_ref, extra_ref, *out_refs):
        for j, out_ref in enumerate(out_refs):
            span = slice(j * rows, (j + 1) * rows)
            total = own_ref[span].astype(jnp.float32) + prev_ref[span].astype(jnp.float32)
            total += next_ref[span].astype(jnp.float32)
            out_ref[:, :narrow] = total.astype(jnp.bfloat16)
            out_ref[:, narrow:] = extra_ref[start + j * rows : start + (j + 1) * rows]

    outs = (bf16(rows, narrow + LANES),) * count
    return call(kernel, outs)(own, from_prev, from_next, extra)


def token_rows(slot_index, back):
    tokens = slot_index.shape[0]
    rows, wide = back[0].shape
    narrow = wide - LANES

    def kernel(slot_ref, *refs):
        out_ref = refs[-1]
        total = jnp.zeros((tokens, narrow), jnp.float32)
        chosen = [jnp.zeros((tokens, LANES), jnp.float32)] * 2
        for h, back_ref in enumerate(refs[:-1]):
            slot = lax.broadcasted_iota(jnp.int32, (tokens, rows), 1) + h * rows
            picks = [
                jnp.where(slot_ref[:, k : k + 1] == slot, 1.0, 0.0).astype(jnp.bfloat16)
                for k in range(2)
            ]
            total += dot(picks[0] + picks[1], back_ref[:, :narrow])
            chosen = [c + dot(p, back_ref[:, narrow:]) for c, p in zip(chosen, picks)]
        out_ref[:, :narrow] = total.astype(jnp.bfloat16)
        lane = lax.broadcasted_iota(jnp.int32, (tokens, LANES), 1)
        tail = jnp.zeros((tokens, LANES), jnp.float32)
        for k in range(2):
            value = chosen[k][:, 0:1] + chosen[k][:, 1:2]
            high = value.astype(jnp.bfloat16).astype(jnp.float32)
            tail = jnp.where(lane == 2 * k, high, jnp.where(lane == 2 * k + 1, value - high, tail))
        out_ref[:, narrow:] = tail.astype(jnp.bfloat16)

    return call(kernel, bf16(tokens, wide))(slot_index, *back)


def finish_tokens(here, gate_probs, gathered):
    tokens, wide = gathered[0].shape
    narrow = wide - LANES

    def kernel(here_ref, probs_ref, *refs):
        out_ref, logit_ref = refs[RING:]
        total = jnp.zeros((tokens, LANES), jnp.float32)
        for q in range(RING):
            first = ((here_ref[0] + here_ref[1] + q) % RING) * narrow
            out_ref[:, pl.ds(pl.multiple_of(first, LANES), narrow)] = refs[q][:, :narrow]
            total += refs[q][:, narrow:].astype(jnp.float32)
        chosen = [
            (total[:, 2 * k : 2 * k + 1] + total[:, 2 * k + 1 : 2 * k + 2])
            .astype(jnp.bfloat16)
            .astype(jnp.float32)
            for k in range(2)
        ]
        both = chosen[0] + chosen[1]
        for k in range(2):
            logit_ref[:, k : k + 1] = chosen[k] - probs_ref[:, k : k + 1] * both

    whole = pl.BlockSpec(memory_space=pltpu.VMEM)
    return call(
        kernel,
        (bf16(tokens, RING * narrow), f32(tokens, 2)),
        grid_spec=pltpu.PrefetchScalarGridSpec(
            num_scalar_prefetch=1,
            grid=(1,),
            in_specs=[whole] * (RING + 1),
            out_specs=(whole,) * 2,
        ),
    )(here, gate_probs, *gathered)


def slots_of(routes, z, core, capacity, experts):
    tokens = routes.shape[0]
    hot = (routes[:, :, None] == jnp.arange(experts, dtype=jnp.int32)).astype(jnp.bfloat16)
    before = jnp.arange(tokens)[:, None] > jnp.arange(tokens)[None, :]
    earlier = dot(before.astype(jnp.bfloat16), hot[:, 0] + hot[:, 1])
    place = jnp.sum(earlier[:, None, :] * hot.astype(jnp.float32), axis=2).astype(jnp.int32)
    count = len(SHIFTS)
    distance = (routes // 2 - z + count) % count
    index = jnp.where(
        distance <= count // 2, jnp.maximum(2 * distance - 1, 0), 2 * (count - distance)
    )
    other = (routes % 2 != core).astype(jnp.int32)
    return (other * count + index) * capacity + place


def layer(out_grad, routes, chosen_logits, routed_inputs, w_gate, w_up, w_down):
    experts = lax.axis_size("ep")
    f, t = lax.axis_index("fsdp"), lax.axis_index("tp")
    z, core = lax.axis_index("ep") // 2, lax.axis_index("ep") % 2
    here = jnp.stack([f, t, z, core]).astype(jnp.int32)
    model_width = out_grad.shape[1]
    capacity = routed_inputs.shape[3]
    slots = experts * capacity
    narrow = model_width // RING
    width = w_gate.shape[2]
    block = 2 * capacity

    weights = ring_gather(pack(w_gate[0], w_up[0], w_down[0]), "fsdp")

    gate_probs = jax.nn.softmax(chosen_logits, axis=-1)
    slot_index = slots_of(routes, z, core, capacity, experts)
    piece = lax.dynamic_slice_in_dim(out_grad, ((f + t) % RING) * narrow, narrow, 1)
    weighted = gate_probs[:, :, None] * piece.astype(jnp.float32)[:, None, :]
    weighted = weighted.astype(jnp.bfloat16)

    def routed(first):
        slot = first + jnp.arange(slots // 2, dtype=jnp.int32)
        picks = (slot_index[:, :, None] == slot).astype(jnp.bfloat16)
        return lax.dot_general(
            picks, weighted, (((0, 1), (0, 1)), ((), ())), preferred_element_type=jnp.float32
        ).astype(jnp.bfloat16)

    own, other = routed(0), swap_cores(routed(slots // 2))
    sent = messages(own, other)
    arrived = [sent[0]] + [shift_z(sent[j], SHIFTS[j]) for j in range(1, len(SHIFTS))]
    gathered = [ring_gather(join([arrived[j] for j in group]), "tp") for group in GROUPS]

    hidden, silu, slope = activations(here, routed_inputs, weights, width)
    pair, extra, scaled, far = pair_gradients(here, gathered, weights, hidden, silu, slope)
    parts = slot_gradients(here, pair, weights, [len(group) * block for group in GROUPS])
    leaving = []
    for g, group in enumerate(GROUPS):
        own, following, prev = parts[g]
        received = ring_reduce(following, *far[g], prev, "tp")
        leaving += leaving_rows(own, *received, extra, group[0] * block, len(group))

    chunk = functools.partial(
        weight_chunk, here, routed_inputs=routed_inputs, hidden=hidden, pairs=[pair], scaled=[scaled]
    )
    received = ring_reduce(*chunk(1), *chunk(2), *chunk(3), "fsdp")
    grad_gate, grad_up, grad_down = chunk(0, received=received)

    returned = [leaving[0]] + [shift_z(leaving[j], -SHIFTS[j]) for j in range(1, len(SHIFTS))]
    own, other = unpack_messages(returned)
    mine = token_rows(slot_index, [own, swap_cores(other)])
    tokens_by_ring = [mine] + [shift(mine, "tp", -q) for q in range(1, RING)]
    input_grad, logit_grad = finish_tokens(here, gate_probs, tokens_by_ring)
    return input_grad, logit_grad, grad_gate[None], grad_up[None], grad_down[None]


def solution(mesh):
    return jax.shard_map(
        layer,
        mesh=mesh,
        in_specs=(
            P(("ep", "fsdp"), None),
            P(("ep", "fsdp"), None),
            P(("ep", "fsdp"), None),
            P("ep", None, "fsdp", None, None),
            P("ep", "fsdp", "tp"),
            P("ep", "fsdp", "tp"),
            P("ep", "tp", "fsdp"),
        ),
        out_specs=(
            P(("ep", "fsdp"), None),
            P(("ep", "fsdp"), None),
            P("ep", "fsdp", "tp"),
            P("ep", "fsdp", "tp"),
            P("ep", "tp", "fsdp"),
        ),
        check_vma=False,
    )
```

```python
import functools

import jax
import jax.numpy as jnp
from jax import lax
from jax.experimental import pallas as pl
from jax.experimental.pallas import tpu as pltpu
from jax.sharding import PartitionSpec as P


RING = 4
LANES = 128
MIB = 1 << 20


SHIFTS = (0, 1, -1, 2, -2, 3, -3, 4)
GROUPS = ((0, 1, 2, 3, 4), (5, 6, 7))


def shift(x, axis, step):
    n = lax.axis_size(axis)
    return lax.ppermute(x, axis, [(i, (i + step) % n) for i in range(n)])


def shift_z(x, step):
    n = lax.axis_size("ep")
    return lax.ppermute(x, "ep", [(i, (i + 2 * step) % n) for i in range(n)])


def swap_cores(x):
    return lax.ppermute(x, "ep", [(i, i ^ 1) for i in range(lax.axis_size("ep"))])


def ring_gather(block, axis):
    half = block.shape[0] // 2
    prev = shift(block, axis, 1)
    following = shift(block, axis, -1)
    far_top = shift(prev[:half], axis, 1)
    far_bottom = shift(following[half:], axis, -1)
    return block, following, far_top, far_bottom, prev


def far_halves(top, bottom, axis):
    return shift(top, axis, 1), shift(bottom, axis, -1)


def neighbours(following, prev, axis):
    return shift(following, axis, 1), shift(prev, axis, -1)


def call(kernel, out_shape, mib=8, **options):
    return pl.pallas_call(
        kernel,
        out_shape=out_shape,
        compiler_params=pltpu.CompilerParams(vmem_limit_bytes=mib * MIB),
        **options,
    )


def bf16(*shape):
    return jax.ShapeDtypeStruct(shape, jnp.bfloat16)


def f32(*shape):
    return jax.ShapeDtypeStruct(shape, jnp.float32)


def dot(left, right, left_dim=1, right_dim=0):
    return lax.dot_general(
        left, right, (((left_dim,), (right_dim,)), ((), ())), preferred_element_type=jnp.float32
    )


def add_half(whole, half, index, start=0):
    rows, columns = whole.shape
    rows //= 2
    blocks = max(rows // 512, 1)
    rows //= blocks

    def kernel(whole_ref, half_ref, out_ref):
        first = pl.multiple_of(start + pl.program_id(0) * rows, 16)
        total = whole_ref[...].astype(jnp.float32)
        total += half_ref[pl.ds(first, rows)].astype(jnp.float32)
        out_ref[...] = total.astype(jnp.bfloat16)

    spec = pl.BlockSpec((rows, columns), lambda i: (index * blocks + i, 0))
    return call(
        kernel,
        bf16(*whole.shape),
        grid=(blocks,),
        in_specs=[spec, pl.BlockSpec(memory_space=pltpu.VMEM)],
        out_specs=spec,
        input_output_aliases={0: 0},
    )(whole, half)


def pack(w_gate, w_up, w_down):
    depth, width = w_gate.shape

    def kernel(gate_ref, up_ref, down_ref, out_ref):
        out_ref[:depth] = gate_ref[...]
        out_ref[depth : 2 * depth] = up_ref[...]
        out_ref[2 * depth :] = down_ref[...].T

    return call(kernel, bf16(3 * depth, width))(
        *(pltpu.with_memory_space_constraint(w, pltpu.HBM) for w in (w_gate, w_up, w_down))
    )


def weight_parts(refs, r, depth):
    half = depth // 2
    if r == 2:
        top, bottom = refs[2], refs[3]
        return [(top, 0, depth)], [(top, depth, half), (bottom, 0, half)], [(bottom, half, depth)]
    ref = refs[(0, 1, None, 4)[r]]
    return tuple([(ref, i * depth, depth)] for i in range(3))


def start_select(refs, r, out_ref, sem, depth):
    for k in range(RING):

        @pl.when(r == k)
        def _():
            if k == 2:
                rows = 3 * depth // 2
                pieces = [(refs[2], 0, rows), (refs[3], rows, 2 * depth - rows)]
            else:
                pieces = [(refs[(0, 1, None, 4)[k]], 0, 2 * depth)]
            for ref, first, count in pieces:
                source = ref.at[pl.ds(0, count)]
                pltpu.make_async_copy(source, out_ref.at[pl.ds(first, count)], sem).start()


def wait_select(out_ref, sem):
    pltpu.make_async_copy(out_ref, out_ref, sem).wait()


def fill_rows(here_ref, x_ref, rows_ref):
    capacity = x_ref.shape[3]
    z, core = here_ref[2], here_ref[3]
    count = len(SHIFTS)
    for j, step in enumerate(SHIFTS):
        for k in range(2):
            source = ((z - step + count) % count) * 2 + (core if k == 0 else 1 - core)
            rows_ref[pl.ds((2 * j + k) * capacity, capacity)] = x_ref[0, source, 0]


def activations(here, routed_inputs, weights, width):
    _, sources, _, capacity, model_width = routed_inputs.shape
    depth = model_width // RING
    slots = sources * capacity

    def kernel(here_ref, x_ref, w0, w1, w2, w3, w4, hidden_ref, silu_ref, slope_ref, x, gate, up):
        refs = (w0, w1, w2, w3, w4)
        step = pl.program_id(0)
        fill_rows(here_ref, x_ref, x)
        for r in range(RING):

            @pl.when(step == r)
            def _():
                gates, ups, _ = weight_parts(refs, r, depth)
                for pieces, total in ((gates, gate), (ups, up)):
                    at, value = 0, None
                    for ref, first, count in pieces:
                        term = dot(x[:, at : at + count], ref[pl.ds(first, count)])
                        value = term if value is None else value + term
                        at += count
                    total[...] = value if r == 0 else total[...] + value

        @pl.when(step == RING - 1)
        def _():
            gate_act, up_act = gate[...], up[...]
            sigmoid_gate = jax.nn.sigmoid(gate_act)
            silu_gate = gate_act * sigmoid_gate
            hidden_ref[...] = (silu_gate * up_act).astype(jnp.bfloat16)
            silu_ref[...] = silu_gate
            slope_ref[...] = up_act * sigmoid_gate * (1.0 + gate_act * (1.0 - sigmoid_gate))

    whole = pl.BlockSpec(memory_space=pltpu.VMEM)
    return call(
        kernel,
        (bf16(slots, width), f32(slots, width), f32(slots, width)),
        mib=16,
        grid_spec=pltpu.PrefetchScalarGridSpec(
            num_scalar_prefetch=1,
            grid=(RING,),
            in_specs=[
                pl.BlockSpec(
                    (1, sources, 1, capacity, depth),
                    lambda i, here: (0, 0, 0, 0, (here[0] + i) % RING),
                )
            ]
            + [whole] * 5,
            out_specs=(pl.BlockSpec((slots, width), lambda i, here: (0, 0)),) * 3,
            scratch_shapes=[pltpu.VMEM((slots, depth), jnp.bfloat16)]
            + [pltpu.VMEM((slots, width), jnp.float32)] * 2,
        ),
    )(here, routed_inputs, *weights)


def pair_gradients(here, scaled, weights, hidden, silu, slope):
    slots, width = hidden.shape
    depth = scaled[0][0].shape[1]
    spans, places, at = [], [], 0
    for group in scaled:
        rows = group[0].shape[0]
        spans.append((at, rows))
        for q, first, count in (
            (0, 0, rows),
            (1, 0, rows),
            (2, 0, rows // 2),
            (2, rows // 2, rows // 2),
            (3, 0, rows),
        ):
            places.append((q, at + first, count))
        at += rows

    def kernel(here_ref, *refs):
        scaled_refs, refs = refs[: len(places)], refs[len(places) :]
        weight_refs, (hidden_ref, silu_ref, slope_ref) = refs[:5], refs[5:8]
        pair_ref, extra_ref, by_r = refs[8:11]
        top_ref, bottom_ref, sems, chosen, chosen_sem = refs[11:]
        t = here_ref[1]
        copies = [
            pltpu.make_async_copy(
                scaled_refs[i],
                by_r.at[(t + q) % RING, pl.ds(first, count)],
                sems.at[(t + q) % RING],
            )
            for i, (q, first, count) in enumerate(places)
        ]
        for copy in copies:
            copy.start()
        start_select(weight_refs, (t + 2) % RING, chosen, chosen_sem, depth)
        hidden_grad = jnp.zeros((slots, width), jnp.float32)
        for r in range(RING):
            pltpu.make_async_copy(by_r.at[r], by_r.at[r], sems.at[r]).wait()
            ((ref, first, count),) = weight_parts(weight_refs, r, depth)[2]
            hidden_grad += dot(by_r[r], ref[pl.ds(first, count)])
        products = jnp.sum(
            hidden_grad * hidden_ref[...].astype(jnp.float32), axis=1, keepdims=True
        )
        high = products.astype(jnp.bfloat16).astype(jnp.float32)
        lane = lax.broadcasted_iota(jnp.int32, (slots, LANES), 1)
        extra = jnp.where(lane == 0, high, jnp.where(lane == 1, products - high, 0.0))
        extra_ref[...] = extra.astype(jnp.bfloat16)
        pair_ref[:, :width] = (hidden_grad * slope_ref[...]).astype(jnp.bfloat16)
        pair_ref[:, width:] = (hidden_grad * silu_ref[...]).astype(jnp.bfloat16)
        wait_select(chosen, chosen_sem)
        for columns, value in slot_part(pair_ref, chosen, depth):
            for start, rows in spans:
                middle = start + rows // 2
                half = pl.ds(start // 2, rows // 2)
                top_ref[half, columns] = value[start:middle]
                bottom_ref[half, columns] = value[middle : start + rows]

    anywhere = pl.BlockSpec(memory_space=pl.ANY)
    whole = pl.BlockSpec(memory_space=pltpu.VMEM)
    outs = [bf16(slots, 2 * width), bf16(slots, LANES), bf16(RING, slots, depth)]
    outs += [bf16(slots // 2, depth)] * 2
    return call(
        kernel,
        tuple(outs),
        mib=22,
        grid_spec=pltpu.PrefetchScalarGridSpec(
            num_scalar_prefetch=1,
            grid=(1,),
            in_specs=[anywhere] * len(places) + [whole] * 8,
            out_specs=(whole,) * len(outs),
            scratch_shapes=[
                pltpu.SemaphoreType.DMA((RING,)),
                pltpu.VMEM((2 * depth, width), jnp.bfloat16),
                pltpu.SemaphoreType.DMA,
            ],
        ),
    )(here, *[part for group in scaled for part in group], *weights, hidden, silu, slope)


def slot_part(pair_ref, weights, depth):
    half = depth // 2
    width = pair_ref.shape[1] // 2
    for i in range(2):
        value = dot(pair_ref[:, :width], weights[pl.ds(i * half, half)], 1, 1)
        value += dot(pair_ref[:, width:], weights[pl.ds(depth + i * half, half)], 1, 1)
        yield slice(i * half, (i + 1) * half), value.astype(jnp.bfloat16)


def slot_gradients(here, pair, weights, groups):
    slots = pair.shape[0]
    width = pair.shape[1] // 2
    depth = weights[0].shape[0] // 3
    spans, at = [], 0
    for rows in groups:
        spans.append(slice(at, at + rows))
        at += rows

    def kernel(here_ref, pair_ref, *refs):
        weight_refs, out_refs, (parts, chosen, sems) = refs[:5], refs[5:-3], refs[-3:]
        t, step = here_ref[1], pl.program_id(0)

        def start(i):
            q = i + i // 2
            start_select(weight_refs, (t + q) % RING, chosen.at[i % 2], sems.at[i % 2], depth)

        @pl.when(step == 0)
        def _():
            start(0)
            start(1)

        now = step % 2
        wait_select(chosen.at[now], sems.at[now])
        for columns, value in slot_part(pair_ref, chosen.at[now], depth):
            parts[step, :, columns] = value

        @pl.when(step == 0)
        def _():
            start(2)

        @pl.when(step == 2)
        def _():
            for i, span in enumerate(spans):
                for j in range(3):
                    out_refs[3 * i + j][...] = parts[j, span]

    whole = pl.BlockSpec(memory_space=pltpu.VMEM)
    outs = tuple(bf16(rows, depth) for rows in groups for _ in range(3))
    parts = call(
        kernel,
        outs,
        mib=17,
        grid_spec=pltpu.PrefetchScalarGridSpec(
            num_scalar_prefetch=1,
            grid=(3,),
            in_specs=[whole] * 6,
            out_specs=(whole,) * len(outs),
            scratch_shapes=[
                pltpu.VMEM((3, slots, depth), jnp.bfloat16),
                pltpu.VMEM((2, 2 * depth, width), jnp.bfloat16),
                pltpu.SemaphoreType.DMA((2,)),
            ],
        ),
    )(here, pair, *weights)
    return [parts[3 * i : 3 * i + 3] for i in range(len(groups))]


def weight_chunk(here, r, routed_inputs, hidden, pairs, scaled, received=None):
    _, sources, _, capacity, model_width = routed_inputs.shape
    depth = model_width // RING
    width = hidden.shape[1]
    half = depth // 2
    groups = len(pairs)
    spans, at = [], 0
    for pair in pairs:
        spans.append(slice(at, at + pair.shape[0]))
        at += pair.shape[0]

    def kernel(here_ref, x_ref, hidden_ref, *refs):
        pair_refs, scaled_refs, refs = refs[:groups], refs[groups : 2 * groups], refs[2 * groups :]
        x, refs = refs[-1], refs[:-1]
        fill_rows(here_ref, x_ref, x)

        for i in range(6):
            if i < 4:
                lanes = slice((i // 2) * width, (i // 2 + 1) * width)
                columns = slice((i % 2) * half, (i % 2 + 1) * half)
                value = sum(
                    dot(x[spans[h], columns], pair_refs[h][:, lanes], 0, 0) for h in range(groups)
                )
                values = [(value, slice(0, half))]
            else:
                values = []
                for c in range(half // width):
                    first = (i - 4) * half + c * width
                    value = sum(
                        dot(
                            hidden_ref[spans[h]],
                            scaled_refs[h][0, :, first : first + width],
                            0,
                            0,
                        )
                        for h in range(groups)
                    )
                    values.append((value, slice(c * width, (c + 1) * width)))
            for value, place in values:
                source = pl.ds(i * half + place.start, place.stop - place.start)
                if r:
                    out_ref = refs[i // 3] if r == 2 else refs[0]
                    at = (i % 3 if r == 2 else i) * half + place.start
                    out_ref[pl.ds(at, place.stop - place.start)] = value.astype(jnp.bfloat16)
                    continue
                value += refs[0][source].astype(jnp.float32) + refs[1][source].astype(jnp.float32)
                if i < 4:
                    refs[2 + i // 2][pl.ds((i % 2) * half, half)] = value
                else:
                    first = (i - 4) * half + place.start
                    refs[4][:, first : first + width] = value

    whole = pl.BlockSpec(memory_space=pltpu.VMEM)
    chunks = [
        pl.BlockSpec((1, pair.shape[0], depth), lambda i, here: (r, 0, 0)) for pair in pairs
    ]
    if r == 0:
        outs = (f32(depth, width), f32(depth, width), f32(width, depth))
    elif r == 2:
        outs = (bf16(3 * half, width), bf16(3 * half, width))
    else:
        outs = (bf16(6 * half, width),)
    received = received or ()
    return call(
        kernel,
        outs,
        mib=18 if r == 0 else 12,
        grid_spec=pltpu.PrefetchScalarGridSpec(
            num_scalar_prefetch=1,
            grid=(1,),
            in_specs=[
                pl.BlockSpec(
                    (1, sources, 1, capacity, depth),
                    lambda i, here: (0, 0, 0, 0, (here[0] + r) % RING),
                ),
                whole,
            ]
            + [whole] * groups
            + chunks
            + [whole] * len(received),
            out_specs=(whole,) * len(outs),
            scratch_shapes=[pltpu.VMEM((sources * capacity, depth), jnp.bfloat16)],
        ),
    )(here, routed_inputs, hidden, *pairs, *scaled, *received)


def join(arrays):
    def kernel(*refs):
        at = 0
        for ref in refs[:-1]:
            refs[-1][pl.ds(at, ref.shape[0])] = ref[...]
            at += ref.shape[0]

    return call(kernel, bf16(sum(a.shape[0] for a in arrays), arrays[0].shape[1]))(*arrays)


def messages(own, other):
    count = len(SHIFTS)
    rows, columns = own.shape
    rows //= count

    def kernel(own_ref, other_ref, *out_refs):
        for j, out_ref in enumerate(out_refs):
            out_ref[:rows] = own_ref[j * rows : (j + 1) * rows]
            out_ref[rows:] = other_ref[j * rows : (j + 1) * rows]

    return call(kernel, (bf16(2 * rows, columns),) * count)(own, other)


def unpack_messages(blocks):
    rows, columns = blocks[0].shape
    rows //= 2

    def kernel(*refs):
        own_ref, other_ref = refs[-2:]
        for j, ref in enumerate(refs[:-2]):
            own_ref[pl.ds(j * rows, rows)] = ref[:rows]
            other_ref[pl.ds(j * rows, rows)] = ref[rows:]

    return call(kernel, (bf16(len(blocks) * rows, columns),) * 2)(*blocks)


def leaving_rows(own, from_prev, from_next, extra, start, count):
    rows, narrow = own.shape
    rows //= count

    def kernel(own_ref, prev_ref, next_ref, extra_ref, *out_refs):
        for j, out_ref in enumerate(out_refs):
            span = slice(j * rows, (j + 1) * rows)
            total = own_ref[span].astype(jnp.float32) + prev_ref[span].astype(jnp.float32)
            total += next_ref[span].astype(jnp.float32)
            out_ref[:, :narrow] = total.astype(jnp.bfloat16)
            out_ref[:, narrow:] = extra_ref[start + j * rows : start + (j + 1) * rows]

    outs = (bf16(rows, narrow + LANES),) * count
    return call(kernel, outs)(own, from_prev, from_next, extra)


def token_rows(slot_index, back):
    tokens = slot_index.shape[0]
    rows, wide = back[0].shape
    narrow = wide - LANES

    def kernel(slot_ref, *refs):
        out_ref = refs[-1]
        total = jnp.zeros((tokens, narrow), jnp.float32)
        chosen = [jnp.zeros((tokens, LANES), jnp.float32)] * 2
        for h, back_ref in enumerate(refs[:-1]):
            slot = lax.broadcasted_iota(jnp.int32, (tokens, rows), 1) + h * rows
            picks = [
                jnp.where(slot_ref[:, k : k + 1] == slot, 1.0, 0.0).astype(jnp.bfloat16)
                for k in range(2)
            ]
            total += dot(picks[0] + picks[1], back_ref[:, :narrow])
            chosen = [c + dot(p, back_ref[:, narrow:]) for c, p in zip(chosen, picks)]
        out_ref[:, :narrow] = total.astype(jnp.bfloat16)
        lane = lax.broadcasted_iota(jnp.int32, (tokens, LANES), 1)
        tail = jnp.zeros((tokens, LANES), jnp.float32)
        for k in range(2):
            value = chosen[k][:, 0:1] + chosen[k][:, 1:2]
            high = value.astype(jnp.bfloat16).astype(jnp.float32)
            tail = jnp.where(lane == 2 * k, high, jnp.where(lane == 2 * k + 1, value - high, tail))
        out_ref[:, narrow:] = tail.astype(jnp.bfloat16)

    return call(kernel, bf16(tokens, wide))(slot_index, *back)


def finish_tokens(here, gate_probs, gathered):
    tokens, wide = gathered[0].shape
    narrow = wide - LANES

    def kernel(here_ref, probs_ref, *refs):
        out_ref, logit_ref = refs[RING:]
        total = jnp.zeros((tokens, LANES), jnp.float32)
        for q in range(RING):
            first = ((here_ref[0] + here_ref[1] + q) % RING) * narrow
            out_ref[:, pl.ds(pl.multiple_of(first, LANES), narrow)] = refs[q][:, :narrow]
            total += refs[q][:, narrow:].astype(jnp.float32)
        chosen = [
            (total[:, 2 * k : 2 * k + 1] + total[:, 2 * k + 1 : 2 * k + 2])
            .astype(jnp.bfloat16)
            .astype(jnp.float32)
            for k in range(2)
        ]
        both = chosen[0] + chosen[1]
        for k in range(2):
            logit_ref[:, k : k + 1] = chosen[k] - probs_ref[:, k : k + 1] * both

    whole = pl.BlockSpec(memory_space=pltpu.VMEM)
    return call(
        kernel,
        (bf16(tokens, RING * narrow), f32(tokens, 2)),
        grid_spec=pltpu.PrefetchScalarGridSpec(
            num_scalar_prefetch=1,
            grid=(1,),
            in_specs=[whole] * (RING + 1),
            out_specs=(whole,) * 2,
        ),
    )(here, gate_probs, *gathered)


def slots_of(routes, z, core, capacity, experts):
    tokens = routes.shape[0]
    hot = (routes[:, :, None] == jnp.arange(experts, dtype=jnp.int32)).astype(jnp.bfloat16)
    before = jnp.arange(tokens)[:, None] > jnp.arange(tokens)[None, :]
    earlier = dot(before.astype(jnp.bfloat16), hot[:, 0] + hot[:, 1])
    place = jnp.sum(earlier[:, None, :] * hot.astype(jnp.float32), axis=2).astype(jnp.int32)
    count = len(SHIFTS)
    distance = (routes // 2 - z + count) % count
    index = jnp.where(
        distance <= count // 2, jnp.maximum(2 * distance - 1, 0), 2 * (count - distance)
    )
    other = (routes % 2 != core).astype(jnp.int32)
    return (other * count + index) * capacity + place


def layer(out_grad, routes, chosen_logits, routed_inputs, w_gate, w_up, w_down):
    experts = lax.axis_size("ep")
    f, t = lax.axis_index("fsdp"), lax.axis_index("tp")
    z, core = lax.axis_index("ep") // 2, lax.axis_index("ep") % 2
    here = jnp.stack([f, t, z, core]).astype(jnp.int32)
    model_width = out_grad.shape[1]
    capacity = routed_inputs.shape[3]
    slots = experts * capacity
    narrow = model_width // RING
    width = w_gate.shape[2]
    block = 2 * capacity

    weights = ring_gather(pack(w_gate[0], w_up[0], w_down[0]), "fsdp")

    gate_probs = jax.nn.softmax(chosen_logits, axis=-1)
    slot_index = slots_of(routes, z, core, capacity, experts)
    piece = lax.dynamic_slice_in_dim(out_grad, ((f + t) % RING) * narrow, narrow, 1)
    weighted = gate_probs[:, :, None] * piece.astype(jnp.float32)[:, None, :]
    weighted = weighted.astype(jnp.bfloat16)

    def routed(first):
        slot = first + jnp.arange(slots // 2, dtype=jnp.int32)
        picks = (slot_index[:, :, None] == slot).astype(jnp.bfloat16)
        return lax.dot_general(
            picks, weighted, (((0, 1), (0, 1)), ((), ())), preferred_element_type=jnp.float32
        ).astype(jnp.bfloat16)

    own, other = routed(0), swap_cores(routed(slots // 2))
    sent = messages(own, other)
    arrived = [sent[0]] + [shift_z(sent[j], SHIFTS[j]) for j in range(1, len(SHIFTS))]
    gathered = [ring_gather(join([arrived[j] for j in group]), "tp") for group in GROUPS]

    hidden, silu, slope = activations(here, routed_inputs, weights, width)
    pair, extra, scaled, *far = pair_gradients(here, gathered, weights, hidden, silu, slope)
    far = far_halves(*far, "tp")
    parts = slot_gradients(here, pair, weights, [len(group) * block for group in GROUPS])
    leaving = []
    for g, group in enumerate(GROUPS):
        own, following, prev = parts[g]
        start = group[0] * block
        following = add_half(following, far[0], 0, start // 2)
        prev = add_half(prev, far[1], 1, start // 2)
        received = neighbours(following, prev, "tp")
        leaving += leaving_rows(own, *received, extra, start, len(group))

    chunk = functools.partial(
        weight_chunk, here, routed_inputs=routed_inputs, hidden=hidden, pairs=[pair], scaled=[scaled]
    )
    far = far_halves(*chunk(2), "fsdp")
    received = neighbours(add_half(*chunk(1), far[0], 0), add_half(*chunk(3), far[1], 1), "fsdp")
    grad_gate, grad_up, grad_down = chunk(0, received=received)

    returned = [leaving[0]] + [shift_z(leaving[j], -SHIFTS[j]) for j in range(1, len(SHIFTS))]
    own, other = unpack_messages(returned)
    mine = token_rows(slot_index, [own, swap_cores(other)])
    tokens_by_ring = [mine] + [shift(mine, "tp", -q) for q in range(1, RING)]
    input_grad, logit_grad = finish_tokens(here, gate_probs, tokens_by_ring)
    return input_grad, logit_grad, grad_gate[None], grad_up[None], grad_down[None]


def solution(mesh):
    return jax.shard_map(
        layer,
        mesh=mesh,
        in_specs=(
            P(("ep", "fsdp"), None),
            P(("ep", "fsdp"), None),
            P(("ep", "fsdp"), None),
            P("ep", None, "fsdp", None, None),
            P("ep", "fsdp", "tp"),
            P("ep", "fsdp", "tp"),
            P("ep", "tp", "fsdp"),
        ),
        out_specs=(
            P(("ep", "fsdp"), None),
            P(("ep", "fsdp"), None),
            P("ep", "fsdp", "tp"),
            P("ep", "fsdp", "tp"),
            P("ep", "tp", "fsdp"),
        ),
        check_vma=False,
    )
```

```python
import functools

import jax
import jax.numpy as jnp
from jax import lax
from jax.experimental import pallas as pl
from jax.experimental.pallas import tpu as pltpu
from jax.sharding import PartitionSpec as P


RING = 4
LANES = 128
MIB = 1 << 20


SHIFTS = (0, 1, -1, 2, -2, 3, -3, 4)
GROUPS = ((0, 1, 2, 3, 4), (5, 6, 7))


def shift(x, axis, step):
    n = lax.axis_size(axis)
    return lax.ppermute(x, axis, [(i, (i + step) % n) for i in range(n)])


def shift_z(x, step):
    n = lax.axis_size("ep")
    return lax.ppermute(x, "ep", [(i, (i + 2 * step) % n) for i in range(n)])


def swap_cores(x):
    return lax.ppermute(x, "ep", [(i, i ^ 1) for i in range(lax.axis_size("ep"))])


def ring_gather(block, axis):
    half = block.shape[0] // 2
    prev = shift(block, axis, 1)
    following = shift(block, axis, -1)
    far_top = shift(prev[:half], axis, 1)
    far_bottom = shift(following[half:], axis, -1)
    return block, following, far_top, far_bottom, prev


def far_halves(top, bottom, axis):
    return shift(top, axis, 1), shift(bottom, axis, -1)


def neighbours(following, prev, axis):
    return shift(following, axis, 1), shift(prev, axis, -1)


def call(kernel, out_shape, mib=8, **options):
    return pl.pallas_call(
        kernel,
        out_shape=out_shape,
        compiler_params=pltpu.CompilerParams(vmem_limit_bytes=mib * MIB),
        **options,
    )


def bf16(*shape):
    return jax.ShapeDtypeStruct(shape, jnp.bfloat16)


def f32(*shape):
    return jax.ShapeDtypeStruct(shape, jnp.float32)


def dot(left, right, left_dim=1, right_dim=0):
    return lax.dot_general(
        left, right, (((left_dim,), (right_dim,)), ((), ())), preferred_element_type=jnp.float32
    )


def add_half(whole, half, index, start=0):
    rows, columns = whole.shape
    rows //= 2
    blocks = max(rows // 512, 1)
    rows //= blocks

    def kernel(whole_ref, half_ref, out_ref):
        first = pl.multiple_of(start + pl.program_id(0) * rows, 16)
        total = whole_ref[...].astype(jnp.float32)
        total += half_ref[pl.ds(first, rows)].astype(jnp.float32)
        out_ref[...] = total.astype(jnp.bfloat16)

    spec = pl.BlockSpec((rows, columns), lambda i: (index * blocks + i, 0))
    return call(
        kernel,
        bf16(*whole.shape),
        grid=(blocks,),
        in_specs=[spec, pl.BlockSpec(memory_space=pltpu.VMEM)],
        out_specs=spec,
        input_output_aliases={0: 0},
    )(whole, half)


def pack(w_gate, w_up, w_down):
    depth, width = w_gate.shape

    def kernel(gate_ref, up_ref, down_ref, out_ref):
        out_ref[:depth] = gate_ref[...]
        out_ref[depth : 2 * depth] = up_ref[...]
        out_ref[2 * depth :] = down_ref[...].T

    return call(kernel, bf16(3 * depth, width))(
        *(pltpu.with_memory_space_constraint(w, pltpu.HBM) for w in (w_gate, w_up, w_down))
    )


def weight_parts(refs, r, depth):
    half = depth // 2
    if r == 2:
        top, bottom = refs[2], refs[3]
        return [(top, 0, depth)], [(top, depth, half), (bottom, 0, half)], [(bottom, half, depth)]
    ref = refs[(0, 1, None, 4)[r]]
    return tuple([(ref, i * depth, depth)] for i in range(3))


def start_select(refs, r, out_ref, sem, depth):
    for k in range(RING):

        @pl.when(r == k)
        def _():
            if k == 2:
                rows = 3 * depth // 2
                pieces = [(refs[2], 0, rows), (refs[3], rows, 2 * depth - rows)]
            else:
                pieces = [(refs[(0, 1, None, 4)[k]], 0, 2 * depth)]
            for ref, first, count in pieces:
                source = ref.at[pl.ds(0, count)]
                pltpu.make_async_copy(source, out_ref.at[pl.ds(first, count)], sem).start()


def wait_select(out_ref, sem):
    pltpu.make_async_copy(out_ref, out_ref, sem).wait()


def fill_rows(here_ref, x_ref, rows_ref):
    capacity = x_ref.shape[3]
    z, core = here_ref[2], here_ref[3]
    count = len(SHIFTS)
    for j, step in enumerate(SHIFTS):
        for k in range(2):
            source = ((z - step + count) % count) * 2 + (core if k == 0 else 1 - core)
            rows_ref[pl.ds((2 * j + k) * capacity, capacity)] = x_ref[0, source, 0]


def activations(here, routed_inputs, weights, width):
    _, sources, _, capacity, model_width = routed_inputs.shape
    depth = model_width // RING
    slots = sources * capacity

    def kernel(here_ref, x_ref, *refs):
        weight_refs, (hidden_ref, silu_ref, slope_ref) = refs[:5], refs[5:8]
        x, gate, up, chosen, sems = refs[8:]
        step = pl.program_id(0)
        now = step % 2

        def start(r):
            start_select(weight_refs, r, chosen.at[r % 2], sems.at[r % 2], depth)

        @pl.when(step == 0)
        def _():
            start(step)

        @pl.when(step < RING - 1)
        def _():
            start(step + 1)

        @pl.when(step == 0)
        def _():
            gate[...] = jnp.zeros_like(gate)
            up[...] = jnp.zeros_like(up)

        fill_rows(here_ref, x_ref, x)
        wait_select(chosen.at[now], sems.at[now])
        gate[...] += dot(x[...], chosen[now, :depth])
        up[...] += dot(x[...], chosen[now, depth:])

        @pl.when(step == RING - 1)
        def _():
            gate_act, up_act = gate[...], up[...]
            sigmoid_gate = jax.nn.sigmoid(gate_act)
            silu_gate = gate_act * sigmoid_gate
            hidden_ref[...] = (silu_gate * up_act).astype(jnp.bfloat16)
            silu_ref[...] = silu_gate
            slope_ref[...] = up_act * sigmoid_gate * (1.0 + gate_act * (1.0 - sigmoid_gate))

    whole = pl.BlockSpec(memory_space=pltpu.VMEM)
    return call(
        kernel,
        (bf16(slots, width), f32(slots, width), f32(slots, width)),
        mib=18,
        grid_spec=pltpu.PrefetchScalarGridSpec(
            num_scalar_prefetch=1,
            grid=(RING,),
            in_specs=[
                pl.BlockSpec(
                    (1, sources, 1, capacity, depth),
                    lambda i, here: (0, 0, 0, 0, (here[0] + i) % RING),
                )
            ]
            + [whole] * 5,
            out_specs=(pl.BlockSpec((slots, width), lambda i, here: (0, 0)),) * 3,
            scratch_shapes=[pltpu.VMEM((slots, depth), jnp.bfloat16)]
            + [pltpu.VMEM((slots, width), jnp.float32)] * 2
            + [pltpu.VMEM((2, 2 * depth, width), jnp.bfloat16), pltpu.SemaphoreType.DMA((2,))],
        ),
    )(here, routed_inputs, *weights)


def pair_gradients(here, scaled, weights, hidden, silu, slope, groups):
    slots, width = hidden.shape
    depth = scaled[0][0].shape[1]
    places, at = [], 0
    for group in scaled:
        rows = group[0].shape[0]
        first = 0
        for q, part in zip((0, 1, 2, 3) if len(group) == 4 else (0, 1, 2, 2, 3), group):
            places.append((q, at + first % rows, part.shape[0]))
            first += part.shape[0]
        at += rows
    spans, at = [], 0
    for rows in groups:
        spans.append((at, rows))
        at += rows

    def kernel(here_ref, *refs):
        scaled_refs, refs = refs[: len(places)], refs[len(places) :]
        weight_refs, (hidden_ref, silu_ref, slope_ref) = refs[:5], refs[5:8]
        pair_ref, extra_ref, by_r, top_ref, bottom_ref = refs[8:13]
        chosen, downs, hidden_grad_ref, chosen_sem, sems = refs[13:]
        t = here_ref[1]
        for i, (q, first, count) in enumerate(places):
            r = (t + q) % RING
            pltpu.make_async_copy(
                scaled_refs[i], by_r.at[r, pl.ds(first, count)], sems.at[0, r]
            ).start()
        for r in range(RING):
            ((ref, first, count),) = weight_parts(weight_refs, r, depth)[2]
            pltpu.make_async_copy(ref.at[pl.ds(first, count)], downs.at[r], sems.at[1, r]).start()
        start_select(weight_refs, (t + 2) % RING, chosen, chosen_sem, depth)
        hidden_grad_ref[...] = jnp.zeros_like(hidden_grad_ref)

        def add_columns(r, carry):
            pltpu.make_async_copy(by_r.at[r], by_r.at[r], sems.at[0, r]).wait()
            pltpu.make_async_copy(downs.at[r], downs.at[r], sems.at[1, r]).wait()
            hidden_grad_ref[...] += dot(by_r[r], downs[r])
            return carry

        lax.fori_loop(0, RING, add_columns, 0)
        hidden_grad = hidden_grad_ref[...]
        products = jnp.sum(
            hidden_grad * hidden_ref[...].astype(jnp.float32), axis=1, keepdims=True
        )
        high = products.astype(jnp.bfloat16).astype(jnp.float32)
        lane = lax.broadcasted_iota(jnp.int32, (slots, LANES), 1)
        extra = jnp.where(lane == 0, high, jnp.where(lane == 1, products - high, 0.0))
        extra_ref[...] = extra.astype(jnp.bfloat16)
        pair_ref[:, :width] = (hidden_grad * slope_ref[...]).astype(jnp.bfloat16)
        pair_ref[:, width:] = (hidden_grad * silu_ref[...]).astype(jnp.bfloat16)
        wait_select(chosen, chosen_sem)

        def put(columns, value):
            for start, rows in spans:
                middle = start + rows // 2
                half = pl.ds(start // 2, rows // 2)
                top_ref[half, columns] = value[start:middle]
                bottom_ref[half, columns] = value[middle : start + rows]

        slot_part(pair_ref, chosen, depth, put)

    anywhere = pl.BlockSpec(memory_space=pl.ANY)
    whole = pl.BlockSpec(memory_space=pltpu.VMEM)
    outs = [bf16(slots, 2 * width), bf16(slots, LANES), bf16(RING, slots, depth)]
    outs += [bf16(slots // 2, depth)] * 2
    return call(
        kernel,
        tuple(outs),
        mib=24,
        grid_spec=pltpu.PrefetchScalarGridSpec(
            num_scalar_prefetch=1,
            grid=(1,),
            in_specs=[anywhere] * len(places) + [whole] * 8,
            out_specs=(whole,) * len(outs),
            scratch_shapes=[
                pltpu.VMEM((2 * depth, width), jnp.bfloat16),
                pltpu.VMEM((RING, depth, width), jnp.bfloat16),
                pltpu.VMEM((slots, width), jnp.float32),
                pltpu.SemaphoreType.DMA,
                pltpu.SemaphoreType.DMA((2, RING)),
            ],
        ),
    )(here, *[part for group in scaled for part in group], *weights, hidden, silu, slope)


def slot_part(pair_ref, weights, depth, put):
    half = depth // 2
    width = pair_ref.shape[1] // 2

    def columns(i, carry):
        at = pl.multiple_of(i * half, half)
        value = dot(pair_ref[:, :width], weights[pl.ds(at, half)], 1, 1)
        value += dot(pair_ref[:, width:], weights[pl.ds(depth + at, half)], 1, 1)
        put(pl.ds(at, half), value.astype(jnp.bfloat16))
        return carry

    lax.fori_loop(0, 2, columns, 0)


def slot_gradients(here, pair, weights, groups):
    slots = pair.shape[0]
    width = pair.shape[1] // 2
    depth = weights[0].shape[0] // 3
    spans, at = [], 0
    for rows in groups:
        spans.append(slice(at, at + rows))
        at += rows

    def kernel(here_ref, pair_ref, *refs):
        weight_refs, out_refs, (parts, chosen, sems) = refs[:5], refs[5:-3], refs[-3:]
        t, step = here_ref[1], pl.program_id(0)

        def start(i):
            q = i + i // 2
            start_select(weight_refs, (t + q) % RING, chosen.at[i % 2], sems.at[i % 2], depth)

        @pl.when(step == 0)
        def _():
            start(0)
            start(1)

        now = step % 2
        wait_select(chosen.at[now], sems.at[now])

        def put(columns, value):
            parts[step, :, columns] = value

        slot_part(pair_ref, chosen.at[now], depth, put)

        @pl.when(step == 0)
        def _():
            start(2)

        @pl.when(step == 2)
        def _():
            for i, span in enumerate(spans):
                for j in range(3):
                    out_refs[3 * i + j][...] = parts[j, span]

    whole = pl.BlockSpec(memory_space=pltpu.VMEM)
    outs = tuple(bf16(rows, depth) for rows in groups for _ in range(3))
    parts = call(
        kernel,
        outs,
        mib=17,
        grid_spec=pltpu.PrefetchScalarGridSpec(
            num_scalar_prefetch=1,
            grid=(3,),
            in_specs=[whole] * 6,
            out_specs=(whole,) * len(outs),
            scratch_shapes=[
                pltpu.VMEM((3, slots, depth), jnp.bfloat16),
                pltpu.VMEM((2, 2 * depth, width), jnp.bfloat16),
                pltpu.SemaphoreType.DMA((2,)),
            ],
        ),
    )(here, pair, *weights)
    return [parts[3 * i : 3 * i + 3] for i in range(len(groups))]


def weight_chunk(here, r, routed_inputs, hidden, pair, scaled, received=None):
    _, sources, _, capacity, model_width = routed_inputs.shape
    depth = model_width // RING
    slots, width = hidden.shape
    half = depth // 2
    received = received or ()

    def kernel(here_ref, x_ref, hidden_ref, pair_ref, scaled_ref, *refs):
        x, refs = refs[-1], refs[:-1]
        fill_rows(here_ref, x_ref, x)

        def put(at, value):
            place = pl.ds(at, value.shape[0])
            if received:
                value += refs[0][place].astype(jnp.float32) + refs[1][place].astype(jnp.float32)
                for i in range(2):

                    @pl.when((at >= i * depth) & (at < (i + 1) * depth))
                    def _():
                        refs[2 + i][pl.ds(at - i * depth, value.shape[0])] = value

                return value
            if r != 2:
                refs[0][place] = value.astype(jnp.bfloat16)
                return value
            for i in range(2):

                @pl.when((at >= 3 * i * half) & (at < 3 * (i + 1) * half))
                def _():
                    start = at - 3 * i * half
                    refs[i][pl.ds(start, value.shape[0])] = value.astype(jnp.bfloat16)

            return value

        def inputs_part(i, carry):
            columns = pl.ds(pl.multiple_of((i % 2) * half, half), half)
            lanes = pl.ds(pl.multiple_of((i // 2) * width, width), width)
            put(pl.multiple_of(i * half, half), dot(x[:, columns], pair_ref[:, lanes], 0, 0))
            return carry

        def down_part(c, carry):
            lanes = pl.ds(pl.multiple_of(c * width, width), width)
            value = dot(hidden_ref[...], scaled_ref[0, :, lanes], 0, 0)
            at = pl.multiple_of(2 * depth + c * width, width)
            value = put(at, value)
            if received:
                refs[4][:, lanes] = value
            return carry

        lax.fori_loop(0, 4, inputs_part, 0)
        lax.fori_loop(0, depth // width, down_part, 0)

    whole = pl.BlockSpec(memory_space=pltpu.VMEM)
    if r == 0:
        outs = (f32(depth, width), f32(depth, width), f32(width, depth))
    elif r == 2:
        outs = (bf16(3 * half, width), bf16(3 * half, width))
    else:
        outs = (bf16(6 * half, width),)
    return call(
        kernel,
        outs,
        mib=18 if r == 0 else 12,
        grid_spec=pltpu.PrefetchScalarGridSpec(
            num_scalar_prefetch=1,
            grid=(1,),
            in_specs=[
                pl.BlockSpec(
                    (1, sources, 1, capacity, depth),
                    lambda i, here: (0, 0, 0, 0, (here[0] + r) % RING),
                ),
                whole,
                whole,
                pl.BlockSpec((1, slots, depth), lambda i, here: (r, 0, 0)),
            ]
            + [whole] * len(received),
            out_specs=(whole,) * len(outs),
            scratch_shapes=[pltpu.VMEM((slots, depth), jnp.bfloat16)],
        ),
    )(here, routed_inputs, hidden, pair, scaled, *received)


def join(arrays):
    def kernel(*refs):
        at = 0
        for ref in refs[:-1]:
            refs[-1][pl.ds(at, ref.shape[0])] = ref[...]
            at += ref.shape[0]

    return call(kernel, bf16(sum(a.shape[0] for a in arrays), arrays[0].shape[1]))(*arrays)


def messages(own, other):
    count = len(SHIFTS)
    rows, columns = own.shape
    rows //= count

    def kernel(own_ref, other_ref, *out_refs):
        for j, out_ref in enumerate(out_refs):
            out_ref[:rows] = own_ref[j * rows : (j + 1) * rows]
            out_ref[rows:] = other_ref[j * rows : (j + 1) * rows]

    return call(kernel, (bf16(2 * rows, columns),) * count)(own, other)


def unpack_messages(blocks):
    rows, columns = blocks[0].shape
    rows //= 2

    def kernel(*refs):
        own_ref, other_ref = refs[-2:]
        for j, ref in enumerate(refs[:-2]):
            own_ref[pl.ds(j * rows, rows)] = ref[:rows]
            other_ref[pl.ds(j * rows, rows)] = ref[rows:]

    return call(kernel, (bf16(len(blocks) * rows, columns),) * 2)(*blocks)


def leaving_rows(own, from_prev, from_next, extra, start, count):
    rows, narrow = own.shape
    rows //= count

    def kernel(own_ref, prev_ref, next_ref, extra_ref, *out_refs):
        for j, out_ref in enumerate(out_refs):
            span = slice(j * rows, (j + 1) * rows)
            total = own_ref[span].astype(jnp.float32) + prev_ref[span].astype(jnp.float32)
            total += next_ref[span].astype(jnp.float32)
            out_ref[:, :narrow] = total.astype(jnp.bfloat16)
            out_ref[:, narrow:] = extra_ref[start + j * rows : start + (j + 1) * rows]

    outs = (bf16(rows, narrow + LANES),) * count
    return call(kernel, outs)(own, from_prev, from_next, extra)


def token_rows(slot_index, back):
    tokens = slot_index.shape[0]
    rows, wide = back[0].shape
    narrow = wide - LANES

    def kernel(slot_ref, *refs):
        out_ref = refs[-1]
        total = jnp.zeros((tokens, narrow), jnp.float32)
        chosen = [jnp.zeros((tokens, LANES), jnp.float32)] * 2
        for h, back_ref in enumerate(refs[:-1]):
            slot = lax.broadcasted_iota(jnp.int32, (tokens, rows), 1) + h * rows
            picks = [
                jnp.where(slot_ref[:, k : k + 1] == slot, 1.0, 0.0).astype(jnp.bfloat16)
                for k in range(2)
            ]
            total += dot(picks[0] + picks[1], back_ref[:, :narrow])
            chosen = [c + dot(p, back_ref[:, narrow:]) for c, p in zip(chosen, picks)]
        out_ref[:, :narrow] = total.astype(jnp.bfloat16)
        lane = lax.broadcasted_iota(jnp.int32, (tokens, LANES), 1)
        tail = jnp.zeros((tokens, LANES), jnp.float32)
        for k in range(2):
            value = chosen[k][:, 0:1] + chosen[k][:, 1:2]
            high = value.astype(jnp.bfloat16).astype(jnp.float32)
            tail = jnp.where(lane == 2 * k, high, jnp.where(lane == 2 * k + 1, value - high, tail))
        out_ref[:, narrow:] = tail.astype(jnp.bfloat16)

    return call(kernel, bf16(tokens, wide))(slot_index, *back)


def finish_tokens(here, gate_probs, gathered):
    tokens, wide = gathered[0].shape
    narrow = wide - LANES

    def kernel(here_ref, probs_ref, *refs):
        out_ref, logit_ref = refs[RING:]
        total = jnp.zeros((tokens, LANES), jnp.float32)
        for q in range(RING):
            first = ((here_ref[0] + here_ref[1] + q) % RING) * narrow
            out_ref[:, pl.ds(pl.multiple_of(first, LANES), narrow)] = refs[q][:, :narrow]
            total += refs[q][:, narrow:].astype(jnp.float32)
        chosen = [
            (total[:, 2 * k : 2 * k + 1] + total[:, 2 * k + 1 : 2 * k + 2])
            .astype(jnp.bfloat16)
            .astype(jnp.float32)
            for k in range(2)
        ]
        both = chosen[0] + chosen[1]
        for k in range(2):
            logit_ref[:, k : k + 1] = chosen[k] - probs_ref[:, k : k + 1] * both

    whole = pl.BlockSpec(memory_space=pltpu.VMEM)
    return call(
        kernel,
        (bf16(tokens, RING * narrow), f32(tokens, 2)),
        grid_spec=pltpu.PrefetchScalarGridSpec(
            num_scalar_prefetch=1,
            grid=(1,),
            in_specs=[whole] * (RING + 1),
            out_specs=(whole,) * 2,
        ),
    )(here, gate_probs, *gathered)


def slots_of(routes, z, core, capacity, experts):
    tokens = routes.shape[0]
    hot = (routes[:, :, None] == jnp.arange(experts, dtype=jnp.int32)).astype(jnp.bfloat16)
    before = jnp.arange(tokens)[:, None] > jnp.arange(tokens)[None, :]
    earlier = dot(before.astype(jnp.bfloat16), hot[:, 0] + hot[:, 1])
    place = jnp.sum(earlier[:, None, :] * hot.astype(jnp.float32), axis=2).astype(jnp.int32)
    count = len(SHIFTS)
    distance = (routes // 2 - z + count) % count
    index = jnp.where(
        distance <= count // 2, jnp.maximum(2 * distance - 1, 0), 2 * (count - distance)
    )
    other = (routes % 2 != core).astype(jnp.int32)
    return (other * count + index) * capacity + place


def layer(out_grad, routes, chosen_logits, routed_inputs, w_gate, w_up, w_down):
    experts = lax.axis_size("ep")
    f, t = lax.axis_index("fsdp"), lax.axis_index("tp")
    z, core = lax.axis_index("ep") // 2, lax.axis_index("ep") % 2
    here = jnp.stack([f, t, z, core]).astype(jnp.int32)
    model_width = out_grad.shape[1]
    capacity = routed_inputs.shape[3]
    slots = experts * capacity
    narrow = model_width // RING
    width = w_gate.shape[2]
    block = 2 * capacity

    weights = ring_gather(pack(w_gate[0], w_up[0], w_down[0]), "fsdp")

    gate_probs = jax.nn.softmax(chosen_logits, axis=-1)
    slot_index = slots_of(routes, z, core, capacity, experts)
    piece = lax.dynamic_slice_in_dim(out_grad, ((f + t) % RING) * narrow, narrow, 1)
    weighted = gate_probs[:, :, None] * piece.astype(jnp.float32)[:, None, :]
    weighted = weighted.astype(jnp.bfloat16)

    def routed(first):
        slot = first + jnp.arange(slots // 2, dtype=jnp.int32)
        picks = (slot_index[:, :, None] == slot).astype(jnp.bfloat16)
        return lax.dot_general(
            picks, weighted, (((0, 1), (0, 1)), ((), ())), preferred_element_type=jnp.float32
        ).astype(jnp.bfloat16)

    own, other = routed(0), swap_cores(routed(slots // 2))
    sent = messages(own, other)
    arrived = [sent[0]] + [shift_z(sent[j], SHIFTS[j]) for j in range(1, len(SHIFTS))]
    gathered = [ring_gather(join([arrived[j] for j in group]), "tp") for group in GROUPS]

    hidden, silu, slope = activations(here, routed_inputs, weights, width)
    groups = [len(group) * block for group in GROUPS]
    pair, extra, scaled, *far = pair_gradients(
        here, gathered, weights, hidden, silu, slope, groups
    )
    far = far_halves(*far, "tp")
    parts = slot_gradients(here, pair, weights, groups)
    leaving = []
    for g, group in enumerate(GROUPS):
        own, following, prev = parts[g]
        start = group[0] * block
        following = add_half(following, far[0], 0, start // 2)
        prev = add_half(prev, far[1], 1, start // 2)
        received = neighbours(following, prev, "tp")
        leaving += leaving_rows(own, *received, extra, start, len(group))

    chunk = functools.partial(
        weight_chunk, here, routed_inputs=routed_inputs, hidden=hidden, pair=pair, scaled=scaled
    )
    far = far_halves(*chunk(2), "fsdp")
    received = neighbours(add_half(*chunk(1), far[0], 0), add_half(*chunk(3), far[1], 1), "fsdp")
    grad_gate, grad_up, grad_down = chunk(0, received=received)

    returned = [leaving[0]] + [shift_z(leaving[j], -SHIFTS[j]) for j in range(1, len(SHIFTS))]
    own, other = unpack_messages(returned)
    mine = token_rows(slot_index, [own, swap_cores(other)])
    tokens_by_ring = [mine] + [shift(mine, "tp", -q) for q in range(1, RING)]
    input_grad, logit_grad = finish_tokens(here, gate_probs, tokens_by_ring)
    return input_grad, logit_grad, grad_gate[None], grad_up[None], grad_down[None]


def solution(mesh):
    return jax.shard_map(
        layer,
        mesh=mesh,
        in_specs=(
            P(("ep", "fsdp"), None),
            P(("ep", "fsdp"), None),
            P(("ep", "fsdp"), None),
            P("ep", None, "fsdp", None, None),
            P("ep", "fsdp", "tp"),
            P("ep", "fsdp", "tp"),
            P("ep", "tp", "fsdp"),
        ),
        out_specs=(
            P(("ep", "fsdp"), None),
            P(("ep", "fsdp"), None),
            P("ep", "fsdp", "tp"),
            P("ep", "fsdp", "tp"),
            P("ep", "tp", "fsdp"),
        ),
        check_vma=False,
    )
```

```python
import functools

import jax
import jax.numpy as jnp
from jax import lax
from jax.experimental import pallas as pl
from jax.experimental.pallas import tpu as pltpu
from jax.sharding import PartitionSpec as P


RING = 4
LANES = 128
MIB = 1 << 20


SHIFTS = (0, 1, -1, 2, -2, 3, -3, 4)
GROUPS = ((0, 1, 2, 3, 4), (5, 6, 7))


def shift(x, axis, step):
    n = lax.axis_size(axis)
    return lax.ppermute(x, axis, [(i, (i + step) % n) for i in range(n)])


def shift_z(x, step):
    n = lax.axis_size("ep")
    return lax.ppermute(x, "ep", [(i, (i + 2 * step) % n) for i in range(n)])


def swap_cores(x):
    return lax.ppermute(x, "ep", [(i, i ^ 1) for i in range(lax.axis_size("ep"))])


def ring_gather(block, axis):
    half = block.shape[0] // 2
    prev = shift(block, axis, 1)
    following = shift(block, axis, -1)
    far_top = shift(prev[:half], axis, 1)
    far_bottom = shift(following[half:], axis, -1)
    return block, following, far_top, far_bottom, prev


def far_halves(top, bottom, axis):
    return shift(top, axis, 1), shift(bottom, axis, -1)


def neighbours(following, prev, axis):
    return shift(following, axis, 1), shift(prev, axis, -1)


def call(kernel, out_shape, mib=8, **options):
    return pl.pallas_call(
        kernel,
        out_shape=out_shape,
        compiler_params=pltpu.CompilerParams(vmem_limit_bytes=mib * MIB),
        **options,
    )


def bf16(*shape):
    return jax.ShapeDtypeStruct(shape, jnp.bfloat16)


def f32(*shape):
    return jax.ShapeDtypeStruct(shape, jnp.float32)


def dot(left, right, left_dim=1, right_dim=0):
    return lax.dot_general(
        left, right, (((left_dim,), (right_dim,)), ((), ())), preferred_element_type=jnp.float32
    )


def add_half(whole, half, index, start=0):
    rows, columns = whole.shape
    rows //= 2
    blocks = max(rows // 512, 1)
    rows //= blocks

    def kernel(whole_ref, half_ref, out_ref):
        first = pl.multiple_of(start + pl.program_id(0) * rows, 16)
        total = whole_ref[...].astype(jnp.float32)
        total += half_ref[pl.ds(first, rows)].astype(jnp.float32)
        out_ref[...] = total.astype(jnp.bfloat16)

    spec = pl.BlockSpec((rows, columns), lambda i: (index * blocks + i, 0))
    return call(
        kernel,
        bf16(*whole.shape),
        grid=(blocks,),
        in_specs=[spec, pl.BlockSpec(memory_space=pltpu.VMEM)],
        out_specs=spec,
        input_output_aliases={0: 0},
    )(whole, half)


def pack(w_gate, w_up, w_down):
    depth, width = w_gate.shape

    def kernel(gate_ref, up_ref, down_ref, out_ref):
        out_ref[:depth] = gate_ref[...]
        out_ref[depth : 2 * depth] = up_ref[...]
        out_ref[2 * depth :] = down_ref[...].T

    return call(kernel, bf16(3 * depth, width))(
        *(pltpu.with_memory_space_constraint(w, pltpu.HBM) for w in (w_gate, w_up, w_down))
    )


def weight_parts(refs, r, depth):
    half = depth // 2
    if r == 2:
        top, bottom = refs[2], refs[3]
        return [(top, 0, depth)], [(top, depth, half), (bottom, 0, half)], [(bottom, half, depth)]
    ref = refs[(0, 1, None, 4)[r]]
    return tuple([(ref, i * depth, depth)] for i in range(3))


def start_select(refs, r, out_ref, sem, depth):
    for k in range(RING):

        @pl.when(r == k)
        def _():
            if k == 2:
                rows = 3 * depth // 2
                pieces = [(refs[2], 0, rows), (refs[3], rows, 2 * depth - rows)]
            else:
                pieces = [(refs[(0, 1, None, 4)[k]], 0, 2 * depth)]
            for ref, first, count in pieces:
                source = ref.at[pl.ds(0, count)]
                pltpu.make_async_copy(source, out_ref.at[pl.ds(first, count)], sem).start()


def wait_select(out_ref, sem):
    pltpu.make_async_copy(out_ref, out_ref, sem).wait()


def fill_rows(here_ref, x_ref, rows_ref):
    capacity = x_ref.shape[3]
    z, core = here_ref[2], here_ref[3]
    count = len(SHIFTS)
    for j, step in enumerate(SHIFTS):
        for k in range(2):
            source = ((z - step + count) % count) * 2 + (core if k == 0 else 1 - core)
            rows_ref[pl.ds((2 * j + k) * capacity, capacity)] = x_ref[0, source, 0]


def activations(here, routed_inputs, weights, width):
    _, sources, _, capacity, model_width = routed_inputs.shape
    depth = model_width // RING
    slots = sources * capacity

    def kernel(here_ref, x_ref, w0, w1, w2, w3, w4, hidden_ref, silu_ref, slope_ref, x, gate, up):
        refs = (w0, w1, w2, w3, w4)
        step = pl.program_id(0)
        fill_rows(here_ref, x_ref, x)
        for r in range(RING):

            @pl.when(step == r)
            def _():
                gates, ups, _ = weight_parts(refs, r, depth)
                for pieces, total in ((gates, gate), (ups, up)):
                    at, value = 0, None
                    for ref, first, count in pieces:
                        term = dot(x[:, at : at + count], ref[pl.ds(first, count)])
                        value = term if value is None else value + term
                        at += count
                    total[...] = value if r == 0 else total[...] + value

        @pl.when(step == RING - 1)
        def _():
            gate_act, up_act = gate[...], up[...]
            sigmoid_gate = jax.nn.sigmoid(gate_act)
            silu_gate = gate_act * sigmoid_gate
            hidden_ref[...] = (silu_gate * up_act).astype(jnp.bfloat16)
            silu_ref[...] = silu_gate
            slope_ref[...] = up_act * sigmoid_gate * (1.0 + gate_act * (1.0 - sigmoid_gate))

    whole = pl.BlockSpec(memory_space=pltpu.VMEM)
    return call(
        kernel,
        (bf16(slots, width), f32(slots, width), f32(slots, width)),
        mib=16,
        grid_spec=pltpu.PrefetchScalarGridSpec(
            num_scalar_prefetch=1,
            grid=(RING,),
            in_specs=[
                pl.BlockSpec(
                    (1, sources, 1, capacity, depth),
                    lambda i, here: (0, 0, 0, 0, (here[0] + i) % RING),
                )
            ]
            + [whole] * 5,
            out_specs=(pl.BlockSpec((slots, width), lambda i, here: (0, 0)),) * 3,
            scratch_shapes=[pltpu.VMEM((slots, depth), jnp.bfloat16)]
            + [pltpu.VMEM((slots, width), jnp.float32)] * 2,
        ),
    )(here, routed_inputs, *weights)


def pair_gradients(here, scaled, weights, hidden, silu, slope, groups):
    slots, width = hidden.shape
    depth = scaled[0][0].shape[1]
    places, at = [], 0
    for group in scaled:
        rows = group[0].shape[0]
        first = 0
        for q, part in zip((0, 1, 2, 3) if len(group) == 4 else (0, 1, 2, 2, 3), group):
            places.append((q, at + first % rows, part.shape[0]))
            first += part.shape[0]
        at += rows
    spans, at = [], 0
    for rows in groups:
        spans.append((at, rows))
        at += rows

    def kernel(here_ref, *refs):
        scaled_refs, refs = refs[: len(places)], refs[len(places) :]
        weight_refs, (hidden_ref, silu_ref, slope_ref) = refs[:5], refs[5:8]
        pair_ref, extra_ref, by_r, top_ref, bottom_ref = refs[8:13]
        chosen, downs, hidden_grad_ref, chosen_sem, sems = refs[13:]
        t = here_ref[1]
        for i, (q, first, count) in enumerate(places):
            r = (t + q) % RING
            pltpu.make_async_copy(
                scaled_refs[i], by_r.at[r, pl.ds(first, count)], sems.at[0, r]
            ).start()
        for r in range(RING):
            ((ref, first, count),) = weight_parts(weight_refs, r, depth)[2]
            pltpu.make_async_copy(ref.at[pl.ds(first, count)], downs.at[r], sems.at[1, r]).start()
        start_select(weight_refs, (t + 2) % RING, chosen, chosen_sem, depth)
        hidden_grad_ref[...] = jnp.zeros_like(hidden_grad_ref)

        def add_columns(r, carry):
            pltpu.make_async_copy(by_r.at[r], by_r.at[r], sems.at[0, r]).wait()
            pltpu.make_async_copy(downs.at[r], downs.at[r], sems.at[1, r]).wait()
            hidden_grad_ref[...] += dot(by_r[r], downs[r])
            return carry

        lax.fori_loop(0, RING, add_columns, 0)
        hidden_grad = hidden_grad_ref[...]
        products = jnp.sum(
            hidden_grad * hidden_ref[...].astype(jnp.float32), axis=1, keepdims=True
        )
        high = products.astype(jnp.bfloat16).astype(jnp.float32)
        lane = lax.broadcasted_iota(jnp.int32, (slots, LANES), 1)
        extra = jnp.where(lane == 0, high, jnp.where(lane == 1, products - high, 0.0))
        extra_ref[...] = extra.astype(jnp.bfloat16)
        pair_ref[:, :width] = (hidden_grad * slope_ref[...]).astype(jnp.bfloat16)
        pair_ref[:, width:] = (hidden_grad * silu_ref[...]).astype(jnp.bfloat16)
        wait_select(chosen, chosen_sem)
        for columns, value in slot_part(pair_ref, chosen, depth):
            for start, rows in spans:
                middle = start + rows // 2
                half = pl.ds(start // 2, rows // 2)
                top_ref[half, columns] = value[start:middle]
                bottom_ref[half, columns] = value[middle : start + rows]

    anywhere = pl.BlockSpec(memory_space=pl.ANY)
    whole = pl.BlockSpec(memory_space=pltpu.VMEM)
    outs = [bf16(slots, 2 * width), bf16(slots, LANES), bf16(RING, slots, depth)]
    outs += [bf16(slots // 2, depth)] * 2
    return call(
        kernel,
        tuple(outs),
        mib=24,
        grid_spec=pltpu.PrefetchScalarGridSpec(
            num_scalar_prefetch=1,
            grid=(1,),
            in_specs=[anywhere] * len(places) + [whole] * 8,
            out_specs=(whole,) * len(outs),
            scratch_shapes=[
                pltpu.VMEM((2 * depth, width), jnp.bfloat16),
                pltpu.VMEM((RING, depth, width), jnp.bfloat16),
                pltpu.VMEM((slots, width), jnp.float32),
                pltpu.SemaphoreType.DMA,
                pltpu.SemaphoreType.DMA((2, RING)),
            ],
        ),
    )(here, *[part for group in scaled for part in group], *weights, hidden, silu, slope)


def slot_part(pair_ref, weights, depth):
    half = depth // 2
    width = pair_ref.shape[1] // 2
    for i in range(2):
        value = dot(pair_ref[:, :width], weights[pl.ds(i * half, half)], 1, 1)
        value += dot(pair_ref[:, width:], weights[pl.ds(depth + i * half, half)], 1, 1)
        yield slice(i * half, (i + 1) * half), value.astype(jnp.bfloat16)


def slot_gradients(here, pair, weights, groups):
    slots = pair.shape[0]
    width = pair.shape[1] // 2
    depth = weights[0].shape[0] // 3
    spans, at = [], 0
    for rows in groups:
        spans.append(slice(at, at + rows))
        at += rows

    def kernel(here_ref, pair_ref, *refs):
        weight_refs, out_refs, (parts, chosen, sems) = refs[:5], refs[5:-3], refs[-3:]
        t, step = here_ref[1], pl.program_id(0)

        def start(i):
            q = i + i // 2
            start_select(weight_refs, (t + q) % RING, chosen.at[i % 2], sems.at[i % 2], depth)

        @pl.when(step == 0)
        def _():
            start(0)
            start(1)

        now = step % 2
        wait_select(chosen.at[now], sems.at[now])
        for columns, value in slot_part(pair_ref, chosen.at[now], depth):
            parts[step, :, columns] = value

        @pl.when(step == 0)
        def _():
            start(2)

        @pl.when(step == 2)
        def _():
            for i, span in enumerate(spans):
                for j in range(3):
                    out_refs[3 * i + j][...] = parts[j, span]

    whole = pl.BlockSpec(memory_space=pltpu.VMEM)
    outs = tuple(bf16(rows, depth) for rows in groups for _ in range(3))
    parts = call(
        kernel,
        outs,
        mib=17,
        grid_spec=pltpu.PrefetchScalarGridSpec(
            num_scalar_prefetch=1,
            grid=(3,),
            in_specs=[whole] * 6,
            out_specs=(whole,) * len(outs),
            scratch_shapes=[
                pltpu.VMEM((3, slots, depth), jnp.bfloat16),
                pltpu.VMEM((2, 2 * depth, width), jnp.bfloat16),
                pltpu.SemaphoreType.DMA((2,)),
            ],
        ),
    )(here, pair, *weights)
    return [parts[3 * i : 3 * i + 3] for i in range(len(groups))]


def weight_chunk(here, r, routed_inputs, hidden, pairs, scaled, received=None):
    _, sources, _, capacity, model_width = routed_inputs.shape
    depth = model_width // RING
    width = hidden.shape[1]
    half = depth // 2
    groups = len(pairs)
    spans, at = [], 0
    for pair in pairs:
        spans.append(slice(at, at + pair.shape[0]))
        at += pair.shape[0]

    def kernel(here_ref, x_ref, hidden_ref, *refs):
        pair_refs, scaled_refs, refs = refs[:groups], refs[groups : 2 * groups], refs[2 * groups :]
        x, refs = refs[-1], refs[:-1]
        fill_rows(here_ref, x_ref, x)

        for i in range(6):
            if i < 4:
                lanes = slice((i // 2) * width, (i // 2 + 1) * width)
                columns = slice((i % 2) * half, (i % 2 + 1) * half)
                value = sum(
                    dot(x[spans[h], columns], pair_refs[h][:, lanes], 0, 0) for h in range(groups)
                )
                values = [(value, slice(0, half))]
            else:
                values = []
                for c in range(half // width):
                    first = (i - 4) * half + c * width
                    value = sum(
                        dot(
                            hidden_ref[spans[h]],
                            scaled_refs[h][0, :, first : first + width],
                            0,
                            0,
                        )
                        for h in range(groups)
                    )
                    values.append((value, slice(c * width, (c + 1) * width)))
            for value, place in values:
                source = pl.ds(i * half + place.start, place.stop - place.start)
                if r:
                    out_ref = refs[i // 3] if r == 2 else refs[0]
                    at = (i % 3 if r == 2 else i) * half + place.start
                    out_ref[pl.ds(at, place.stop - place.start)] = value.astype(jnp.bfloat16)
                    continue
                value += refs[0][source].astype(jnp.float32) + refs[1][source].astype(jnp.float32)
                if i < 4:
                    refs[2 + i // 2][pl.ds((i % 2) * half, half)] = value
                else:
                    first = (i - 4) * half + place.start
                    refs[4][:, first : first + width] = value

    whole = pl.BlockSpec(memory_space=pltpu.VMEM)
    chunks = [
        pl.BlockSpec((1, pair.shape[0], depth), lambda i, here: (r, 0, 0)) for pair in pairs
    ]
    if r == 0:
        outs = (f32(depth, width), f32(depth, width), f32(width, depth))
    elif r == 2:
        outs = (bf16(3 * half, width), bf16(3 * half, width))
    else:
        outs = (bf16(6 * half, width),)
    received = received or ()
    return call(
        kernel,
        outs,
        mib=18 if r == 0 else 12,
        grid_spec=pltpu.PrefetchScalarGridSpec(
            num_scalar_prefetch=1,
            grid=(1,),
            in_specs=[
                pl.BlockSpec(
                    (1, sources, 1, capacity, depth),
                    lambda i, here: (0, 0, 0, 0, (here[0] + r) % RING),
                ),
                whole,
            ]
            + [whole] * groups
            + chunks
            + [whole] * len(received),
            out_specs=(whole,) * len(outs),
            scratch_shapes=[pltpu.VMEM((sources * capacity, depth), jnp.bfloat16)],
        ),
    )(here, routed_inputs, hidden, *pairs, *scaled, *received)


def join(arrays):
    def kernel(*refs):
        at = 0
        for ref in refs[:-1]:
            refs[-1][pl.ds(at, ref.shape[0])] = ref[...]
            at += ref.shape[0]

    return call(kernel, bf16(sum(a.shape[0] for a in arrays), arrays[0].shape[1]))(*arrays)


def messages(own, other):
    count = len(SHIFTS)
    rows, columns = own.shape
    rows //= count

    def kernel(own_ref, other_ref, *out_refs):
        for j, out_ref in enumerate(out_refs):
            out_ref[:rows] = own_ref[j * rows : (j + 1) * rows]
            out_ref[rows:] = other_ref[j * rows : (j + 1) * rows]

    return call(kernel, (bf16(2 * rows, columns),) * count)(own, other)


def unpack_messages(blocks):
    rows, columns = blocks[0].shape
    rows //= 2

    def kernel(*refs):
        own_ref, other_ref = refs[-2:]
        for j, ref in enumerate(refs[:-2]):
            own_ref[pl.ds(j * rows, rows)] = ref[:rows]
            other_ref[pl.ds(j * rows, rows)] = ref[rows:]

    return call(kernel, (bf16(len(blocks) * rows, columns),) * 2)(*blocks)


def leaving_rows(own, from_prev, from_next, extra, start, count):
    rows, narrow = own.shape
    rows //= count

    def kernel(own_ref, prev_ref, next_ref, extra_ref, *out_refs):
        for j, out_ref in enumerate(out_refs):
            span = slice(j * rows, (j + 1) * rows)
            total = own_ref[span].astype(jnp.float32) + prev_ref[span].astype(jnp.float32)
            total += next_ref[span].astype(jnp.float32)
            out_ref[:, :narrow] = total.astype(jnp.bfloat16)
            out_ref[:, narrow:] = extra_ref[start + j * rows : start + (j + 1) * rows]

    outs = (bf16(rows, narrow + LANES),) * count
    return call(kernel, outs)(own, from_prev, from_next, extra)


def token_rows(slot_index, back):
    tokens = slot_index.shape[0]
    rows, wide = back[0].shape
    narrow = wide - LANES

    def kernel(slot_ref, *refs):
        out_ref = refs[-1]
        total = jnp.zeros((tokens, narrow), jnp.float32)
        chosen = [jnp.zeros((tokens, LANES), jnp.float32)] * 2
        for h, back_ref in enumerate(refs[:-1]):
            slot = lax.broadcasted_iota(jnp.int32, (tokens, rows), 1) + h * rows
            picks = [
                jnp.where(slot_ref[:, k : k + 1] == slot, 1.0, 0.0).astype(jnp.bfloat16)
                for k in range(2)
            ]
            total += dot(picks[0] + picks[1], back_ref[:, :narrow])
            chosen = [c + dot(p, back_ref[:, narrow:]) for c, p in zip(chosen, picks)]
        out_ref[:, :narrow] = total.astype(jnp.bfloat16)
        lane = lax.broadcasted_iota(jnp.int32, (tokens, LANES), 1)
        tail = jnp.zeros((tokens, LANES), jnp.float32)
        for k in range(2):
            value = chosen[k][:, 0:1] + chosen[k][:, 1:2]
            high = value.astype(jnp.bfloat16).astype(jnp.float32)
            tail = jnp.where(lane == 2 * k, high, jnp.where(lane == 2 * k + 1, value - high, tail))
        out_ref[:, narrow:] = tail.astype(jnp.bfloat16)

    return call(kernel, bf16(tokens, wide))(slot_index, *back)


def finish_tokens(here, gate_probs, gathered):
    tokens, wide = gathered[0].shape
    narrow = wide - LANES

    def kernel(here_ref, probs_ref, *refs):
        out_ref, logit_ref = refs[RING:]
        total = jnp.zeros((tokens, LANES), jnp.float32)
        for q in range(RING):
            first = ((here_ref[0] + here_ref[1] + q) % RING) * narrow
            out_ref[:, pl.ds(pl.multiple_of(first, LANES), narrow)] = refs[q][:, :narrow]
            total += refs[q][:, narrow:].astype(jnp.float32)
        chosen = [
            (total[:, 2 * k : 2 * k + 1] + total[:, 2 * k + 1 : 2 * k + 2])
            .astype(jnp.bfloat16)
            .astype(jnp.float32)
            for k in range(2)
        ]
        both = chosen[0] + chosen[1]
        for k in range(2):
            logit_ref[:, k : k + 1] = chosen[k] - probs_ref[:, k : k + 1] * both

    whole = pl.BlockSpec(memory_space=pltpu.VMEM)
    return call(
        kernel,
        (bf16(tokens, RING * narrow), f32(tokens, 2)),
        grid_spec=pltpu.PrefetchScalarGridSpec(
            num_scalar_prefetch=1,
            grid=(1,),
            in_specs=[whole] * (RING + 1),
            out_specs=(whole,) * 2,
        ),
    )(here, gate_probs, *gathered)


def slots_of(routes, z, core, capacity, experts):
    tokens = routes.shape[0]
    hot = (routes[:, :, None] == jnp.arange(experts, dtype=jnp.int32)).astype(jnp.bfloat16)
    before = jnp.arange(tokens)[:, None] > jnp.arange(tokens)[None, :]
    earlier = dot(before.astype(jnp.bfloat16), hot[:, 0] + hot[:, 1])
    place = jnp.sum(earlier[:, None, :] * hot.astype(jnp.float32), axis=2).astype(jnp.int32)
    count = len(SHIFTS)
    distance = (routes // 2 - z + count) % count
    index = jnp.where(
        distance <= count // 2, jnp.maximum(2 * distance - 1, 0), 2 * (count - distance)
    )
    other = (routes % 2 != core).astype(jnp.int32)
    return (other * count + index) * capacity + place


def layer(out_grad, routes, chosen_logits, routed_inputs, w_gate, w_up, w_down):
    experts = lax.axis_size("ep")
    f, t = lax.axis_index("fsdp"), lax.axis_index("tp")
    z, core = lax.axis_index("ep") // 2, lax.axis_index("ep") % 2
    here = jnp.stack([f, t, z, core]).astype(jnp.int32)
    model_width = out_grad.shape[1]
    capacity = routed_inputs.shape[3]
    slots = experts * capacity
    narrow = model_width // RING
    width = w_gate.shape[2]
    block = 2 * capacity

    weights = ring_gather(pack(w_gate[0], w_up[0], w_down[0]), "fsdp")

    gate_probs = jax.nn.softmax(chosen_logits, axis=-1)
    slot_index = slots_of(routes, z, core, capacity, experts)
    piece = lax.dynamic_slice_in_dim(out_grad, ((f + t) % RING) * narrow, narrow, 1)
    weighted = gate_probs[:, :, None] * piece.astype(jnp.float32)[:, None, :]
    weighted = weighted.astype(jnp.bfloat16)

    def routed(first):
        slot = first + jnp.arange(slots // 2, dtype=jnp.int32)
        picks = (slot_index[:, :, None] == slot).astype(jnp.bfloat16)
        return lax.dot_general(
            picks, weighted, (((0, 1), (0, 1)), ((), ())), preferred_element_type=jnp.float32
        ).astype(jnp.bfloat16)

    own, other = routed(0), swap_cores(routed(slots // 2))
    sent = messages(own, other)
    arrived = [sent[0]] + [shift_z(sent[j], SHIFTS[j]) for j in range(1, len(SHIFTS))]
    gathered = [ring_gather(join([arrived[j] for j in group]), "tp") for group in GROUPS]

    hidden, silu, slope = activations(here, routed_inputs, weights, width)
    groups = [len(group) * block for group in GROUPS]
    pair, extra, scaled, *far = pair_gradients(
        here, gathered, weights, hidden, silu, slope, groups
    )
    far = far_halves(*far, "tp")
    parts = slot_gradients(here, pair, weights, groups)
    leaving = []
    for g, group in enumerate(GROUPS):
        own, following, prev = parts[g]
        start = group[0] * block
        following = add_half(following, far[0], 0, start // 2)
        prev = add_half(prev, far[1], 1, start // 2)
        received = neighbours(following, prev, "tp")
        leaving += leaving_rows(own, *received, extra, start, len(group))

    chunk = functools.partial(
        weight_chunk, here, routed_inputs=routed_inputs, hidden=hidden, pairs=[pair], scaled=[scaled]
    )
    far = far_halves(*chunk(2), "fsdp")
    received = neighbours(add_half(*chunk(1), far[0], 0), add_half(*chunk(3), far[1], 1), "fsdp")
    grad_gate, grad_up, grad_down = chunk(0, received=received)

    returned = [leaving[0]] + [shift_z(leaving[j], -SHIFTS[j]) for j in range(1, len(SHIFTS))]
    own, other = unpack_messages(returned)
    mine = token_rows(slot_index, [own, swap_cores(other)])
    tokens_by_ring = [mine] + [shift(mine, "tp", -q) for q in range(1, RING)]
    input_grad, logit_grad = finish_tokens(here, gate_probs, tokens_by_ring)
    return input_grad, logit_grad, grad_gate[None], grad_up[None], grad_down[None]


def solution(mesh):
    return jax.shard_map(
        layer,
        mesh=mesh,
        in_specs=(
            P(("ep", "fsdp"), None),
            P(("ep", "fsdp"), None),
            P(("ep", "fsdp"), None),
            P("ep", None, "fsdp", None, None),
            P("ep", "fsdp", "tp"),
            P("ep", "fsdp", "tp"),
            P("ep", "tp", "fsdp"),
        ),
        out_specs=(
            P(("ep", "fsdp"), None),
            P(("ep", "fsdp"), None),
            P("ep", "fsdp", "tp"),
            P("ep", "fsdp", "tp"),
            P("ep", "tp", "fsdp"),
        ),
        check_vma=False,
    )
```

```python
import functools

import jax
import jax.numpy as jnp
from jax import lax
from jax.experimental import pallas as pl
from jax.experimental.pallas import tpu as pltpu
from jax.sharding import PartitionSpec as P


RING = 4
LANES = 128
MIB = 1 << 20


SHIFTS = (0, 1, -1, 2, -2, 3, -3, 4)
GROUPS = ((0, 1, 2, 3, 4), (5, 6, 7))


def shift(x, axis, step):
    n = lax.axis_size(axis)
    return lax.ppermute(x, axis, [(i, (i + step) % n) for i in range(n)])


def shift_z(x, step):
    n = lax.axis_size("ep")
    return lax.ppermute(x, "ep", [(i, (i + 2 * step) % n) for i in range(n)])


def swap_cores(x):
    return lax.ppermute(x, "ep", [(i, i ^ 1) for i in range(lax.axis_size("ep"))])


def ring_gather(block, axis):
    half = block.shape[0] // 2
    prev = shift(block, axis, 1)
    following = shift(block, axis, -1)
    far_top = shift(prev[:half], axis, 1)
    far_bottom = shift(following[half:], axis, -1)
    return block, following, far_top, far_bottom, prev


def far_halves(top, bottom, axis):
    return shift(top, axis, 1), shift(bottom, axis, -1)


def neighbours(following, prev, axis):
    return shift(following, axis, 1), shift(prev, axis, -1)


def call(kernel, out_shape, mib=8, **options):
    return pl.pallas_call(
        kernel,
        out_shape=out_shape,
        compiler_params=pltpu.CompilerParams(vmem_limit_bytes=mib * MIB),
        **options,
    )


def bf16(*shape):
    return jax.ShapeDtypeStruct(shape, jnp.bfloat16)


def f32(*shape):
    return jax.ShapeDtypeStruct(shape, jnp.float32)


def dot(left, right, left_dim=1, right_dim=0):
    return lax.dot_general(
        left, right, (((left_dim,), (right_dim,)), ((), ())), preferred_element_type=jnp.float32
    )


def add_half(whole, half, index, start=0):
    rows, columns = whole.shape
    rows //= 2
    blocks = max(rows // 512, 1)
    rows //= blocks

    def kernel(whole_ref, half_ref, out_ref):
        first = pl.multiple_of(start + pl.program_id(0) * rows, 16)
        total = whole_ref[...].astype(jnp.float32)
        total += half_ref[pl.ds(first, rows)].astype(jnp.float32)
        out_ref[...] = total.astype(jnp.bfloat16)

    spec = pl.BlockSpec((rows, columns), lambda i: (index * blocks + i, 0))
    return call(
        kernel,
        bf16(*whole.shape),
        grid=(blocks,),
        in_specs=[spec, pl.BlockSpec(memory_space=pltpu.VMEM)],
        out_specs=spec,
        input_output_aliases={0: 0},
    )(whole, half)


def pack(w_gate, w_up, w_down):
    depth, width = w_gate.shape

    def kernel(gate_ref, up_ref, down_ref, out_ref):
        out_ref[:depth] = gate_ref[...]
        out_ref[depth : 2 * depth] = up_ref[...]
        out_ref[2 * depth :] = down_ref[...].T

    return call(kernel, bf16(3 * depth, width))(
        *(pltpu.with_memory_space_constraint(w, pltpu.HBM) for w in (w_gate, w_up, w_down))
    )


def weight_parts(refs, r, depth):
    half = depth // 2
    if r == 2:
        top, bottom = refs[2], refs[3]
        return [(top, 0, depth)], [(top, depth, half), (bottom, 0, half)], [(bottom, half, depth)]
    ref = refs[(0, 1, None, 4)[r]]
    return tuple([(ref, i * depth, depth)] for i in range(3))


def start_select(refs, r, out_ref, sem, depth):
    for k in range(RING):

        @pl.when(r == k)
        def _():
            if k == 2:
                rows = 3 * depth // 2
                pieces = [(refs[2], 0, rows), (refs[3], rows, 2 * depth - rows)]
            else:
                pieces = [(refs[(0, 1, None, 4)[k]], 0, 2 * depth)]
            for ref, first, count in pieces:
                source = ref.at[pl.ds(0, count)]
                pltpu.make_async_copy(source, out_ref.at[pl.ds(first, count)], sem).start()


def wait_select(out_ref, sem):
    pltpu.make_async_copy(out_ref, out_ref, sem).wait()


def fill_rows(here_ref, x_ref, rows_ref):
    capacity = x_ref.shape[3]
    z, core = here_ref[2], here_ref[3]
    count = len(SHIFTS)
    for j, step in enumerate(SHIFTS):
        for k in range(2):
            source = ((z - step + count) % count) * 2 + (core if k == 0 else 1 - core)
            rows_ref[pl.ds((2 * j + k) * capacity, capacity)] = x_ref[0, source, 0]


def activations(here, routed_inputs, weights, width):
    _, sources, _, capacity, model_width = routed_inputs.shape
    depth = model_width // RING
    slots = sources * capacity

    def kernel(here_ref, x_ref, *refs):
        weight_refs, (hidden_ref, silu_ref, slope_ref) = refs[:5], refs[5:8]
        x, total, chosen, sems = refs[8:]
        step = pl.program_id(0)
        now = step % 2

        def start(r):
            start_select(weight_refs, r, chosen.at[r % 2], sems.at[r % 2], depth)

        @pl.when(step == 0)
        def _():
            start(step)

        @pl.when(step < RING - 1)
        def _():
            start(step + 1)

        @pl.when(step == 0)
        def _():
            total[...] = jnp.zeros_like(total)

        fill_rows(here_ref, x_ref, x)
        wait_select(chosen.at[now], sems.at[now])

        def add(k, carry):
            rows = pl.ds(pl.multiple_of(k * depth, depth), depth)
            total[k] += dot(x[...], chosen[now, rows])
            return carry

        lax.fori_loop(0, 2, add, 0)

        @pl.when(step == RING - 1)
        def _():
            gate_act, up_act = total[0], total[1]
            sigmoid_gate = jax.nn.sigmoid(gate_act)
            silu_gate = gate_act * sigmoid_gate
            hidden_ref[...] = (silu_gate * up_act).astype(jnp.bfloat16)
            silu_ref[...] = silu_gate
            slope_ref[...] = up_act * sigmoid_gate * (1.0 + gate_act * (1.0 - sigmoid_gate))

    whole = pl.BlockSpec(memory_space=pltpu.VMEM)
    return call(
        kernel,
        (bf16(slots, width), f32(slots, width), f32(slots, width)),
        mib=18,
        grid_spec=pltpu.PrefetchScalarGridSpec(
            num_scalar_prefetch=1,
            grid=(RING,),
            in_specs=[
                pl.BlockSpec(
                    (1, sources, 1, capacity, depth),
                    lambda i, here: (0, 0, 0, 0, (here[0] + i) % RING),
                )
            ]
            + [whole] * 5,
            out_specs=(pl.BlockSpec((slots, width), lambda i, here: (0, 0)),) * 3,
            scratch_shapes=[pltpu.VMEM((slots, depth), jnp.bfloat16)]
            + [pltpu.VMEM((2, slots, width), jnp.float32)]
            + [pltpu.VMEM((2, 2 * depth, width), jnp.bfloat16), pltpu.SemaphoreType.DMA((2,))],
        ),
    )(here, routed_inputs, *weights)


def pair_gradients(here, arrays, places, weights, hidden, silu, slope, groups):
    slots, width = hidden.shape
    depth = arrays[0].shape[1]
    spans, at = [], 0
    for rows in groups:
        spans.append((at, rows))
        at += rows

    def kernel(here_ref, *refs):
        scaled_refs, refs = refs[: len(arrays)], refs[len(arrays) :]
        weight_refs, (hidden_ref, silu_ref, slope_ref) = refs[:5], refs[5:8]
        pair_ref, extra_ref, by_r, top_ref, bottom_ref = refs[8:13]
        chosen, downs, hidden_grad_ref, chosen_sem, sems = refs[13:]
        t = here_ref[1]
        for array, first, q, slot, count in places:
            r = (t + q) % RING
            source = scaled_refs[array].at[pl.ds(first, count)]
            pltpu.make_async_copy(source, by_r.at[r, pl.ds(slot, count)], sems.at[0, r]).start()
        for r in range(RING):
            ((ref, first, count),) = weight_parts(weight_refs, r, depth)[2]
            pltpu.make_async_copy(ref.at[pl.ds(first, count)], downs.at[r], sems.at[1, r]).start()
        start_select(weight_refs, (t + 2) % RING, chosen, chosen_sem, depth)
        hidden_grad_ref[...] = jnp.zeros_like(hidden_grad_ref)

        def add_columns(r, carry):
            pltpu.make_async_copy(by_r.at[r], by_r.at[r], sems.at[0, r]).wait()
            pltpu.make_async_copy(downs.at[r], downs.at[r], sems.at[1, r]).wait()
            hidden_grad_ref[...] += dot(by_r[r], downs[r])
            return carry

        lax.fori_loop(0, RING, add_columns, 0)
        hidden_grad = hidden_grad_ref[...]
        products = jnp.sum(
            hidden_grad * hidden_ref[...].astype(jnp.float32), axis=1, keepdims=True
        )
        high = products.astype(jnp.bfloat16).astype(jnp.float32)
        lane = lax.broadcasted_iota(jnp.int32, (slots, LANES), 1)
        extra = jnp.where(lane == 0, high, jnp.where(lane == 1, products - high, 0.0))
        extra_ref[...] = extra.astype(jnp.bfloat16)
        pair_ref[:, :width] = (hidden_grad * slope_ref[...]).astype(jnp.bfloat16)
        pair_ref[:, width:] = (hidden_grad * silu_ref[...]).astype(jnp.bfloat16)
        wait_select(chosen, chosen_sem)

        def put(columns, value):
            for start, rows in spans:
                middle = start + rows // 2
                half = pl.ds(start // 2, rows // 2)
                top_ref[half, columns] = value[start:middle]
                bottom_ref[half, columns] = value[middle : start + rows]

        slot_part(pair_ref, chosen, depth, put)

    anywhere = pl.BlockSpec(memory_space=pl.ANY)
    whole = pl.BlockSpec(memory_space=pltpu.VMEM)
    outs = [bf16(slots, 2 * width), bf16(slots, LANES), bf16(RING, slots, depth)]
    outs += [bf16(slots // 2, depth)] * 2
    return call(
        kernel,
        tuple(outs),
        mib=24,
        grid_spec=pltpu.PrefetchScalarGridSpec(
            num_scalar_prefetch=1,
            grid=(1,),
            in_specs=[anywhere] * len(arrays) + [whole] * 8,
            out_specs=(whole,) * len(outs),
            scratch_shapes=[
                pltpu.VMEM((2 * depth, width), jnp.bfloat16),
                pltpu.VMEM((RING, depth, width), jnp.bfloat16),
                pltpu.VMEM((slots, width), jnp.float32),
                pltpu.SemaphoreType.DMA,
                pltpu.SemaphoreType.DMA((2, RING)),
            ],
        ),
    )(here, *arrays, *weights, hidden, silu, slope)


def slot_part(pair_ref, weights, depth, put):
    half = depth // 2
    width = pair_ref.shape[1] // 2

    def columns(i, carry):
        at = pl.multiple_of(i * half, half)
        value = dot(pair_ref[:, :width], weights[pl.ds(at, half)], 1, 1)
        value += dot(pair_ref[:, width:], weights[pl.ds(depth + at, half)], 1, 1)
        put(pl.ds(at, half), value.astype(jnp.bfloat16))
        return carry

    lax.fori_loop(0, 2, columns, 0)


def slot_gradients(here, pair, weights, groups):
    slots = pair.shape[0]
    width = pair.shape[1] // 2
    depth = weights[0].shape[0] // 3
    spans, at = [], 0
    for rows in groups:
        spans.append(slice(at, at + rows))
        at += rows

    def kernel(here_ref, pair_ref, *refs):
        weight_refs, out_refs, (parts, chosen, sems) = refs[:5], refs[5:-3], refs[-3:]
        t, step = here_ref[1], pl.program_id(0)

        def start(i):
            q = i + i // 2
            start_select(weight_refs, (t + q) % RING, chosen.at[i % 2], sems.at[i % 2], depth)

        @pl.when(step == 0)
        def _():
            start(0)
            start(1)

        now = step % 2
        wait_select(chosen.at[now], sems.at[now])

        def put(columns, value):
            parts[step, :, columns] = value

        slot_part(pair_ref, chosen.at[now], depth, put)

        @pl.when(step == 0)
        def _():
            start(2)

        @pl.when(step == 2)
        def _():
            for i, span in enumerate(spans):
                for j in range(3):
                    out_refs[3 * i + j][...] = parts[j, span]

    whole = pl.BlockSpec(memory_space=pltpu.VMEM)
    outs = tuple(bf16(rows, depth) for rows in groups for _ in range(3))
    parts = call(
        kernel,
        outs,
        mib=17,
        grid_spec=pltpu.PrefetchScalarGridSpec(
            num_scalar_prefetch=1,
            grid=(3,),
            in_specs=[whole] * 6,
            out_specs=(whole,) * len(outs),
            scratch_shapes=[
                pltpu.VMEM((3, slots, depth), jnp.bfloat16),
                pltpu.VMEM((2, 2 * depth, width), jnp.bfloat16),
                pltpu.SemaphoreType.DMA((2,)),
            ],
        ),
    )(here, pair, *weights)
    return [parts[3 * i : 3 * i + 3] for i in range(len(groups))]


def weight_chunk(here, distances, routed_inputs, hidden, pair, scaled, received=None):
    _, sources, _, capacity, model_width = routed_inputs.shape
    depth = model_width // RING
    slots, width = hidden.shape
    half = depth // 2
    received = received or ()
    near = len(distances) == 2

    def distance(i):
        return distances[0] + 2 * i if near else distances[0]

    def kernel(here_ref, x_ref, hidden_ref, pair_ref, scaled_ref, *refs):
        x, refs = refs[-1], refs[:-1]
        fill_rows(here_ref, x_ref, x)

        def put(at, value):
            place = pl.ds(at, value.shape[0])
            if received:
                value += refs[0][place].astype(jnp.float32) + refs[1][place].astype(jnp.float32)
                for i in range(2):

                    @pl.when((at >= i * depth) & (at < (i + 1) * depth))
                    def _():
                        refs[2 + i][pl.ds(at - i * depth, value.shape[0])] = value

                return value
            if near:
                for i in range(2):

                    @pl.when(pl.program_id(0) == i)
                    def _():
                        refs[i][place] = value.astype(jnp.bfloat16)

                return value
            for i in range(2):

                @pl.when((at >= 3 * i * half) & (at < 3 * (i + 1) * half))
                def _():
                    start = at - 3 * i * half
                    refs[i][pl.ds(start, value.shape[0])] = value.astype(jnp.bfloat16)

            return value

        def inputs_part(i, carry):
            columns = pl.ds(pl.multiple_of((i % 2) * half, half), half)
            lanes = pl.ds(pl.multiple_of((i // 2) * width, width), width)
            put(pl.multiple_of(i * half, half), dot(x[:, columns], pair_ref[:, lanes], 0, 0))
            return carry

        def down_part(c, carry):
            lanes = pl.ds(pl.multiple_of(c * width, width), width)
            value = dot(hidden_ref[...], scaled_ref[0, :, lanes], 0, 0)
            at = pl.multiple_of(2 * depth + c * width, width)
            value = put(at, value)
            if received:
                refs[4][:, lanes] = value
            return carry

        lax.fori_loop(0, 4, inputs_part, 0)
        lax.fori_loop(0, depth // width, down_part, 0)

    whole = pl.BlockSpec(memory_space=pltpu.VMEM)
    if received:
        outs = (f32(depth, width), f32(depth, width), f32(width, depth))
    elif near:
        outs = (bf16(6 * half, width),) * 2
    else:
        outs = (bf16(3 * half, width),) * 2
    return call(
        kernel,
        outs,
        mib=18 if received else 14,
        grid_spec=pltpu.PrefetchScalarGridSpec(
            num_scalar_prefetch=1,
            grid=(len(distances),),
            in_specs=[
                pl.BlockSpec(
                    (1, sources, 1, capacity, depth),
                    lambda i, here: (0, 0, 0, 0, (here[0] + distance(i)) % RING),
                ),
                whole,
                whole,
                pl.BlockSpec((1, slots, depth), lambda i, here: (distance(i), 0, 0)),
            ]
            + [whole] * len(received),
            out_specs=(whole,) * len(outs),
            scratch_shapes=[pltpu.VMEM((slots, depth), jnp.bfloat16)],
        ),
    )(here, routed_inputs, hidden, pair, scaled, *received)


def join(outs):
    arrays = []
    for out in outs:
        for array, _, _ in out:
            if not any(array is a for a in arrays):
                arrays.append(array)
    index = {id(a): i for i, a in enumerate(arrays)}

    def kernel(*refs):
        for out, out_ref in zip(outs, refs[len(arrays) :]):
            at = 0
            for array, first, rows in out:
                out_ref[pl.ds(at, rows)] = refs[index[id(array)]][first : first + rows]
                at += rows

    columns = arrays[0].shape[1]
    shapes = tuple(bf16(sum(rows for _, _, rows in out), columns) for out in outs)
    return call(kernel, shapes)(*arrays)


def messages(own, other):
    count = len(SHIFTS)
    rows, columns = own.shape
    rows //= count

    def kernel(own_ref, other_ref, *out_refs):
        for j, out_ref in enumerate(out_refs):
            out_ref[:rows] = own_ref[j * rows : (j + 1) * rows]
            out_ref[rows:] = other_ref[j * rows : (j + 1) * rows]

    return call(kernel, (bf16(2 * rows, columns),) * count)(own, other)


def unpack_messages(blocks):
    rows, columns = blocks[0].shape
    rows //= 2

    def kernel(*refs):
        own_ref, other_ref = refs[-2:]
        for j, ref in enumerate(refs[:-2]):
            own_ref[pl.ds(j * rows, rows)] = ref[:rows]
            other_ref[pl.ds(j * rows, rows)] = ref[rows:]

    return call(kernel, (bf16(len(blocks) * rows, columns),) * 2)(*blocks)


def leaving_rows(own, from_prev, from_next, extra, start, count):
    rows, narrow = own.shape
    rows //= count

    def kernel(own_ref, prev_ref, next_ref, extra_ref, *out_refs):
        for j, out_ref in enumerate(out_refs):
            span = slice(j * rows, (j + 1) * rows)
            total = own_ref[span].astype(jnp.float32) + prev_ref[span].astype(jnp.float32)
            total += next_ref[span].astype(jnp.float32)
            out_ref[:, :narrow] = total.astype(jnp.bfloat16)
            out_ref[:, narrow:] = extra_ref[start + j * rows : start + (j + 1) * rows]

    outs = (bf16(rows, narrow + LANES),) * count
    return call(kernel, outs)(own, from_prev, from_next, extra)


def routed_rows(here, slot_index, gate_probs, out_grad, slots):
    tokens, model_width = out_grad.shape
    narrow = model_width // RING
    wide = narrow // RING
    half = slots // 2

    def kernel(here_ref, slot_ref, probs_ref, grad_ref, own_ref, other_ref, weighted):
        piece = grad_ref[...].astype(jnp.float32)
        for k in range(2):
            weighted[k] = (probs_ref[:, k : k + 1] * piece).astype(jnp.bfloat16)

        def fill(step, carry):
            h = step // RING
            lanes = pl.ds(pl.multiple_of((step % RING) * wide, wide), wide)
            slot = lax.broadcasted_iota(jnp.int32, (tokens, half), 1) + h * half
            total = jnp.zeros((half, wide), jnp.float32)
            for k in range(2):
                picks = jnp.where(slot_ref[:, k : k + 1] == slot, 1.0, 0.0).astype(jnp.bfloat16)
                total += dot(picks, weighted[k, :, lanes], 0, 0)
            for i, ref in enumerate((own_ref, other_ref)):

                @pl.when(h == i)
                def _():
                    ref[:, lanes] = total.astype(jnp.bfloat16)

            return carry

        lax.fori_loop(0, 2 * RING, fill, 0)

    whole = pl.BlockSpec(memory_space=pltpu.VMEM)
    return call(
        kernel,
        (bf16(half, narrow),) * 2,
        grid_spec=pltpu.PrefetchScalarGridSpec(
            num_scalar_prefetch=1,
            grid=(1,),
            in_specs=[
                whole,
                whole,
                pl.BlockSpec((tokens, narrow), lambda i, here: (0, (here[0] + here[1]) % RING)),
            ],
            out_specs=(whole,) * 2,
            scratch_shapes=[pltpu.VMEM((2, tokens, narrow), jnp.bfloat16)],
        ),
    )(here, slot_index, gate_probs, out_grad)


def token_rows(slot_index, back):
    tokens = slot_index.shape[0]
    rows, wide = back[0].shape
    narrow = wide - LANES

    def kernel(slot_ref, *refs):
        out_ref = refs[-1]
        total = jnp.zeros((tokens, narrow), jnp.float32)
        chosen = [jnp.zeros((tokens, LANES), jnp.float32)] * 2
        for h, back_ref in enumerate(refs[:-1]):
            slot = lax.broadcasted_iota(jnp.int32, (tokens, rows), 1) + h * rows
            picks = [
                jnp.where(slot_ref[:, k : k + 1] == slot, 1.0, 0.0).astype(jnp.bfloat16)
                for k in range(2)
            ]
            total += dot(picks[0] + picks[1], back_ref[:, :narrow])
            chosen = [c + dot(p, back_ref[:, narrow:]) for c, p in zip(chosen, picks)]
        out_ref[:, :narrow] = total.astype(jnp.bfloat16)
        lane = lax.broadcasted_iota(jnp.int32, (tokens, LANES), 1)
        tail = jnp.zeros((tokens, LANES), jnp.float32)
        for k in range(2):
            value = chosen[k][:, 0:1] + chosen[k][:, 1:2]
            high = value.astype(jnp.bfloat16).astype(jnp.float32)
            tail = jnp.where(lane == 2 * k, high, jnp.where(lane == 2 * k + 1, value - high, tail))
        out_ref[:, narrow:] = tail.astype(jnp.bfloat16)

    return call(kernel, bf16(tokens, wide))(slot_index, *back)


def finish_tokens(here, gate_probs, gathered):
    tokens, wide = gathered[0].shape
    narrow = wide - LANES

    def kernel(here_ref, probs_ref, *refs):
        out_ref, logit_ref = refs[RING:]
        total = jnp.zeros((tokens, LANES), jnp.float32)
        for q in range(RING):
            first = ((here_ref[0] + here_ref[1] + q) % RING) * narrow
            out_ref[:, pl.ds(pl.multiple_of(first, LANES), narrow)] = refs[q][:, :narrow]
            total += refs[q][:, narrow:].astype(jnp.float32)
        chosen = [
            (total[:, 2 * k : 2 * k + 1] + total[:, 2 * k + 1 : 2 * k + 2])
            .astype(jnp.bfloat16)
            .astype(jnp.float32)
            for k in range(2)
        ]
        both = chosen[0] + chosen[1]
        for k in range(2):
            logit_ref[:, k : k + 1] = chosen[k] - probs_ref[:, k : k + 1] * both

    whole = pl.BlockSpec(memory_space=pltpu.VMEM)
    return call(
        kernel,
        (bf16(tokens, RING * narrow), f32(tokens, 2)),
        grid_spec=pltpu.PrefetchScalarGridSpec(
            num_scalar_prefetch=1,
            grid=(1,),
            in_specs=[whole] * (RING + 1),
            out_specs=(whole,) * 2,
        ),
    )(here, gate_probs, *gathered)


def slots_of(routes, z, core, capacity, experts):
    tokens = routes.shape[0]
    hot = (routes[:, :, None] == jnp.arange(experts, dtype=jnp.int32)).astype(jnp.bfloat16)
    before = jnp.arange(tokens)[:, None] > jnp.arange(tokens)[None, :]
    earlier = dot(before.astype(jnp.bfloat16), hot[:, 0] + hot[:, 1])
    place = jnp.sum(earlier[:, None, :] * hot.astype(jnp.float32), axis=2).astype(jnp.int32)
    count = len(SHIFTS)
    distance = (routes // 2 - z + count) % count
    index = jnp.where(
        distance <= count // 2, jnp.maximum(2 * distance - 1, 0), 2 * (count - distance)
    )
    other = (routes % 2 != core).astype(jnp.int32)
    return (other * count + index) * capacity + place


def layer(out_grad, routes, chosen_logits, routed_inputs, w_gate, w_up, w_down):
    experts = lax.axis_size("ep")
    f, t = lax.axis_index("fsdp"), lax.axis_index("tp")
    z, core = lax.axis_index("ep") // 2, lax.axis_index("ep") % 2
    here = jnp.stack([f, t, z, core]).astype(jnp.int32)
    capacity = routed_inputs.shape[3]
    slots = experts * capacity
    width = w_gate.shape[2]
    block = 2 * capacity

    weights = ring_gather(pack(w_gate[0], w_up[0], w_down[0]), "fsdp")

    gate_probs = jax.nn.softmax(chosen_logits, axis=-1)
    slot_index = slots_of(routes, z, core, capacity, experts)
    own, other = routed_rows(here, slot_index, gate_probs, out_grad, slots)
    other = swap_cores(other)
    sent = messages(own, other)
    arrived = [sent[0]] + [shift_z(sent[j], SHIFTS[j]) for j in range(1, len(SHIFTS))]
    groups = [len(group) * block for group in GROUPS]
    count0, count1 = groups
    half = count0 // 2
    own0 = join([[(arrived[j], 0, block) for j in GROUPS[0]]])[0]
    prev0, next0 = shift(own0, "tp", 1), shift(own0, "tp", -1)
    pieces = [(arrived[j], 0, block) for j in GROUPS[1]]
    own1, prev1, next1 = join(
        [pieces, pieces + [(prev0, 0, half)], pieces + [(next0, half, half)]]
    )
    prev1, next1 = shift(prev1, "tp", 1), shift(next1, "tp", -1)
    far1 = shift(own1, "tp", 2)
    arrays = [own0, next0, prev0, own1, next1, prev1, far1]
    places = [(0, 0, 0, 0, count0), (1, 0, 1, 0, count0), (2, 0, 3, 0, count0)]
    places += [(3, 0, 0, count0, count1), (4, 0, 1, count0, count1), (5, 0, 3, count0, count1)]
    places += [(5, count1, 2, 0, half), (4, count1, 2, half, half), (6, 0, 2, count0, count1)]

    hidden, silu, slope = activations(here, routed_inputs, weights, width)
    pair, extra, scaled, *far = pair_gradients(
        here, arrays, places, weights, hidden, silu, slope, groups
    )
    far = far_halves(*far, "tp")
    parts = slot_gradients(here, pair, weights, groups)
    leaving = []
    for g, group in enumerate(GROUPS):
        own, following, prev = parts[g]
        start = group[0] * block
        following = add_half(following, far[0], 0, start // 2)
        prev = add_half(prev, far[1], 1, start // 2)
        received = neighbours(following, prev, "tp")
        leaving += leaving_rows(own, *received, extra, start, len(group))

    chunk = functools.partial(
        weight_chunk, here, routed_inputs=routed_inputs, hidden=hidden, pair=pair, scaled=scaled
    )
    far = far_halves(*chunk((2,)), "fsdp")
    following, prev = chunk((1, 3))
    received = neighbours(add_half(following, far[0], 0), add_half(prev, far[1], 1), "fsdp")
    grad_gate, grad_up, grad_down = chunk((0,), received=received)

    returned = [leaving[0]] + [shift_z(leaving[j], -SHIFTS[j]) for j in range(1, len(SHIFTS))]
    own, other = unpack_messages(returned)
    mine = token_rows(slot_index, [own, swap_cores(other)])
    tokens_by_ring = [mine] + [shift(mine, "tp", -q) for q in range(1, RING)]
    input_grad, logit_grad = finish_tokens(here, gate_probs, tokens_by_ring)
    return input_grad, logit_grad, grad_gate[None], grad_up[None], grad_down[None]


def solution(mesh):
    return jax.shard_map(
        layer,
        mesh=mesh,
        in_specs=(
            P(("ep", "fsdp"), None),
            P(("ep", "fsdp"), None),
            P(("ep", "fsdp"), None),
            P("ep", None, "fsdp", None, None),
            P("ep", "fsdp", "tp"),
            P("ep", "fsdp", "tp"),
            P("ep", "tp", "fsdp"),
        ),
        out_specs=(
            P(("ep", "fsdp"), None),
            P(("ep", "fsdp"), None),
            P("ep", "fsdp", "tp"),
            P("ep", "fsdp", "tp"),
            P("ep", "tp", "fsdp"),
        ),
        check_vma=False,
    )
```

```python
import functools

import jax
import jax.numpy as jnp
from jax import lax
from jax.experimental import pallas as pl
from jax.experimental.pallas import tpu as pltpu
from jax.sharding import PartitionSpec as P


RING = 4
LANES = 128
MIB = 1 << 20


SHIFTS = (0, 1, -1, 2, -2, 3, -3, 4)
GROUPS = ((0, 1, 2, 3, 4), (5, 6, 7))


def shift(x, axis, step):
    n = lax.axis_size(axis)
    return lax.ppermute(x, axis, [(i, (i + step) % n) for i in range(n)])


def shift_z(x, step):
    n = lax.axis_size("ep")
    return lax.ppermute(x, "ep", [(i, (i + 2 * step) % n) for i in range(n)])


def swap_cores(x):
    return lax.ppermute(x, "ep", [(i, i ^ 1) for i in range(lax.axis_size("ep"))])


def ring_gather(block, axis):
    half = block.shape[0] // 2
    prev = shift(block, axis, 1)
    following = shift(block, axis, -1)
    far_top = shift(prev[:half], axis, 1)
    far_bottom = shift(following[half:], axis, -1)
    return block, following, far_top, far_bottom, prev


def far_halves(top, bottom, axis):
    return shift(top, axis, 1), shift(bottom, axis, -1)


def neighbours(following, prev, axis):
    return shift(following, axis, 1), shift(prev, axis, -1)


def call(kernel, out_shape, mib=8, **options):
    return pl.pallas_call(
        kernel,
        out_shape=out_shape,
        compiler_params=pltpu.CompilerParams(vmem_limit_bytes=mib * MIB),
        **options,
    )


def bf16(*shape):
    return jax.ShapeDtypeStruct(shape, jnp.bfloat16)


def f32(*shape):
    return jax.ShapeDtypeStruct(shape, jnp.float32)


def dot(left, right, left_dim=1, right_dim=0):
    return lax.dot_general(
        left, right, (((left_dim,), (right_dim,)), ((), ())), preferred_element_type=jnp.float32
    )


def add_half(whole, half, index, start=0):
    rows, columns = whole.shape
    rows //= 2
    blocks = max(rows // 512, 1)
    rows //= blocks

    def kernel(whole_ref, half_ref, out_ref):
        first = pl.multiple_of(start + pl.program_id(0) * rows, 16)
        total = whole_ref[...].astype(jnp.float32)
        total += half_ref[pl.ds(first, rows)].astype(jnp.float32)
        out_ref[...] = total.astype(jnp.bfloat16)

    spec = pl.BlockSpec((rows, columns), lambda i: (index * blocks + i, 0))
    return call(
        kernel,
        bf16(*whole.shape),
        grid=(blocks,),
        in_specs=[spec, pl.BlockSpec(memory_space=pltpu.VMEM)],
        out_specs=spec,
        input_output_aliases={0: 0},
    )(whole, half)


def pack(w_gate, w_up, w_down):
    depth, width = w_gate.shape

    def kernel(gate_ref, up_ref, down_ref, out_ref):
        out_ref[:depth] = gate_ref[...]
        out_ref[depth : 2 * depth] = up_ref[...]
        out_ref[2 * depth :] = down_ref[...].T

    return call(kernel, bf16(3 * depth, width))(
        *(pltpu.with_memory_space_constraint(w, pltpu.HBM) for w in (w_gate, w_up, w_down))
    )


def weight_parts(refs, r, depth):
    half = depth // 2
    if r == 2:
        top, bottom = refs[2], refs[3]
        return [(top, 0, depth)], [(top, depth, half), (bottom, 0, half)], [(bottom, half, depth)]
    ref = refs[(0, 1, None, 4)[r]]
    return tuple([(ref, i * depth, depth)] for i in range(3))


def start_select(refs, r, out_ref, sem, depth):
    for k in range(RING):

        @pl.when(r == k)
        def _():
            if k == 2:
                rows = 3 * depth // 2
                pieces = [(refs[2], 0, rows), (refs[3], rows, 2 * depth - rows)]
            else:
                pieces = [(refs[(0, 1, None, 4)[k]], 0, 2 * depth)]
            for ref, first, count in pieces:
                source = ref.at[pl.ds(0, count)]
                pltpu.make_async_copy(source, out_ref.at[pl.ds(first, count)], sem).start()


def wait_select(out_ref, sem):
    pltpu.make_async_copy(out_ref, out_ref, sem).wait()


def fill_rows(here_ref, x_ref, rows_ref):
    capacity = x_ref.shape[3]
    z, core = here_ref[2], here_ref[3]
    count = len(SHIFTS)
    for j, step in enumerate(SHIFTS):
        for k in range(2):
            source = ((z - step + count) % count) * 2 + (core if k == 0 else 1 - core)
            rows_ref[pl.ds((2 * j + k) * capacity, capacity)] = x_ref[0, source, 0]


def activations(here, routed_inputs, weights, width):
    _, sources, _, capacity, model_width = routed_inputs.shape
    depth = model_width // RING
    slots = sources * capacity

    def kernel(here_ref, x_ref, *refs):
        weight_refs, (hidden_ref, silu_ref, slope_ref) = refs[:5], refs[5:8]
        x, total, chosen, sems = refs[8:]
        step = pl.program_id(0)
        now = step % 2

        def start(r):
            start_select(weight_refs, r, chosen.at[r % 2], sems.at[r % 2], depth)

        @pl.when(step == 0)
        def _():
            start(step)

        @pl.when(step < RING - 1)
        def _():
            start(step + 1)

        @pl.when(step == 0)
        def _():
            total[...] = jnp.zeros_like(total)

        fill_rows(here_ref, x_ref, x)
        wait_select(chosen.at[now], sems.at[now])

        def add(k, carry):
            rows = pl.ds(pl.multiple_of(k * depth, depth), depth)
            total[k] += dot(x[...], chosen[now, rows])
            return carry

        lax.fori_loop(0, 2, add, 0)

        @pl.when(step == RING - 1)
        def _():
            def finish(i, carry):
                rows = pl.ds(pl.multiple_of(i * LANES, LANES), LANES)
                gate_act, up_act = total[0, rows], total[1, rows]
                sigmoid_gate = jax.nn.sigmoid(gate_act)
                silu_gate = gate_act * sigmoid_gate
                hidden_ref[rows] = (silu_gate * up_act).astype(jnp.bfloat16)
                silu_ref[rows] = silu_gate
                slope_ref[rows] = up_act * sigmoid_gate * (1.0 + gate_act * (1.0 - sigmoid_gate))
                return carry

            lax.fori_loop(0, slots // LANES, finish, 0)

    whole = pl.BlockSpec(memory_space=pltpu.VMEM)
    return call(
        kernel,
        (bf16(slots, width), f32(slots, width), f32(slots, width)),
        mib=18,
        grid_spec=pltpu.PrefetchScalarGridSpec(
            num_scalar_prefetch=1,
            grid=(RING,),
            in_specs=[
                pl.BlockSpec(
                    (1, sources, 1, capacity, depth),
                    lambda i, here: (0, 0, 0, 0, (here[0] + i) % RING),
                )
            ]
            + [whole] * 5,
            out_specs=(pl.BlockSpec((slots, width), lambda i, here: (0, 0)),) * 3,
            scratch_shapes=[pltpu.VMEM((slots, depth), jnp.bfloat16)]
            + [pltpu.VMEM((2, slots, width), jnp.float32)]
            + [pltpu.VMEM((2, 2 * depth, width), jnp.bfloat16), pltpu.SemaphoreType.DMA((2,))],
        ),
    )(here, routed_inputs, *weights)


def pair_gradients(here, arrays, places, weights, hidden, silu, slope, groups):
    slots, width = hidden.shape
    depth = arrays[0].shape[1]
    spans, at = [], 0
    for rows in groups:
        spans.append((at, rows))
        at += rows

    def kernel(here_ref, *refs):
        scaled_refs, refs = refs[: len(arrays)], refs[len(arrays) :]
        weight_refs, (hidden_ref, silu_ref, slope_ref) = refs[:5], refs[5:8]
        pair_ref, extra_ref, by_r, top_ref, bottom_ref = refs[8:13]
        chosen, downs, hidden_grad_ref, chosen_sem, sems = refs[13:]
        t = here_ref[1]
        for array, first, q, slot, count in places:
            r = (t + q) % RING
            source = scaled_refs[array].at[pl.ds(first, count)]
            pltpu.make_async_copy(source, by_r.at[r, pl.ds(slot, count)], sems.at[0, r]).start()
        for r in range(RING):
            ((ref, first, count),) = weight_parts(weight_refs, r, depth)[2]
            pltpu.make_async_copy(ref.at[pl.ds(first, count)], downs.at[r], sems.at[1, r]).start()
        start_select(weight_refs, (t + 2) % RING, chosen, chosen_sem, depth)
        hidden_grad_ref[...] = jnp.zeros_like(hidden_grad_ref)

        def add_columns(r, carry):
            pltpu.make_async_copy(by_r.at[r], by_r.at[r], sems.at[0, r]).wait()
            pltpu.make_async_copy(downs.at[r], downs.at[r], sems.at[1, r]).wait()
            hidden_grad_ref[...] += dot(by_r[r], downs[r])
            return carry

        lax.fori_loop(0, RING, add_columns, 0)

        def finish(i, carry):
            rows = pl.ds(pl.multiple_of(i * LANES, LANES), LANES)
            hidden_grad = hidden_grad_ref[rows]
            products = jnp.sum(
                hidden_grad * hidden_ref[rows].astype(jnp.float32), axis=1, keepdims=True
            )
            high = products.astype(jnp.bfloat16).astype(jnp.float32)
            lane = lax.broadcasted_iota(jnp.int32, (LANES, LANES), 1)
            extra = jnp.where(lane == 0, high, jnp.where(lane == 1, products - high, 0.0))
            extra_ref[rows] = extra.astype(jnp.bfloat16)
            pair_ref[rows, :width] = (hidden_grad * slope_ref[rows]).astype(jnp.bfloat16)
            pair_ref[rows, width:] = (hidden_grad * silu_ref[rows]).astype(jnp.bfloat16)
            return carry

        lax.fori_loop(0, slots // LANES, finish, 0)
        wait_select(chosen, chosen_sem)

        def put(columns, value):
            for start, rows in spans:
                middle = start + rows // 2
                half = pl.ds(start // 2, rows // 2)
                top_ref[half, columns] = value[start:middle]
                bottom_ref[half, columns] = value[middle : start + rows]

        slot_part(pair_ref, chosen, depth, put)

    anywhere = pl.BlockSpec(memory_space=pl.ANY)
    whole = pl.BlockSpec(memory_space=pltpu.VMEM)
    outs = [bf16(slots, 2 * width), bf16(slots, LANES), bf16(RING, slots, depth)]
    outs += [bf16(slots // 2, depth)] * 2
    return call(
        kernel,
        tuple(outs),
        mib=24,
        grid_spec=pltpu.PrefetchScalarGridSpec(
            num_scalar_prefetch=1,
            grid=(1,),
            in_specs=[anywhere] * len(arrays) + [whole] * 8,
            out_specs=(whole,) * len(outs),
            scratch_shapes=[
                pltpu.VMEM((2 * depth, width), jnp.bfloat16),
                pltpu.VMEM((RING, depth, width), jnp.bfloat16),
                pltpu.VMEM((slots, width), jnp.float32),
                pltpu.SemaphoreType.DMA,
                pltpu.SemaphoreType.DMA((2, RING)),
            ],
        ),
    )(here, *arrays, *weights, hidden, silu, slope)


def slot_part(pair_ref, weights, depth, put):
    half = depth // 2
    width = pair_ref.shape[1] // 2

    def columns(i, carry):
        at = pl.multiple_of(i * half, half)
        value = dot(pair_ref[:, :width], weights[pl.ds(at, half)], 1, 1)
        value += dot(pair_ref[:, width:], weights[pl.ds(depth + at, half)], 1, 1)
        put(pl.ds(at, half), value.astype(jnp.bfloat16))
        return carry

    lax.fori_loop(0, 2, columns, 0)


def slot_gradients(here, pair, weights, groups):
    slots = pair.shape[0]
    width = pair.shape[1] // 2
    depth = weights[0].shape[0] // 3
    spans, at = [], 0
    for rows in groups:
        spans.append(slice(at, at + rows))
        at += rows

    def kernel(here_ref, pair_ref, *refs):
        weight_refs, out_refs, (parts, chosen, sems) = refs[:5], refs[5:-3], refs[-3:]
        t, step = here_ref[1], pl.program_id(0)

        def start(i):
            q = i + i // 2
            start_select(weight_refs, (t + q) % RING, chosen.at[i % 2], sems.at[i % 2], depth)

        @pl.when(step == 0)
        def _():
            start(0)
            start(1)

        now = step % 2
        wait_select(chosen.at[now], sems.at[now])

        def put(columns, value):
            parts[step, :, columns] = value

        slot_part(pair_ref, chosen.at[now], depth, put)

        @pl.when(step == 0)
        def _():
            start(2)

        @pl.when(step == 2)
        def _():
            for i, span in enumerate(spans):
                for j in range(3):

                    def copy_rows(k, carry):
                        at = pl.multiple_of(k * 64, 64)
                        out_refs[3 * i + j][pl.ds(at, 64)] = parts[j, pl.ds(span.start + at, 64)]
                        return carry

                    lax.fori_loop(0, (span.stop - span.start) // 64, copy_rows, 0)

    whole = pl.BlockSpec(memory_space=pltpu.VMEM)
    outs = tuple(bf16(rows, depth) for rows in groups for _ in range(3))
    parts = call(
        kernel,
        outs,
        mib=17,
        grid_spec=pltpu.PrefetchScalarGridSpec(
            num_scalar_prefetch=1,
            grid=(3,),
            in_specs=[whole] * 6,
            out_specs=(whole,) * len(outs),
            scratch_shapes=[
                pltpu.VMEM((3, slots, depth), jnp.bfloat16),
                pltpu.VMEM((2, 2 * depth, width), jnp.bfloat16),
                pltpu.SemaphoreType.DMA((2,)),
            ],
        ),
    )(here, pair, *weights)
    return [parts[3 * i : 3 * i + 3] for i in range(len(groups))]


def weight_chunk(here, distances, routed_inputs, hidden, pair, scaled, received=None):
    _, sources, _, capacity, model_width = routed_inputs.shape
    depth = model_width // RING
    slots, width = hidden.shape
    half = depth // 2
    received = received or ()
    near = len(distances) == 2

    def distance(i):
        return distances[0] + 2 * i if near else distances[0]

    def kernel(here_ref, x_ref, hidden_ref, pair_ref, scaled_ref, *refs):
        x, refs = refs[-1], refs[:-1]
        fill_rows(here_ref, x_ref, x)

        def put(at, value):
            place = pl.ds(at, value.shape[0])
            if received:
                value += refs[0][place].astype(jnp.float32) + refs[1][place].astype(jnp.float32)
                for i in range(2):

                    @pl.when((at >= i * depth) & (at < (i + 1) * depth))
                    def _():
                        refs[2 + i][pl.ds(at - i * depth, value.shape[0])] = value

                return value
            if near:
                for i in range(2):

                    @pl.when(pl.program_id(0) == i)
                    def _():
                        refs[i][place] = value.astype(jnp.bfloat16)

                return value
            for i in range(2):

                @pl.when((at >= 3 * i * half) & (at < 3 * (i + 1) * half))
                def _():
                    start = at - 3 * i * half
                    refs[i][pl.ds(start, value.shape[0])] = value.astype(jnp.bfloat16)

            return value

        def inputs_part(i, carry):
            columns = pl.ds(pl.multiple_of((i % 2) * half, half), half)
            lanes = pl.ds(pl.multiple_of((i // 2) * width, width), width)
            put(pl.multiple_of(i * half, half), dot(x[:, columns], pair_ref[:, lanes], 0, 0))
            return carry

        def down_part(c, carry):
            lanes = pl.ds(pl.multiple_of(c * width, width), width)
            value = dot(hidden_ref[...], scaled_ref[0, :, lanes], 0, 0)
            at = pl.multiple_of(2 * depth + c * width, width)
            value = put(at, value)
            if received:
                refs[4][:, lanes] = value
            return carry

        lax.fori_loop(0, 4, inputs_part, 0)
        lax.fori_loop(0, depth // width, down_part, 0)

    whole = pl.BlockSpec(memory_space=pltpu.VMEM)
    if received:
        outs = (f32(depth, width), f32(depth, width), f32(width, depth))
    elif near:
        outs = (bf16(6 * half, width),) * 2
    else:
        outs = (bf16(3 * half, width),) * 2
    return call(
        kernel,
        outs,
        mib=18 if received else 14,
        grid_spec=pltpu.PrefetchScalarGridSpec(
            num_scalar_prefetch=1,
            grid=(len(distances),),
            in_specs=[
                pl.BlockSpec(
                    (1, sources, 1, capacity, depth),
                    lambda i, here: (0, 0, 0, 0, (here[0] + distance(i)) % RING),
                ),
                whole,
                whole,
                pl.BlockSpec((1, slots, depth), lambda i, here: (distance(i), 0, 0)),
            ]
            + [whole] * len(received),
            out_specs=(whole,) * len(outs),
            scratch_shapes=[pltpu.VMEM((slots, depth), jnp.bfloat16)],
        ),
    )(here, routed_inputs, hidden, pair, scaled, *received)


def join(outs):
    arrays = []
    for out in outs:
        for array, _, _ in out:
            if not any(array is a for a in arrays):
                arrays.append(array)
    index = {id(a): i for i, a in enumerate(arrays)}

    def kernel(*refs):
        for out, out_ref in zip(outs, refs[len(arrays) :]):
            at = 0
            for array, first, rows in out:
                out_ref[pl.ds(at, rows)] = refs[index[id(array)]][first : first + rows]
                at += rows

    columns = arrays[0].shape[1]
    shapes = tuple(bf16(sum(rows for _, _, rows in out), columns) for out in outs)
    return call(kernel, shapes)(*arrays)


def messages(own, other):
    count = len(SHIFTS)
    rows, columns = own.shape
    rows //= count

    def kernel(own_ref, other_ref, *out_refs):
        for j, out_ref in enumerate(out_refs):
            out_ref[:rows] = own_ref[j * rows : (j + 1) * rows]
            out_ref[rows:] = other_ref[j * rows : (j + 1) * rows]

    return call(kernel, (bf16(2 * rows, columns),) * count)(own, other)


def unpack_messages(blocks):
    rows, columns = blocks[0].shape
    rows //= 2

    def kernel(*refs):
        own_ref, other_ref = refs[-2:]
        for j, ref in enumerate(refs[:-2]):
            own_ref[pl.ds(j * rows, rows)] = ref[:rows]
            other_ref[pl.ds(j * rows, rows)] = ref[rows:]

    return call(kernel, (bf16(len(blocks) * rows, columns),) * 2)(*blocks)


def leaving_rows(own, from_prev, from_next, extra, start, count):
    rows, narrow = own.shape
    rows //= count

    def kernel(own_ref, prev_ref, next_ref, extra_ref, *out_refs):
        for j, out_ref in enumerate(out_refs):
            span = slice(j * rows, (j + 1) * rows)
            total = own_ref[span].astype(jnp.float32) + prev_ref[span].astype(jnp.float32)
            total += next_ref[span].astype(jnp.float32)
            out_ref[:, :narrow] = total.astype(jnp.bfloat16)
            out_ref[:, narrow:] = extra_ref[start + j * rows : start + (j + 1) * rows]

    outs = (bf16(rows, narrow + LANES),) * count
    return call(kernel, outs)(own, from_prev, from_next, extra)


def token_rows(slot_index, back):
    tokens = slot_index.shape[0]
    rows, wide = back[0].shape
    narrow = wide - LANES

    def kernel(slot_ref, *refs):
        out_ref = refs[-1]
        total = jnp.zeros((tokens, narrow), jnp.float32)
        chosen = [jnp.zeros((tokens, LANES), jnp.float32)] * 2
        for h, back_ref in enumerate(refs[:-1]):
            slot = lax.broadcasted_iota(jnp.int32, (tokens, rows), 1) + h * rows
            picks = [
                jnp.where(slot_ref[:, k : k + 1] == slot, 1.0, 0.0).astype(jnp.bfloat16)
                for k in range(2)
            ]
            total += dot(picks[0] + picks[1], back_ref[:, :narrow])
            chosen = [c + dot(p, back_ref[:, narrow:]) for c, p in zip(chosen, picks)]
        out_ref[:, :narrow] = total.astype(jnp.bfloat16)
        lane = lax.broadcasted_iota(jnp.int32, (tokens, LANES), 1)
        tail = jnp.zeros((tokens, LANES), jnp.float32)
        for k in range(2):
            value = chosen[k][:, 0:1] + chosen[k][:, 1:2]
            high = value.astype(jnp.bfloat16).astype(jnp.float32)
            tail = jnp.where(lane == 2 * k, high, jnp.where(lane == 2 * k + 1, value - high, tail))
        out_ref[:, narrow:] = tail.astype(jnp.bfloat16)

    return call(kernel, bf16(tokens, wide))(slot_index, *back)


def finish_tokens(here, gate_probs, gathered):
    tokens, wide = gathered[0].shape
    narrow = wide - LANES

    def kernel(here_ref, probs_ref, *refs):
        out_ref, logit_ref = refs[RING:]
        total = jnp.zeros((tokens, LANES), jnp.float32)
        for q in range(RING):
            first = ((here_ref[0] + here_ref[1] + q) % RING) * narrow
            out_ref[:, pl.ds(pl.multiple_of(first, LANES), narrow)] = refs[q][:, :narrow]
            total += refs[q][:, narrow:].astype(jnp.float32)
        chosen = [
            (total[:, 2 * k : 2 * k + 1] + total[:, 2 * k + 1 : 2 * k + 2])
            .astype(jnp.bfloat16)
            .astype(jnp.float32)
            for k in range(2)
        ]
        both = chosen[0] + chosen[1]
        for k in range(2):
            logit_ref[:, k : k + 1] = chosen[k] - probs_ref[:, k : k + 1] * both

    whole = pl.BlockSpec(memory_space=pltpu.VMEM)
    return call(
        kernel,
        (bf16(tokens, RING * narrow), f32(tokens, 2)),
        grid_spec=pltpu.PrefetchScalarGridSpec(
            num_scalar_prefetch=1,
            grid=(1,),
            in_specs=[whole] * (RING + 1),
            out_specs=(whole,) * 2,
        ),
    )(here, gate_probs, *gathered)


def slots_of(routes, z, core, capacity, experts):
    tokens = routes.shape[0]
    hot = (routes[:, :, None] == jnp.arange(experts, dtype=jnp.int32)).astype(jnp.bfloat16)
    before = jnp.arange(tokens)[:, None] > jnp.arange(tokens)[None, :]
    earlier = dot(before.astype(jnp.bfloat16), hot[:, 0] + hot[:, 1])
    place = jnp.sum(earlier[:, None, :] * hot.astype(jnp.float32), axis=2).astype(jnp.int32)
    count = len(SHIFTS)
    distance = (routes // 2 - z + count) % count
    index = jnp.where(
        distance <= count // 2, jnp.maximum(2 * distance - 1, 0), 2 * (count - distance)
    )
    other = (routes % 2 != core).astype(jnp.int32)
    return (other * count + index) * capacity + place


def layer(out_grad, routes, chosen_logits, routed_inputs, w_gate, w_up, w_down):
    experts = lax.axis_size("ep")
    f, t = lax.axis_index("fsdp"), lax.axis_index("tp")
    z, core = lax.axis_index("ep") // 2, lax.axis_index("ep") % 2
    here = jnp.stack([f, t, z, core]).astype(jnp.int32)
    model_width = out_grad.shape[1]
    capacity = routed_inputs.shape[3]
    slots = experts * capacity
    narrow = model_width // RING
    width = w_gate.shape[2]
    block = 2 * capacity

    weights = ring_gather(pack(w_gate[0], w_up[0], w_down[0]), "fsdp")

    gate_probs = jax.nn.softmax(chosen_logits, axis=-1)
    slot_index = slots_of(routes, z, core, capacity, experts)
    piece = lax.dynamic_slice_in_dim(out_grad, ((f + t) % RING) * narrow, narrow, 1)
    weighted = gate_probs[:, :, None] * piece.astype(jnp.float32)[:, None, :]
    weighted = weighted.astype(jnp.bfloat16)

    def routed(first):
        slot = first + jnp.arange(slots // 2, dtype=jnp.int32)
        picks = (slot_index[:, :, None] == slot).astype(jnp.bfloat16)
        return lax.dot_general(
            picks, weighted, (((0, 1), (0, 1)), ((), ())), preferred_element_type=jnp.float32
        ).astype(jnp.bfloat16)

    own, other = routed(0), swap_cores(routed(slots // 2))
    sent = messages(own, other)
    arrived = [sent[0]] + [shift_z(sent[j], SHIFTS[j]) for j in range(1, len(SHIFTS))]
    groups = [len(group) * block for group in GROUPS]
    count0, count1 = groups
    half = count0 // 2
    own0 = join([[(arrived[j], 0, block) for j in GROUPS[0]]])[0]
    prev0, next0 = shift(own0, "tp", 1), shift(own0, "tp", -1)
    pieces = [(arrived[j], 0, block) for j in GROUPS[1]]
    own1, prev1, next1 = join(
        [pieces, pieces + [(prev0, 0, half)], pieces + [(next0, half, half)]]
    )
    prev1, next1 = shift(prev1, "tp", 1), shift(next1, "tp", -1)
    far1 = shift(own1, "tp", 2)
    arrays = [own0, next0, prev0, own1, next1, prev1, far1]
    places = [(0, 0, 0, 0, count0), (1, 0, 1, 0, count0), (2, 0, 3, 0, count0)]
    places += [(3, 0, 0, count0, count1), (4, 0, 1, count0, count1), (5, 0, 3, count0, count1)]
    places += [(5, count1, 2, 0, half), (4, count1, 2, half, half), (6, 0, 2, count0, count1)]

    hidden, silu, slope = activations(here, routed_inputs, weights, width)
    pair, extra, scaled, *far = pair_gradients(
        here, arrays, places, weights, hidden, silu, slope, groups
    )
    far = far_halves(*far, "tp")
    parts = slot_gradients(here, pair, weights, groups)
    leaving = []
    for g, group in enumerate(GROUPS):
        own, following, prev = parts[g]
        start = group[0] * block
        following = add_half(following, far[0], 0, start // 2)
        prev = add_half(prev, far[1], 1, start // 2)
        received = neighbours(following, prev, "tp")
        leaving += leaving_rows(own, *received, extra, start, len(group))

    chunk = functools.partial(
        weight_chunk, here, routed_inputs=routed_inputs, hidden=hidden, pair=pair, scaled=scaled
    )
    far = far_halves(*chunk((2,)), "fsdp")
    following, prev = chunk((1, 3))
    received = neighbours(add_half(following, far[0], 0), add_half(prev, far[1], 1), "fsdp")
    grad_gate, grad_up, grad_down = chunk((0,), received=received)

    returned = [leaving[0]] + [shift_z(leaving[j], -SHIFTS[j]) for j in range(1, len(SHIFTS))]
    own, other = unpack_messages(returned)
    mine = token_rows(slot_index, [own, swap_cores(other)])
    tokens_by_ring = [mine] + [shift(mine, "tp", -q) for q in range(1, RING)]
    input_grad, logit_grad = finish_tokens(here, gate_probs, tokens_by_ring)
    return input_grad, logit_grad, grad_gate[None], grad_up[None], grad_down[None]


def solution(mesh):
    return jax.shard_map(
        layer,
        mesh=mesh,
        in_specs=(
            P(("ep", "fsdp"), None),
            P(("ep", "fsdp"), None),
            P(("ep", "fsdp"), None),
            P("ep", None, "fsdp", None, None),
            P("ep", "fsdp", "tp"),
            P("ep", "fsdp", "tp"),
            P("ep", "tp", "fsdp"),
        ),
        out_specs=(
            P(("ep", "fsdp"), None),
            P(("ep", "fsdp"), None),
            P("ep", "fsdp", "tp"),
            P("ep", "fsdp", "tp"),
            P("ep", "tp", "fsdp"),
        ),
        check_vma=False,
    )
```

```python
import functools

import jax
import jax.numpy as jnp
from jax import lax
from jax.experimental import pallas as pl
from jax.experimental.pallas import tpu as pltpu
from jax.sharding import PartitionSpec as P


RING = 4
LANES = 128
MIB = 1 << 20


SHIFTS = (0, 1, -1, 2, -2, 3, -3, 4)
GROUPS = ((0, 1, 2, 3, 4), (5, 6, 7))


def shift(x, axis, step):
    n = lax.axis_size(axis)
    return lax.ppermute(x, axis, [(i, (i + step) % n) for i in range(n)])


def shift_z(x, step):
    n = lax.axis_size("ep")
    return lax.ppermute(x, "ep", [(i, (i + 2 * step) % n) for i in range(n)])


def swap_cores(x):
    return lax.ppermute(x, "ep", [(i, i ^ 1) for i in range(lax.axis_size("ep"))])


def ring_gather(block, axis):
    half = block.shape[0] // 2
    prev = shift(block, axis, 1)
    following = shift(block, axis, -1)
    far_top = shift(prev[:half], axis, 1)
    far_bottom = shift(following[half:], axis, -1)
    return block, following, far_top, far_bottom, prev


def far_halves(top, bottom, axis):
    return shift(top, axis, 1), shift(bottom, axis, -1)


def neighbours(following, prev, axis):
    return shift(following, axis, 1), shift(prev, axis, -1)


def call(kernel, out_shape, mib=8, **options):
    return pl.pallas_call(
        kernel,
        out_shape=out_shape,
        compiler_params=pltpu.CompilerParams(vmem_limit_bytes=mib * MIB),
        **options,
    )


def bf16(*shape):
    return jax.ShapeDtypeStruct(shape, jnp.bfloat16)


def f32(*shape):
    return jax.ShapeDtypeStruct(shape, jnp.float32)


def dot(left, right, left_dim=1, right_dim=0):
    return lax.dot_general(
        left, right, (((left_dim,), (right_dim,)), ((), ())), preferred_element_type=jnp.float32
    )


def add_half(whole, half, index, start=0):
    rows, columns = whole.shape
    rows //= 2
    blocks = max(rows // 512, 1)
    rows //= blocks

    def kernel(whole_ref, half_ref, out_ref):
        first = pl.multiple_of(start + pl.program_id(0) * rows, 16)
        total = whole_ref[...].astype(jnp.float32)
        total += half_ref[pl.ds(first, rows)].astype(jnp.float32)
        out_ref[...] = total.astype(jnp.bfloat16)

    spec = pl.BlockSpec((rows, columns), lambda i: (index * blocks + i, 0))
    return call(
        kernel,
        bf16(*whole.shape),
        grid=(blocks,),
        in_specs=[spec, pl.BlockSpec(memory_space=pltpu.VMEM)],
        out_specs=spec,
        input_output_aliases={0: 0},
    )(whole, half)


def pack(w_gate, w_up, w_down):
    depth, width = w_gate.shape

    def kernel(gate_ref, up_ref, down_ref, out_ref):
        out_ref[:depth] = gate_ref[...]
        out_ref[depth : 2 * depth] = up_ref[...]
        out_ref[2 * depth :] = down_ref[...].T

    return call(kernel, bf16(3 * depth, width))(
        *(pltpu.with_memory_space_constraint(w, pltpu.HBM) for w in (w_gate, w_up, w_down))
    )


def weight_parts(refs, r, depth):
    half = depth // 2
    if r == 2:
        top, bottom = refs[2], refs[3]
        return [(top, 0, depth)], [(top, depth, half), (bottom, 0, half)], [(bottom, half, depth)]
    ref = refs[(0, 1, None, 4)[r]]
    return tuple([(ref, i * depth, depth)] for i in range(3))


def start_select(refs, r, out_ref, sem, depth):
    for k in range(RING):

        @pl.when(r == k)
        def _():
            if k == 2:
                rows = 3 * depth // 2
                pieces = [(refs[2], 0, rows), (refs[3], rows, 2 * depth - rows)]
            else:
                pieces = [(refs[(0, 1, None, 4)[k]], 0, 2 * depth)]
            for ref, first, count in pieces:
                source = ref.at[pl.ds(0, count)]
                pltpu.make_async_copy(source, out_ref.at[pl.ds(first, count)], sem).start()


def wait_select(out_ref, sem):
    pltpu.make_async_copy(out_ref, out_ref, sem).wait()


def fill_rows(here_ref, x_ref, rows_ref):
    capacity = x_ref.shape[3]
    z, core = here_ref[2], here_ref[3]
    count = len(SHIFTS)
    for j, step in enumerate(SHIFTS):
        for k in range(2):
            source = ((z - step + count) % count) * 2 + (core if k == 0 else 1 - core)
            rows_ref[pl.ds((2 * j + k) * capacity, capacity)] = x_ref[0, source, 0]


def activations(here, routed_inputs, weights, width):
    _, sources, _, capacity, model_width = routed_inputs.shape
    depth = model_width // RING
    slots = sources * capacity

    def kernel(here_ref, x_ref, *refs):
        weight_refs, (hidden_ref, silu_ref, slope_ref) = refs[:5], refs[5:8]
        x, total, chosen, sems = refs[8:]
        step = pl.program_id(0)
        now = step % 2

        def start(r):
            start_select(weight_refs, r, chosen.at[r % 2], sems.at[r % 2], depth)

        @pl.when(step == 0)
        def _():
            start(step)

        @pl.when(step < RING - 1)
        def _():
            start(step + 1)

        @pl.when(step == 0)
        def _():
            total[...] = jnp.zeros_like(total)

        fill_rows(here_ref, x_ref, x)
        wait_select(chosen.at[now], sems.at[now])

        def add(k, carry):
            rows = pl.ds(pl.multiple_of(k * depth, depth), depth)
            total[k] += dot(x[...], chosen[now, rows])
            return carry

        lax.fori_loop(0, 2, add, 0)

        @pl.when(step == RING - 1)
        def _():
            def finish(i, carry):
                rows = pl.ds(pl.multiple_of(i * LANES, LANES), LANES)
                gate_act, up_act = total[0, rows], total[1, rows]
                sigmoid_gate = jax.nn.sigmoid(gate_act)
                silu_gate = gate_act * sigmoid_gate
                hidden_ref[rows] = (silu_gate * up_act).astype(jnp.bfloat16)
                silu_ref[rows] = silu_gate
                slope_ref[rows] = up_act * sigmoid_gate * (1.0 + gate_act * (1.0 - sigmoid_gate))
                return carry

            lax.fori_loop(0, slots // LANES, finish, 0)

    whole = pl.BlockSpec(memory_space=pltpu.VMEM)
    return call(
        kernel,
        (bf16(slots, width), f32(slots, width), f32(slots, width)),
        mib=18,
        grid_spec=pltpu.PrefetchScalarGridSpec(
            num_scalar_prefetch=1,
            grid=(RING,),
            in_specs=[
                pl.BlockSpec(
                    (1, sources, 1, capacity, depth),
                    lambda i, here: (0, 0, 0, 0, (here[0] + i) % RING),
                )
            ]
            + [whole] * 5,
            out_specs=(pl.BlockSpec((slots, width), lambda i, here: (0, 0)),) * 3,
            scratch_shapes=[pltpu.VMEM((slots, depth), jnp.bfloat16)]
            + [pltpu.VMEM((2, slots, width), jnp.float32)]
            + [pltpu.VMEM((2, 2 * depth, width), jnp.bfloat16), pltpu.SemaphoreType.DMA((2,))],
        ),
    )(here, routed_inputs, *weights)


def pick_weights(here, weights):
    width = weights[0].shape[1]
    depth = weights[0].shape[0] // 3

    def kernel(here_ref, *refs):
        weight_refs, (downs, chosen, sem, sems) = refs[:5], refs[5:]
        start_select(weight_refs, (here_ref[1] + 2) % RING, chosen, sem, depth)
        copies = []
        for r in range(RING):
            ((ref, first, count),) = weight_parts(weight_refs, r, depth)[2]
            source = ref.at[pl.ds(first, count)]
            copies.append(pltpu.make_async_copy(source, downs.at[r], sems.at[r]))
        for copy in copies:
            copy.start()
        for copy in copies:
            copy.wait()
        wait_select(chosen, sem)

    whole = pl.BlockSpec(memory_space=pltpu.VMEM)
    return call(
        kernel,
        (bf16(RING, depth, width), bf16(2 * depth, width)),
        mib=12,
        grid_spec=pltpu.PrefetchScalarGridSpec(
            num_scalar_prefetch=1,
            grid=(1,),
            in_specs=[whole] * 5,
            out_specs=(whole,) * 2,
            scratch_shapes=[pltpu.SemaphoreType.DMA, pltpu.SemaphoreType.DMA((RING,))],
        ),
    )(here, *weights)


def pair_gradients(here, arrays, places, picked, hidden, silu, slope, groups):
    slots, width = hidden.shape
    depth = arrays[0].shape[1]
    spans, at = [], 0
    for rows in groups:
        spans.append((at, rows))
        at += rows

    def kernel(here_ref, *refs):
        scaled_refs, refs = refs[: len(arrays)], refs[len(arrays) :]
        downs, chosen, hidden_ref, silu_ref, slope_ref = refs[:5]
        pair_ref, extra_ref, by_r, top_ref, bottom_ref, hidden_grad_ref, sems = refs[5:]
        t = here_ref[1]
        for array, first, q, slot, count in places:
            r = (t + q) % RING
            source = scaled_refs[array].at[pl.ds(first, count)]
            pltpu.make_async_copy(source, by_r.at[r, pl.ds(slot, count)], sems.at[r]).start()
        hidden_grad_ref[...] = jnp.zeros_like(hidden_grad_ref)

        def add_columns(r, carry):
            pltpu.make_async_copy(by_r.at[r], by_r.at[r], sems.at[r]).wait()
            hidden_grad_ref[...] += dot(by_r[r], downs[r])
            return carry

        lax.fori_loop(0, RING, add_columns, 0)

        def finish(i, carry):
            rows = pl.ds(pl.multiple_of(i * LANES, LANES), LANES)
            hidden_grad = hidden_grad_ref[rows]
            products = jnp.sum(
                hidden_grad * hidden_ref[rows].astype(jnp.float32), axis=1, keepdims=True
            )
            high = products.astype(jnp.bfloat16).astype(jnp.float32)
            lane = lax.broadcasted_iota(jnp.int32, (LANES, LANES), 1)
            extra = jnp.where(lane == 0, high, jnp.where(lane == 1, products - high, 0.0))
            extra_ref[rows] = extra.astype(jnp.bfloat16)
            pair_ref[rows, :width] = (hidden_grad * slope_ref[rows]).astype(jnp.bfloat16)
            pair_ref[rows, width:] = (hidden_grad * silu_ref[rows]).astype(jnp.bfloat16)
            return carry

        lax.fori_loop(0, slots // LANES, finish, 0)

        def put(columns, value):
            for start, rows in spans:
                middle = start + rows // 2
                half = pl.ds(start // 2, rows // 2)
                top_ref[half, columns] = value[start:middle]
                bottom_ref[half, columns] = value[middle : start + rows]

        slot_part(pair_ref, chosen, depth, put)

    anywhere = pl.BlockSpec(memory_space=pl.ANY)
    whole = pl.BlockSpec(memory_space=pltpu.VMEM)
    outs = [bf16(slots, 2 * width), bf16(slots, LANES), bf16(RING, slots, depth)]
    outs += [bf16(slots // 2, depth)] * 2
    return call(
        kernel,
        tuple(outs),
        mib=24,
        grid_spec=pltpu.PrefetchScalarGridSpec(
            num_scalar_prefetch=1,
            grid=(1,),
            in_specs=[anywhere] * len(arrays) + [whole] * 5,
            out_specs=(whole,) * len(outs),
            scratch_shapes=[
                pltpu.VMEM((slots, width), jnp.float32),
                pltpu.SemaphoreType.DMA((RING,)),
            ],
        ),
    )(here, *arrays, *picked, hidden, silu, slope)


def slot_part(pair_ref, weights, depth, put):
    half = depth // 2
    width = pair_ref.shape[1] // 2

    def columns(i, carry):
        at = pl.multiple_of(i * half, half)
        value = dot(pair_ref[:, :width], weights[pl.ds(at, half)], 1, 1)
        value += dot(pair_ref[:, width:], weights[pl.ds(depth + at, half)], 1, 1)
        put(pl.ds(at, half), value.astype(jnp.bfloat16))
        return carry

    lax.fori_loop(0, 2, columns, 0)


def slot_gradients(here, pair, weights, groups):
    slots = pair.shape[0]
    width = pair.shape[1] // 2
    depth = weights[0].shape[0] // 3
    spans, at = [], 0
    for rows in groups:
        spans.append(slice(at, at + rows))
        at += rows

    def kernel(here_ref, pair_ref, *refs):
        weight_refs, out_refs, (parts, chosen, sems) = refs[:5], refs[5:-3], refs[-3:]
        t, step = here_ref[1], pl.program_id(0)

        def start(i):
            q = i + i // 2
            start_select(weight_refs, (t + q) % RING, chosen.at[i % 2], sems.at[i % 2], depth)

        @pl.when(step == 0)
        def _():
            start(0)
            start(1)

        now = step % 2
        wait_select(chosen.at[now], sems.at[now])

        def put(columns, value):
            parts[step, :, columns] = value

        slot_part(pair_ref, chosen.at[now], depth, put)

        @pl.when(step == 0)
        def _():
            start(2)

        @pl.when(step == 2)
        def _():
            for i, span in enumerate(spans):
                for j in range(3):

                    def copy_rows(k, carry):
                        at = pl.multiple_of(k * 64, 64)
                        out_refs[3 * i + j][pl.ds(at, 64)] = parts[j, pl.ds(span.start + at, 64)]
                        return carry

                    lax.fori_loop(0, (span.stop - span.start) // 64, copy_rows, 0)

    whole = pl.BlockSpec(memory_space=pltpu.VMEM)
    outs = tuple(bf16(rows, depth) for rows in groups for _ in range(3))
    parts = call(
        kernel,
        outs,
        mib=17,
        grid_spec=pltpu.PrefetchScalarGridSpec(
            num_scalar_prefetch=1,
            grid=(3,),
            in_specs=[whole] * 6,
            out_specs=(whole,) * len(outs),
            scratch_shapes=[
                pltpu.VMEM((3, slots, depth), jnp.bfloat16),
                pltpu.VMEM((2, 2 * depth, width), jnp.bfloat16),
                pltpu.SemaphoreType.DMA((2,)),
            ],
        ),
    )(here, pair, *weights)
    return [parts[3 * i : 3 * i + 3] for i in range(len(groups))]


def weight_chunk(here, distances, routed_inputs, hidden, pair, scaled, received=None):
    _, sources, _, capacity, model_width = routed_inputs.shape
    depth = model_width // RING
    slots, width = hidden.shape
    half = depth // 2
    received = received or ()
    near = len(distances) == 2

    def distance(i):
        return distances[0] + 2 * i if near else distances[0]

    def kernel(here_ref, x_ref, hidden_ref, pair_ref, scaled_ref, *refs):
        x, refs = refs[-1], refs[:-1]
        fill_rows(here_ref, x_ref, x)

        def put(at, value):
            place = pl.ds(at, value.shape[0])
            if received:
                value += refs[0][place].astype(jnp.float32) + refs[1][place].astype(jnp.float32)
                for i in range(2):

                    @pl.when((at >= i * depth) & (at < (i + 1) * depth))
                    def _():
                        refs[2 + i][pl.ds(at - i * depth, value.shape[0])] = value

                return value
            if near:
                for i in range(2):

                    @pl.when(pl.program_id(0) == i)
                    def _():
                        refs[i][place] = value.astype(jnp.bfloat16)

                return value
            for i in range(2):

                @pl.when((at >= 3 * i * half) & (at < 3 * (i + 1) * half))
                def _():
                    start = at - 3 * i * half
                    refs[i][pl.ds(start, value.shape[0])] = value.astype(jnp.bfloat16)

            return value

        def inputs_part(i, carry):
            columns = pl.ds(pl.multiple_of((i % 2) * half, half), half)
            lanes = pl.ds(pl.multiple_of((i // 2) * width, width), width)
            put(pl.multiple_of(i * half, half), dot(x[:, columns], pair_ref[:, lanes], 0, 0))
            return carry

        def down_part(c, carry):
            lanes = pl.ds(pl.multiple_of(c * width, width), width)
            value = dot(hidden_ref[...], scaled_ref[0, :, lanes], 0, 0)
            at = pl.multiple_of(2 * depth + c * width, width)
            value = put(at, value)
            if received:
                refs[4][:, lanes] = value
            return carry

        lax.fori_loop(0, 4, inputs_part, 0)
        lax.fori_loop(0, depth // width, down_part, 0)

    whole = pl.BlockSpec(memory_space=pltpu.VMEM)
    if received:
        outs = (f32(depth, width), f32(depth, width), f32(width, depth))
    elif near:
        outs = (bf16(6 * half, width),) * 2
    else:
        outs = (bf16(3 * half, width),) * 2
    return call(
        kernel,
        outs,
        mib=18 if received else 14,
        grid_spec=pltpu.PrefetchScalarGridSpec(
            num_scalar_prefetch=1,
            grid=(len(distances),),
            in_specs=[
                pl.BlockSpec(
                    (1, sources, 1, capacity, depth),
                    lambda i, here: (0, 0, 0, 0, (here[0] + distance(i)) % RING),
                ),
                whole,
                whole,
                pl.BlockSpec((1, slots, depth), lambda i, here: (distance(i), 0, 0)),
            ]
            + [whole] * len(received),
            out_specs=(whole,) * len(outs),
            scratch_shapes=[pltpu.VMEM((slots, depth), jnp.bfloat16)],
        ),
    )(here, routed_inputs, hidden, pair, scaled, *received)


def join(outs):
    arrays = []
    for out in outs:
        for array, _, _ in out:
            if not any(array is a for a in arrays):
                arrays.append(array)
    index = {id(a): i for i, a in enumerate(arrays)}

    def kernel(*refs):
        for out, out_ref in zip(outs, refs[len(arrays) :]):
            at = 0
            for array, first, rows in out:
                out_ref[pl.ds(at, rows)] = refs[index[id(array)]][first : first + rows]
                at += rows

    columns = arrays[0].shape[1]
    shapes = tuple(bf16(sum(rows for _, _, rows in out), columns) for out in outs)
    return call(kernel, shapes)(*arrays)


def messages(own, other):
    count = len(SHIFTS)
    rows, columns = own.shape
    rows //= count

    def kernel(own_ref, other_ref, *out_refs):
        for j, out_ref in enumerate(out_refs):
            out_ref[:rows] = own_ref[j * rows : (j + 1) * rows]
            out_ref[rows:] = other_ref[j * rows : (j + 1) * rows]

    return call(kernel, (bf16(2 * rows, columns),) * count)(own, other)


def unpack_messages(blocks):
    rows, columns = blocks[0].shape
    rows //= 2

    def kernel(*refs):
        own_ref, other_ref = refs[-2:]
        for j, ref in enumerate(refs[:-2]):
            own_ref[pl.ds(j * rows, rows)] = ref[:rows]
            other_ref[pl.ds(j * rows, rows)] = ref[rows:]

    return call(kernel, (bf16(len(blocks) * rows, columns),) * 2)(*blocks)


def leaving_rows(own, from_prev, from_next, extra, start, count):
    rows, narrow = own.shape
    rows //= count

    def kernel(own_ref, prev_ref, next_ref, extra_ref, *out_refs):
        for j, out_ref in enumerate(out_refs):
            span = slice(j * rows, (j + 1) * rows)
            total = own_ref[span].astype(jnp.float32) + prev_ref[span].astype(jnp.float32)
            total += next_ref[span].astype(jnp.float32)
            out_ref[:, :narrow] = total.astype(jnp.bfloat16)
            out_ref[:, narrow:] = extra_ref[start + j * rows : start + (j + 1) * rows]

    outs = (bf16(rows, narrow + LANES),) * count
    return call(kernel, outs)(own, from_prev, from_next, extra)


def token_rows(slot_index, back):
    tokens = slot_index.shape[0]
    rows, wide = back[0].shape
    narrow = wide - LANES

    def kernel(slot_ref, *refs):
        out_ref = refs[-1]
        total = jnp.zeros((tokens, narrow), jnp.float32)
        chosen = [jnp.zeros((tokens, LANES), jnp.float32)] * 2
        for h, back_ref in enumerate(refs[:-1]):
            slot = lax.broadcasted_iota(jnp.int32, (tokens, rows), 1) + h * rows
            picks = [
                jnp.where(slot_ref[:, k : k + 1] == slot, 1.0, 0.0).astype(jnp.bfloat16)
                for k in range(2)
            ]
            total += dot(picks[0] + picks[1], back_ref[:, :narrow])
            chosen = [c + dot(p, back_ref[:, narrow:]) for c, p in zip(chosen, picks)]
        out_ref[:, :narrow] = total.astype(jnp.bfloat16)
        lane = lax.broadcasted_iota(jnp.int32, (tokens, LANES), 1)
        tail = jnp.zeros((tokens, LANES), jnp.float32)
        for k in range(2):
            value = chosen[k][:, 0:1] + chosen[k][:, 1:2]
            high = value.astype(jnp.bfloat16).astype(jnp.float32)
            tail = jnp.where(lane == 2 * k, high, jnp.where(lane == 2 * k + 1, value - high, tail))
        out_ref[:, narrow:] = tail.astype(jnp.bfloat16)

    return call(kernel, bf16(tokens, wide))(slot_index, *back)


def finish_tokens(here, gate_probs, gathered):
    tokens, wide = gathered[0].shape
    narrow = wide - LANES

    def kernel(here_ref, probs_ref, *refs):
        out_ref, logit_ref = refs[RING:]
        total = jnp.zeros((tokens, LANES), jnp.float32)
        for q in range(RING):
            first = ((here_ref[0] + here_ref[1] + q) % RING) * narrow
            out_ref[:, pl.ds(pl.multiple_of(first, LANES), narrow)] = refs[q][:, :narrow]
            total += refs[q][:, narrow:].astype(jnp.float32)
        chosen = [
            (total[:, 2 * k : 2 * k + 1] + total[:, 2 * k + 1 : 2 * k + 2])
            .astype(jnp.bfloat16)
            .astype(jnp.float32)
            for k in range(2)
        ]
        both = chosen[0] + chosen[1]
        for k in range(2):
            logit_ref[:, k : k + 1] = chosen[k] - probs_ref[:, k : k + 1] * both

    whole = pl.BlockSpec(memory_space=pltpu.VMEM)
    return call(
        kernel,
        (bf16(tokens, RING * narrow), f32(tokens, 2)),
        grid_spec=pltpu.PrefetchScalarGridSpec(
            num_scalar_prefetch=1,
            grid=(1,),
            in_specs=[whole] * (RING + 1),
            out_specs=(whole,) * 2,
        ),
    )(here, gate_probs, *gathered)


def slots_of(routes, z, core, capacity, experts):
    tokens = routes.shape[0]
    hot = (routes[:, :, None] == jnp.arange(experts, dtype=jnp.int32)).astype(jnp.bfloat16)
    before = jnp.arange(tokens)[:, None] > jnp.arange(tokens)[None, :]
    earlier = dot(before.astype(jnp.bfloat16), hot[:, 0] + hot[:, 1])
    place = jnp.sum(earlier[:, None, :] * hot.astype(jnp.float32), axis=2).astype(jnp.int32)
    count = len(SHIFTS)
    distance = (routes // 2 - z + count) % count
    index = jnp.where(
        distance <= count // 2, jnp.maximum(2 * distance - 1, 0), 2 * (count - distance)
    )
    other = (routes % 2 != core).astype(jnp.int32)
    return (other * count + index) * capacity + place


def layer(out_grad, routes, chosen_logits, routed_inputs, w_gate, w_up, w_down):
    experts = lax.axis_size("ep")
    f, t = lax.axis_index("fsdp"), lax.axis_index("tp")
    z, core = lax.axis_index("ep") // 2, lax.axis_index("ep") % 2
    here = jnp.stack([f, t, z, core]).astype(jnp.int32)
    model_width = out_grad.shape[1]
    capacity = routed_inputs.shape[3]
    slots = experts * capacity
    narrow = model_width // RING
    width = w_gate.shape[2]
    block = 2 * capacity

    weights = ring_gather(pack(w_gate[0], w_up[0], w_down[0]), "fsdp")

    gate_probs = jax.nn.softmax(chosen_logits, axis=-1)
    slot_index = slots_of(routes, z, core, capacity, experts)
    piece = lax.dynamic_slice_in_dim(out_grad, ((f + t) % RING) * narrow, narrow, 1)
    weighted = gate_probs[:, :, None] * piece.astype(jnp.float32)[:, None, :]
    weighted = weighted.astype(jnp.bfloat16)

    def routed(first):
        slot = first + jnp.arange(slots // 2, dtype=jnp.int32)
        picks = (slot_index[:, :, None] == slot).astype(jnp.bfloat16)
        return lax.dot_general(
            picks, weighted, (((0, 1), (0, 1)), ((), ())), preferred_element_type=jnp.float32
        ).astype(jnp.bfloat16)

    own, other = routed(0), swap_cores(routed(slots // 2))
    sent = messages(own, other)
    arrived = [sent[0]] + [shift_z(sent[j], SHIFTS[j]) for j in range(1, len(SHIFTS))]
    groups = [len(group) * block for group in GROUPS]
    count0, count1 = groups
    half = count0 // 2
    own0 = join([[(arrived[j], 0, block) for j in GROUPS[0]]])[0]
    prev0, next0 = shift(own0, "tp", 1), shift(own0, "tp", -1)
    pieces = [(arrived[j], 0, block) for j in GROUPS[1]]
    own1, prev1, next1 = join(
        [pieces, pieces + [(prev0, 0, half)], pieces + [(next0, half, half)]]
    )
    prev1, next1 = shift(prev1, "tp", 1), shift(next1, "tp", -1)
    far1 = shift(own1, "tp", 2)
    arrays = [own0, next0, prev0, own1, next1, prev1, far1]
    places = [(0, 0, 0, 0, count0), (1, 0, 1, 0, count0), (2, 0, 3, 0, count0)]
    places += [(3, 0, 0, count0, count1), (4, 0, 1, count0, count1), (5, 0, 3, count0, count1)]
    places += [(5, count1, 2, 0, half), (4, count1, 2, half, half), (6, 0, 2, count0, count1)]

    hidden, silu, slope = activations(here, routed_inputs, weights, width)
    pair, extra, scaled, *far = pair_gradients(
        here, arrays, places, pick_weights(here, weights), hidden, silu, slope, groups
    )
    far = far_halves(*far, "tp")
    parts = slot_gradients(here, pair, weights, groups)
    leaving = []
    for g, group in enumerate(GROUPS):
        own, following, prev = parts[g]
        start = group[0] * block
        following = add_half(following, far[0], 0, start // 2)
        prev = add_half(prev, far[1], 1, start // 2)
        received = neighbours(following, prev, "tp")
        leaving += leaving_rows(own, *received, extra, start, len(group))

    chunk = functools.partial(
        weight_chunk, here, routed_inputs=routed_inputs, hidden=hidden, pair=pair, scaled=scaled
    )
    far = far_halves(*chunk((2,)), "fsdp")
    following, prev = chunk((1, 3))
    received = neighbours(add_half(following, far[0], 0), add_half(prev, far[1], 1), "fsdp")
    grad_gate, grad_up, grad_down = chunk((0,), received=received)

    returned = [leaving[0]] + [shift_z(leaving[j], -SHIFTS[j]) for j in range(1, len(SHIFTS))]
    own, other = unpack_messages(returned)
    mine = token_rows(slot_index, [own, swap_cores(other)])
    tokens_by_ring = [mine] + [shift(mine, "tp", -q) for q in range(1, RING)]
    input_grad, logit_grad = finish_tokens(here, gate_probs, tokens_by_ring)
    return input_grad, logit_grad, grad_gate[None], grad_up[None], grad_down[None]


def solution(mesh):
    return jax.shard_map(
        layer,
        mesh=mesh,
        in_specs=(
            P(("ep", "fsdp"), None),
            P(("ep", "fsdp"), None),
            P(("ep", "fsdp"), None),
            P("ep", None, "fsdp", None, None),
            P("ep", "fsdp", "tp"),
            P("ep", "fsdp", "tp"),
            P("ep", "tp", "fsdp"),
        ),
        out_specs=(
            P(("ep", "fsdp"), None),
            P(("ep", "fsdp"), None),
            P("ep", "fsdp", "tp"),
            P("ep", "fsdp", "tp"),
            P("ep", "tp", "fsdp"),
        ),
        check_vma=False,
    )
```
